32 devices in a mesh: pair: 2 (over x), tp: 4 (over z), side: 4 (over y, core).
Axes of the slice: x: 2, y: 2, z: 4, core: 2. Of those that a mesh axis runs over, the one named last changes fastest.
Arguments:
- x_prompt: bfloat16 [8, 2048, 3584], P(('pair', 'side')), parts along dimension 0
- s_len: int32 [8], P(('pair', 'side')), parts along dimension 0
- y_tok: bfloat16 [256, 3584], P(('pair', 'side')), parts along dimension 0
- c_len: int32 [256], P(('pair', 'side')), parts along dimension 0
- k_cache: bfloat16 [1, 256, 256, 4, 128], P(None, ('pair', 'side'), 'tp'), parts along dimension 1
- v_cache: bfloat16 [1, 256, 256, 4, 128], P(None, ('pair', 'side'), 'tp'), parts along dimension 1
- attn_gain: bfloat16 [1, 3584], replicated
- w_qkv: bfloat16 [1, 3584, 4, 9, 128], P(None, None, 'tp')
- w_out: bfloat16 [1, 4, 7, 128, 3584], P(None, 'tp')
- mlp_gain: bfloat16 [1, 3584], replicated
- w_gate_up: bfloat16 [1, 3584, 2, 18944], P(None, None, None, 'tp')
- w_down: bfloat16 [1, 18944, 3584], P(None, 'tp')
Outputs:
- output 1: bfloat16 [8, 2048, 3584], P(('pair', 'side')), parts along dimension 0
- output 2: bfloat16 [256, 3584], P(('pair', 'side')), parts along dimension 0
- output 3: bfloat16 [1, 8, 2048, 4, 128], P(None, ('pair', 'side'), 'tp'), parts along dimension 1
- output 4: bfloat16 [1, 8, 2048, 4, 128], P(None, ('pair', 'side'), 'tp'), parts along dimension 1
- output 5: bfloat16 [1, 256, 256, 4, 128], P(None, ('pair', 'side'), 'tp'), parts along dimension 1
- output 6: bfloat16 [1, 256, 256, 4, 128], P(None, ('pair', 'side'), 'tp'), parts along dimension 1
There are 2 independent parts. The reference program is written for one: setup_inputs(seed, part) draws one part's arguments, and reference() takes and returns one part's arrays. A program takes and returns all parts, laid end to end along the dimension named above; an argument that names none is the same for every part.
All inputs are finite; a program needn't handle non-finite values.
Results may differ from the reference program's by a relative error of at most 0.0063243.
Values are sent between devices in bfloat16 or wider.
A program may use at most 1 GiB of HBM per device.

```python
import jax
import jax.numpy as jnp
from jax import lax

D = 3584
HEADS = 28
KV_HEADS = 4
HEAD = 128
FF = 18944
PROMPT_LEN = 2048
BATCH_DEC = 32
CACHE_LEN = 256
LAYERS = 1
GROUPS = 4
Q_BLOCK = 128
GROUP_Q = HEADS // KV_HEADS
ROPE_BASE = 10000.0
NORM_EPS = 1e-5


def setup_inputs(seed: int = 0, part: int = 0) -> dict:
    rng_key = jax.random.fold_in(jax.random.key(seed), part)
    key_list = jax.random.split(rng_key, 6)
    shared = jax.random.split(jax.random.key(seed + 1), 6)
    cache_shape = (LAYERS, GROUPS * BATCH_DEC, CACHE_LEN, KV_HEADS, HEAD)
    x_prompt = jax.random.normal(key_list[0], (GROUPS, PROMPT_LEN, D), jnp.float32).astype(jnp.bfloat16)
    s_len = jax.random.randint(key_list[1], (GROUPS,), PROMPT_LEN // 2, PROMPT_LEN + 1, jnp.int32)
    s_len = s_len.at[0].set(PROMPT_LEN)
    y_tok = jax.random.normal(key_list[2], (GROUPS * BATCH_DEC, D), jnp.float32).astype(jnp.bfloat16)
    c_len = jax.random.randint(key_list[3], (GROUPS, BATCH_DEC), CACHE_LEN // 2, CACHE_LEN, jnp.int32)
    c_len = c_len.at[:, 0].set(CACHE_LEN - 1).reshape(GROUPS * BATCH_DEC)
    k_cache = (1.5 * jax.random.normal(key_list[4], cache_shape, jnp.float32)).astype(jnp.bfloat16)
    v_cache = jax.random.normal(key_list[5], cache_shape, jnp.float32).astype(jnp.bfloat16)
    attn_gain = (1.0 + 0.3 * jax.random.normal(shared[0], (LAYERS, D), jnp.float32)).astype(jnp.bfloat16)
    w_qkv = (jax.random.normal(shared[1], (LAYERS, D, KV_HEADS, GROUP_Q + 2, HEAD), jnp.float32) * D ** -0.5).astype(jnp.bfloat16)
    w_out = (jax.random.normal(shared[2], (LAYERS, KV_HEADS, GROUP_Q, HEAD, D), jnp.float32) * (HEADS * HEAD) ** -0.5).astype(jnp.bfloat16)
    mlp_gain = (1.0 + 0.3 * jax.random.normal(shared[3], (LAYERS, D), jnp.float32)).astype(jnp.bfloat16)
    w_gate_up = (jax.random.normal(shared[4], (LAYERS, D, 2, FF), jnp.float32) * D ** -0.5).astype(jnp.bfloat16)
    w_down = (jax.random.normal(shared[5], (LAYERS, FF, D), jnp.float32) * FF ** -0.5).astype(jnp.bfloat16)
    return {'x_prompt': x_prompt, 's_len': s_len, 'y_tok': y_tok, 'c_len': c_len, 'k_cache': k_cache, 'v_cache': v_cache, 'attn_gain': attn_gain, 'w_qkv': w_qkv, 'w_out': w_out, 'mlp_gain': mlp_gain, 'w_gate_up': w_gate_up, 'w_down': w_down}


def rms_norm(hidden, norm_gain):
    hidden_f32 = hidden.astype(jnp.float32)
    inv_rms = lax.rsqrt(jnp.mean(hidden_f32 * hidden_f32, axis=-1, keepdims=True) + NORM_EPS)
    return (hidden_f32 * inv_rms * norm_gain.astype(jnp.float32)).astype(jnp.bfloat16)


def rope_rotate(vals_f32, positions):
    half_dim = HEAD // 2
    inv_freq = ROPE_BASE ** (-2.0 * jnp.arange(half_dim, dtype=jnp.float32) / HEAD)
    angles = positions.astype(jnp.float32)[:, None] * inv_freq[None, :]
    cos_table = jnp.cos(angles)[:, None, None, :]
    sin_table = jnp.sin(angles)[:, None, None, :]
    first_half = vals_f32[..., :half_dim]
    second_half = vals_f32[..., half_dim:]
    return jnp.concatenate([first_half * cos_table - second_half * sin_table, second_half * cos_table + first_half * sin_table], axis=-1)


def mlp_sum(hidden, norm_gain, w_gate_up, w_down):
    normed = rms_norm(hidden, norm_gain)
    gate_up = jnp.einsum('nd,dcf->ncf', normed.astype(jnp.float32), w_gate_up.astype(jnp.float32))
    activated = (jax.nn.silu(gate_up[:, 0]) * gate_up[:, 1]).astype(jnp.bfloat16)
    return jnp.dot(activated, w_down, preferred_element_type=jnp.float32)


def prefill_context(queries, key_rows, value_rows, key_valid):
    positions = jnp.arange(PROMPT_LEN)
    query_blocks = queries.reshape(PROMPT_LEN // Q_BLOCK, Q_BLOCK, KV_HEADS, GROUP_Q, HEAD)
    block_starts = jnp.arange(PROMPT_LEN // Q_BLOCK) * Q_BLOCK
    key_f32 = key_rows.astype(jnp.float32)
    value_f32 = value_rows.astype(jnp.float32)

    def attend_block(block_args):
        query_block, block_start = block_args
        scores = jnp.einsum('qkgh,tkh->kgqt', query_block.astype(jnp.float32), key_f32) * HEAD ** -0.5
        query_pos = block_start + jnp.arange(Q_BLOCK)
        allowed = (positions[None, :] <= query_pos[:, None]) & key_valid[None, :]
        scores = jnp.where(allowed, scores, -1e30)
        weights = jnp.exp(scores - jnp.max(scores, axis=-1, keepdims=True))
        weight_sum = jnp.sum(weights, axis=-1, keepdims=True)
        mixed_sum = jnp.einsum('kgqt,tkh->kgqh', weights.astype(jnp.bfloat16).astype(jnp.float32), value_f32)
        return jnp.transpose(mixed_sum / weight_sum, (2, 0, 1, 3)).astype(jnp.bfloat16)

    context = lax.map(attend_block, (query_blocks, block_starts))
    return context.reshape(PROMPT_LEN, KV_HEADS, GROUP_Q, HEAD)


def prefill_group(prompt_one, slen_one, weight_stack):
    positions = jnp.arange(PROMPT_LEN)
    key_valid = positions < slen_one
    keep_mask = key_valid[:, None, None].astype(jnp.bfloat16)

    def layer_step(hidden, layer_weights):
        gain_attn, w_qkv, w_out, gain_mlp, w_gate_up, w_down = layer_weights
        normed = rms_norm(hidden, gain_attn)
        projected = jnp.einsum('sd,dkjh->skjh', normed.astype(jnp.float32), w_qkv.astype(jnp.float32))
        rotated = rope_rotate(projected[:, :, :GROUP_Q + 1], positions).astype(jnp.bfloat16)
        value_rows = projected[:, :, GROUP_Q + 1].astype(jnp.bfloat16)
        key_rows = rotated[:, :, GROUP_Q]
        context = prefill_context(rotated[:, :, :GROUP_Q], key_rows, value_rows, key_valid)
        attn_sum = jnp.einsum('skgh,kghd->sd', context.astype(jnp.float32), w_out.astype(jnp.float32))
        hidden = (hidden.astype(jnp.float32) + attn_sum).astype(jnp.bfloat16)
        down_sum = mlp_sum(hidden, gain_mlp, w_gate_up, w_down)
        hidden = (hidden.astype(jnp.float32) + down_sum).astype(jnp.bfloat16)
        return hidden, (key_rows * keep_mask, value_rows * keep_mask)

    hidden, (key_all, value_all) = lax.scan(layer_step, prompt_one, weight_stack)
    return hidden, key_all, value_all


def decode_group(tokens, cache_lens, key_cache, value_cache, weight_stack):
    cache_pos = jnp.arange(CACHE_LEN)
    write_mask = (cache_pos[None, :] == cache_lens[:, None])[:, :, None, None]
    allowed = (cache_pos[None, :] <= cache_lens[:, None])[:, None, None, :]

    def layer_step(hidden, layer_weights):
        gain_attn, w_qkv, w_out, gain_mlp, w_gate_up, w_down, key_old, value_old = layer_weights
        normed = rms_norm(hidden, gain_attn)
        projected = jnp.einsum('bd,dkjh->bkjh', normed.astype(jnp.float32), w_qkv.astype(jnp.float32))
        rotated = rope_rotate(projected[:, :, :GROUP_Q + 1], cache_lens).astype(jnp.bfloat16)
        value_new = projected[:, :, GROUP_Q + 1].astype(jnp.bfloat16)
        key_now = jnp.where(write_mask, rotated[:, None, :, GROUP_Q], key_old)
        value_now = jnp.where(write_mask, value_new[:, None], value_old)
        scores = jnp.einsum('bkgh,btkh->bkgt', rotated[:, :, :GROUP_Q].astype(jnp.float32), key_now.astype(jnp.float32)) * HEAD ** -0.5
        scores = jnp.where(allowed, scores, -1e30)
        weights = jnp.exp(scores - jnp.max(scores, axis=-1, keepdims=True))
        weight_sum = jnp.sum(weights, axis=-1)
        mixed_sum = jnp.einsum('bkgt,btkh->bkgh', weights.astype(jnp.bfloat16).astype(jnp.float32), value_now.astype(jnp.float32))
        context = (mixed_sum / weight_sum[..., None]).astype(jnp.bfloat16)
        attn_sum = jnp.einsum('bkgh,kghd->bd', context.astype(jnp.float32), w_out.astype(jnp.float32))
        hidden = (hidden.astype(jnp.float32) + attn_sum).astype(jnp.bfloat16)
        down_sum = mlp_sum(hidden, gain_mlp, w_gate_up, w_down)
        hidden = (hidden.astype(jnp.float32) + down_sum).astype(jnp.bfloat16)
        return hidden, (key_now, value_now)

    hidden, (key_all, value_all) = lax.scan(layer_step, tokens, weight_stack + (key_cache, value_cache))
    return hidden, key_all, value_all


def reference(x_prompt, s_len, y_tok, c_len, k_cache, v_cache, attn_gain, w_qkv, w_out, mlp_gain, w_gate_up, w_down):
    weight_stack = (attn_gain, w_qkv, w_out, mlp_gain, w_gate_up, w_down)

    def run_prefill(group_args):
        return prefill_group(group_args[0], group_args[1], weight_stack)

    hidden_out, key_pre, value_pre = lax.map(run_prefill, (x_prompt, s_len))
    k_prompt = jnp.moveaxis(jnp.roll(key_pre, 1, axis=0), 0, 1)
    v_prompt = jnp.moveaxis(jnp.roll(value_pre, 1, axis=0), 0, 1)
    cache_shape = (LAYERS, GROUPS, BATCH_DEC, CACHE_LEN, KV_HEADS, HEAD)

    def run_decode(group_args):
        return decode_group(group_args[0], group_args[1], group_args[2], group_args[3], weight_stack)

    decode_in = (y_tok.reshape(GROUPS, BATCH_DEC, D), c_len.reshape(GROUPS, BATCH_DEC), jnp.moveaxis(k_cache.reshape(cache_shape), 1, 0), jnp.moveaxis(v_cache.reshape(cache_shape), 1, 0))
    y_out, key_new, value_new = lax.map(run_decode, decode_in)
    k_cache_out = jnp.moveaxis(key_new, 0, 1).reshape(k_cache.shape)
    v_cache_out = jnp.moveaxis(value_new, 0, 1).reshape(v_cache.shape)
    return (hidden_out, y_out.reshape(GROUPS * BATCH_DEC, D), k_prompt, v_prompt, k_cache_out, v_cache_out)
```

```python
import functools

import jax
import jax.numpy as jnp
from jax import lax
from jax.experimental import pallas as pl
from jax.experimental.pallas import tpu as pltpu
from jax.sharding import PartitionSpec as P

ROPE_BASE = 10000.0
NORM_EPS = 1e-5
LOG2E = 1.4426950408889634
BF = jnp.bfloat16
F32 = jnp.float32


def rms_norm(hidden, norm_gain):
    hidden_f32 = hidden.astype(F32)
    inv_rms = lax.rsqrt(jnp.mean(hidden_f32 * hidden_f32, axis=-1, keepdims=True) + NORM_EPS)
    return (hidden_f32 * inv_rms * norm_gain.astype(F32)).astype(BF)


def rope_tables(positions, head_dim):
    half_dim = head_dim // 2
    inv_freq = ROPE_BASE ** (-2.0 * jnp.arange(half_dim, dtype=F32) / head_dim)
    angles = positions.astype(F32)[:, None] * inv_freq[None, :]
    return jnp.cos(angles), jnp.sin(angles)


def rope_rotate(vals_f32, positions):
    half_dim = vals_f32.shape[-1] // 2
    cos_table, sin_table = rope_tables(positions, vals_f32.shape[-1])
    cos_table, sin_table = cos_table[:, None, None, :], sin_table[:, None, None, :]
    first_half = vals_f32[..., :half_dim]
    second_half = vals_f32[..., half_dim:]
    return jnp.concatenate([first_half * cos_table - second_half * sin_table, second_half * cos_table + first_half * sin_table], axis=-1)


def qkv_kernel(x_ref, gain_ref, cos_ref, sin_ref, w_ref, o_ref):
    slots = w_ref.shape[0]
    x = x_ref[...].astype(F32)
    inv = lax.rsqrt(jnp.mean(x * x, axis=-1, keepdims=True) + NORM_EPS)
    normed = (x * inv * gain_ref[...].astype(F32)).astype(BF)
    cos, sin = cos_ref[...], sin_ref[...]
    for first in range(0, slots, 2):
        group = range(first, min(first + 2, slots))
        w = jnp.concatenate([w_ref[s] for s in group], axis=-1)
        y = jnp.dot(normed, w, preferred_element_type=F32)
        for n, s in enumerate(group):
            part = y[:, n * 128:(n + 1) * 128]
            if s < slots - 1:
                part = part * cos + pltpu.roll(part, 64, 1) * sin
            o_ref[s] = part.astype(BF)


def project_qkv(x, gain, cos, sin, w, rows_block=256):
    rows, width = x.shape
    slots, _, head = w.shape
    return pl.pallas_call(
        qkv_kernel,
        grid=(rows // rows_block,),
        in_specs=[
            pl.BlockSpec((rows_block, width), lambda i: (i, 0)),
            pl.BlockSpec((1, width), lambda i: (0, 0)),
            pl.BlockSpec((rows_block, head), lambda i: (i, 0)),
            pl.BlockSpec((rows_block, head), lambda i: (i, 0)),
            pl.BlockSpec((slots, width, head), lambda i: (0, 0, 0), pipeline_mode=pl.Buffered(1)),
        ],
        out_specs=pl.BlockSpec((slots, rows_block, head), lambda i: (0, i, 0)),
        out_shape=jax.ShapeDtypeStruct((slots, rows, head), BF),
        cost_estimate=pl.CostEstimate(flops=2 * rows * width * slots * head, bytes_accessed=2 * (rows * width + slots * head * (width + rows)), transcendentals=0),
        name="project_qkv",
    )(x, gain, cos, sin, w)


def flash_kernel(block_q, block_k, slen_ref, q_ref, k_ref, v_ref, o_ref, m_ref, l_ref, acc_ref):
    i = pl.program_id(0)
    heads, _, head = q_ref.shape
    rows = heads * block_q
    slen = slen_ref[0]
    scale = head ** -0.5 * LOG2E
    q = q_ref[...].reshape(rows, head)
    m_ref[...] = jnp.full_like(m_ref, -jnp.inf)
    l_ref[...] = jnp.zeros_like(l_ref)
    acc_ref[...] = jnp.zeros_like(acc_ref)

    def step(j, masked):
        start = pl.multiple_of(j * block_k, block_k)
        k = k_ref[0, pl.ds(start, block_k), :]
        v = v_ref[0, pl.ds(start, block_k), :]
        s = lax.dot_general(q, k, (((1,), (1,)), ((), ())), preferred_element_type=F32)
        if masked:
            q_pos = i * block_q + lax.broadcasted_iota(jnp.int32, (block_q, block_k), 0)
            k_pos = start + lax.broadcasted_iota(jnp.int32, (block_q, block_k), 1)
            allowed = (k_pos <= q_pos) & (k_pos < slen)
            s = jnp.where(allowed[None], s.reshape(heads, block_q, block_k), -1e30).reshape(rows, block_k)
        m_old = m_ref[...]
        m_new = jnp.maximum(m_old, jnp.max(s, axis=-1, keepdims=True))
        alpha = jnp.exp2((m_old - m_new) * scale)
        p = jnp.exp2((s - m_new) * scale)
        l_ref[...] = l_ref[...] * alpha + jnp.sum(p, axis=-1, keepdims=True)
        acc_ref[...] = acc_ref[...] * alpha + jnp.dot(p.astype(BF), v, preferred_element_type=F32)
        m_ref[...] = m_new

    count = (i * block_q + block_q - 1) // block_k + 1

    @pl.loop(0, count)
    def _(j):
        edge = ((j + 1) * block_k > i * block_q) | ((j + 1) * block_k > slen)

        @pl.when(edge)
        def _():
            step(j, True)

        @pl.when(jnp.logical_not(edge))
        def _():
            step(j, False)

    out = (acc_ref[...] / l_ref[...]).astype(BF)
    for h in range(heads):
        o_ref[:, h * head:(h + 1) * head] = out[h * block_q:(h + 1) * block_q]


def attend(slen, qkv, block_q=256, block_k=512):
    slots, rows, head = qkv.shape
    heads = slots - 2
    return pl.pallas_call(
        functools.partial(flash_kernel, block_q, block_k),
        grid_spec=pltpu.PrefetchScalarGridSpec(
            num_scalar_prefetch=1,
            grid=(rows // block_q,),
            in_specs=[
                pl.BlockSpec((heads, block_q, head), lambda i, _: (0, i, 0)),
                pl.BlockSpec((1, rows, head), lambda i, _: (heads, 0, 0)),
                pl.BlockSpec((1, rows, head), lambda i, _: (heads + 1, 0, 0)),
            ],
            out_specs=pl.BlockSpec((block_q, heads * head), lambda i, _: (i, 0)),
            scratch_shapes=[
                pltpu.VMEM((heads * block_q, 1), F32),
                pltpu.VMEM((heads * block_q, 1), F32),
                pltpu.VMEM((heads * block_q, head), F32),
            ],
        ),
        out_shape=jax.ShapeDtypeStruct((rows, heads * head), BF),
        cost_estimate=pl.CostEstimate(flops=3 * heads * rows * rows * head, bytes_accessed=2 * (2 * heads + 2) * rows * head, transcendentals=heads * rows * rows // 2),
        name="attend",
    )(slen, qkv, qkv, qkv)


def decode_context(tokens, cache_lens, k_cache, v_cache, gain, w_qkv):
    group_q = w_qkv.shape[2] - 2
    head_dim = w_qkv.shape[3]
    cache_local = k_cache.shape[1]
    cache_pos = lax.axis_index('tp') * cache_local + jnp.arange(cache_local)
    write_mask = (cache_pos[None, :] == cache_lens[:, None])[:, :, None, None]
    allowed = (cache_pos[None, :] <= cache_lens[:, None])[:, None, None, :]
    normed = rms_norm(tokens, gain)
    projected = jnp.einsum('bd,dkjh->bkjh', normed, w_qkv, preferred_element_type=F32)
    rotated = rope_rotate(projected[:, :, :group_q + 1], cache_lens)
    local_qkv = jnp.concatenate([rotated, projected[:, :, group_q + 1:]], axis=2).astype(BF)
    full_qkv = lax.all_gather(local_qkv, 'tp', axis=1, tiled=True)
    key_now = jnp.where(write_mask, full_qkv[:, None, :, group_q], k_cache)
    value_now = jnp.where(write_mask, full_qkv[:, None, :, group_q + 1], v_cache)
    scores = jnp.einsum('bkgh,btkh->bkgt', full_qkv[:, :, :group_q], key_now, preferred_element_type=F32) * head_dim ** -0.5
    scores = jnp.where(allowed, scores, -1e30)
    score_max = lax.pmax(jnp.max(scores, axis=-1, keepdims=True), 'tp')
    weights = jnp.exp(scores - score_max)
    sum_own = lax.psum_scatter(jnp.sum(weights, axis=-1), 'tp', scatter_dimension=1, tiled=True)
    mixed_sum = jnp.einsum('bkgt,btkh->bkgh', weights.astype(BF), value_now, preferred_element_type=F32)
    mixed_own = lax.psum_scatter(mixed_sum, 'tp', scatter_dimension=1, tiled=True)
    context = (mixed_own / sum_own[..., None]).astype(BF)
    return context, key_now, value_now


def gather_w_out(w_out, mesh):
    plane = mesh.shape['pair'] * mesh.shape['side']
    rows = w_out.shape[0] // plane
    index = lax.axis_index('pair') * mesh.shape['side'] + lax.axis_index('side')
    own = lax.dynamic_slice_in_dim(w_out, index * rows, rows, 0)
    column = lax.all_gather(own, 'tp')
    return lax.all_gather(column, ('pair', 'side'))


def solution(mesh):
    side_size = mesh.shape['side']
    tp = mesh.shape['tp']
    send_pairs = [(source, (source + 1) % side_size) for source in range(side_size)]
    group_axes = ('pair', 'side')

    def device_fn(x_prompt, s_len, y_tok, c_len, k_cache, v_cache, attn_gain, w_qkv, w_out, mlp_gain, w_gate_up, w_down):
        x = x_prompt[0]
        seq_len, width = x.shape
        group_q, head = w_qkv.shape[3] - 2, w_qkv.shape[4]
        positions = jnp.arange(seq_len)
        keep_mask = (positions < s_len[0])[:, None].astype(BF)
        cos, sin = rope_tables(positions, head)
        cos, sin = jnp.concatenate([cos, cos], -1), jnp.concatenate([-sin, sin], -1)

        w_full = gather_w_out(w_out[0, 0].reshape(group_q * head, width), mesh)
        w_full = jnp.moveaxis(w_full, 1, 0).reshape(tp, group_q * head, width)

        dctx, key_now, value_now = decode_context(y_tok, c_len, k_cache[0], v_cache[0], attn_gain[0], w_qkv[0])
        dctx = dctx.reshape(dctx.shape[0], group_q * head)

        w_slots = jnp.transpose(w_qkv[0, :, 0], (1, 0, 2))
        qkv = project_qkv(x, attn_gain, cos, sin, w_slots)
        ctx = attend(s_len, qkv)

        chunks = 4
        step = seq_len // chunks
        hid = []
        outs = []
        for c in range(chunks):
            ctx_c, x_c = ctx[c * step:(c + 1) * step], x[c * step:(c + 1) * step]
            if c == 0:
                ctx_c, x_c = jnp.concatenate([ctx_c, dctx]), jnp.concatenate([x_c, y_tok])
            full = lax.all_gather(ctx_c, 'tp')
            mixed = jnp.einsum('trf,tfd->rd', full, w_full, preferred_element_type=F32)
            hid.append((x_c.astype(F32) + mixed).astype(BF))
        for c in range(chunks):
            normed = rms_norm(hid[c], mlp_gain[0])
            gate_up = jnp.einsum('rd,dcf->rcf', normed, w_gate_up[0], preferred_element_type=F32)
            activated = (jax.nn.silu(gate_up[:, 0]) * gate_up[:, 1]).astype(BF)
            part = jnp.dot(activated, w_down[0], preferred_element_type=F32)
            own = lax.psum_scatter(part, 'tp', scatter_dimension=0, tiled=True)
            rows = own.shape[0]
            own_hid = lax.dynamic_slice_in_dim(hid[c], lax.axis_index('tp') * rows, rows, 0)
            own = (own_hid.astype(F32) + own).astype(BF)
            outs.append(lax.all_gather(own, 'tp', axis=0, tiled=True))
        tokens = outs[0][step:]
        hidden = jnp.concatenate([outs[0][:step]] + outs[1:])

        kv_pair = (qkv[group_q:] * keep_mask)[:, :, None]
        kv_by_pos = lax.all_to_all(kv_pair, 'tp', 1, 2, tiled=True)
        kv_recv = lax.ppermute(kv_by_pos, 'side', send_pairs)
        return (hidden[None], tokens, kv_recv[0][None, None], kv_recv[1][None, None], key_now[None], value_now[None])

    cache_spec = P(None, group_axes, 'tp', None, None)
    in_specs = (P(group_axes, None, None), P(group_axes), P(group_axes, None), P(group_axes), cache_spec, cache_spec, P(), P(None, None, 'tp', None, None), P(None, 'tp', None, None, None), P(), P(None, None, None, 'tp'), P(None, 'tp', None))
    out_specs = (P(group_axes, None, None), P(group_axes, None), cache_spec, cache_spec, cache_spec, cache_spec)
    return jax.shard_map(device_fn, mesh=mesh, in_specs=in_specs, out_specs=out_specs, check_vma=False)
```

```python
import functools

import jax
import jax.numpy as jnp
from jax import lax
from jax.experimental import pallas as pl
from jax.experimental.pallas import tpu as pltpu
from jax.sharding import PartitionSpec as P

ROPE_BASE = 10000.0
NORM_EPS = 1e-5
LOG2E = 1.4426950408889634
BF = jnp.bfloat16
F32 = jnp.float32


def rms_norm(hidden, norm_gain):
    hidden_f32 = hidden.astype(F32)
    inv_rms = lax.rsqrt(jnp.mean(hidden_f32 * hidden_f32, axis=-1, keepdims=True) + NORM_EPS)
    return (hidden_f32 * inv_rms * norm_gain.astype(F32)).astype(BF)


def rope_tables(positions, head_dim):
    half_dim = head_dim // 2
    inv_freq = ROPE_BASE ** (-2.0 * jnp.arange(half_dim, dtype=F32) / head_dim)
    angles = positions.astype(F32)[:, None] * inv_freq[None, :]
    return jnp.cos(angles), jnp.sin(angles)


def rope_rotate(vals_f32, positions):
    half_dim = vals_f32.shape[-1] // 2
    cos_table, sin_table = rope_tables(positions, vals_f32.shape[-1])
    cos_table, sin_table = cos_table[:, None, None, :], sin_table[:, None, None, :]
    first_half = vals_f32[..., :half_dim]
    second_half = vals_f32[..., half_dim:]
    return jnp.concatenate([first_half * cos_table - second_half * sin_table, second_half * cos_table + first_half * sin_table], axis=-1)


def qkv_kernel(x_ref, gain_ref, cos_ref, sin_ref, w_ref, o_ref):
    slots = w_ref.shape[0]
    x = x_ref[...].astype(F32)
    inv = lax.rsqrt(jnp.mean(x * x, axis=-1, keepdims=True) + NORM_EPS)
    normed = (x * inv * gain_ref[...].astype(F32)).astype(BF)
    cos, sin = cos_ref[...], sin_ref[...]
    for first in range(0, slots, 2):
        group = range(first, min(first + 2, slots))
        w = jnp.concatenate([w_ref[s] for s in group], axis=-1)
        y = jnp.dot(normed, w, preferred_element_type=F32)
        for n, s in enumerate(group):
            part = y[:, n * 128:(n + 1) * 128]
            if s < slots - 1:
                part = part * cos + pltpu.roll(part, 64, 1) * sin
            o_ref[s] = part.astype(BF)


def project_qkv(x, gain, cos, sin, w, rows_block=256):
    rows, width = x.shape
    slots, _, head = w.shape
    return pl.pallas_call(
        qkv_kernel,
        grid=(rows // rows_block,),
        in_specs=[
            pl.BlockSpec((rows_block, width), lambda i: (i, 0)),
            pl.BlockSpec((1, width), lambda i: (0, 0)),
            pl.BlockSpec((rows_block, head), lambda i: (i, 0)),
            pl.BlockSpec((rows_block, head), lambda i: (i, 0)),
            pl.BlockSpec((slots, width, head), lambda i: (0, 0, 0), pipeline_mode=pl.Buffered(1)),
        ],
        out_specs=pl.BlockSpec((slots, rows_block, head), lambda i: (0, i, 0)),
        out_shape=jax.ShapeDtypeStruct((slots, rows, head), BF),
        cost_estimate=pl.CostEstimate(flops=2 * rows * width * slots * head, bytes_accessed=2 * (rows * width + slots * head * (width + rows)), transcendentals=0),
        name="project_qkv",
    )(x, gain, cos, sin, w)


def flash_kernel(block_q, block_k, slen_ref, q_ref, k_ref, v_ref, o_ref, m_ref, l_ref, acc_ref):
    i = pl.program_id(0)
    heads, _, head = q_ref.shape
    rows = heads * block_q
    slen = slen_ref[0]
    scale = head ** -0.5 * LOG2E
    q = q_ref[...].reshape(rows, head)
    m_ref[...] = jnp.full_like(m_ref, -jnp.inf)
    l_ref[...] = jnp.zeros_like(l_ref)
    acc_ref[...] = jnp.zeros_like(acc_ref)

    def step(j, masked):
        start = pl.multiple_of(j * block_k, block_k)
        k = k_ref[0, pl.ds(start, block_k), :]
        v = v_ref[0, pl.ds(start, block_k), :]
        s = lax.dot_general(q, k, (((1,), (1,)), ((), ())), preferred_element_type=F32)
        if masked:
            q_pos = i * block_q + lax.broadcasted_iota(jnp.int32, (block_q, block_k), 0)
            k_pos = start + lax.broadcasted_iota(jnp.int32, (block_q, block_k), 1)
            allowed = (k_pos <= q_pos) & (k_pos < slen)
            s = jnp.where(allowed[None], s.reshape(heads, block_q, block_k), -1e30).reshape(rows, block_k)
        m_old = m_ref[...]
        m_new = jnp.maximum(m_old, jnp.max(s, axis=-1, keepdims=True))
        alpha = jnp.exp2((m_old - m_new) * scale)
        p = jnp.exp2((s - m_new) * scale)
        l_ref[...] = l_ref[...] * alpha + jnp.sum(p, axis=-1, keepdims=True)
        acc_ref[...] = acc_ref[...] * alpha + jnp.dot(p.astype(BF), v, preferred_element_type=F32)
        m_ref[...] = m_new

    count = (i * block_q + block_q - 1) // block_k + 1

    @pl.loop(0, count)
    def _(j):
        edge = ((j + 1) * block_k > i * block_q) | ((j + 1) * block_k > slen)

        @pl.when(edge)
        def _():
            step(j, True)

        @pl.when(jnp.logical_not(edge))
        def _():
            step(j, False)

    out = (acc_ref[...] / l_ref[...]).astype(BF)
    for h in range(heads):
        o_ref[:, h * head:(h + 1) * head] = out[h * block_q:(h + 1) * block_q]


def attend(slen, qkv, block_q=256, block_k=512):
    slots, rows, head = qkv.shape
    heads = slots - 2
    return pl.pallas_call(
        functools.partial(flash_kernel, block_q, block_k),
        grid_spec=pltpu.PrefetchScalarGridSpec(
            num_scalar_prefetch=1,
            grid=(rows // block_q,),
            in_specs=[
                pl.BlockSpec((heads, block_q, head), lambda i, _: (0, i, 0)),
                pl.BlockSpec((1, rows, head), lambda i, _: (heads, 0, 0)),
                pl.BlockSpec((1, rows, head), lambda i, _: (heads + 1, 0, 0)),
            ],
            out_specs=pl.BlockSpec((block_q, heads * head), lambda i, _: (i, 0)),
            scratch_shapes=[
                pltpu.VMEM((heads * block_q, 1), F32),
                pltpu.VMEM((heads * block_q, 1), F32),
                pltpu.VMEM((heads * block_q, head), F32),
            ],
        ),
        out_shape=jax.ShapeDtypeStruct((rows, heads * head), BF),
        cost_estimate=pl.CostEstimate(flops=3 * heads * rows * rows * head, bytes_accessed=2 * (2 * heads + 2) * rows * head, transcendentals=heads * rows * rows // 2),
        name="attend",
    )(slen, qkv, qkv, qkv)


MESH = pl.DeviceIdType.MESH
CHUNKS = 4
SUBS = 5
SLOTS = 2
ACCS = 3
TILE = 256
TILE_OUT = 512


def layer_kernel(geo, ctx_hbm, x_hbm, y_hbm, gain_ref, wo_ref, wg_ref, wu_ref, wd_ref, out_hbm, full_hbm, hid_hbm,
                 cx, hid, acc, slot, fin, res, rs_recv, rs_send, credit, ag_recv, ag_send, fin_sem, res_sem,
                 ctx_recv, ctx_send, load_sem, hid_sem):
    width, head_cols, step, dec, ff_tiles, tail = geo
    rows = step + dec
    sub = rows // SUBS
    total = CHUNKS * SUBS
    half = width // 2
    out_tiles = width // TILE_OUT
    ticks = out_tiles + ff_tiles
    stride = ticks // SUBS
    tp = width // head_cols
    last = tp - 1
    c, j = pl.program_id(0), pl.program_id(1)
    t = lax.axis_index('tp')

    def at(cond):
        return pl.when(cond)

    def ctx_copy(chunk, source, right):
        src = full_hbm.at[source, chunk]
        return pltpu.make_async_remote_copy(
            src_ref=src, dst_ref=full_hbm.at[source, chunk], send_sem=ctx_send.at[chunk, source, 0 if right else 1],
            recv_sem=ctx_recv.at[chunk, source], device_id={'tp': t + 1 if right else t - 1}, device_id_type=MESH)

    def ctx_first(chunk):
        def own(right):
            return pltpu.make_async_remote_copy(
                src_ref=ctx_hbm.at[chunk], dst_ref=full_hbm.at[t, chunk], send_sem=ctx_send.at[chunk, t, 0 if right else 1],
                recv_sem=ctx_recv.at[chunk, t], device_id={'tp': t + 1 if right else t - 1}, device_id_type=MESH)

        @at(t < last)
        def _():
            own(True).start()

        @at(t > 0)
        def _():
            own(False).start()

    def ctx_hop(chunk, hop):
        @at(t >= hop)
        def _():
            ctx_copy(chunk, t - hop, True).wait_recv()

            @at(t < last)
            def _():
                ctx_copy(chunk, t - hop, True).start()

        @at(t + hop <= last)
        def _():
            ctx_copy(chunk, t + hop, False).wait_recv()

            @at(t > 0)
            def _():
                ctx_copy(chunk, t + hop, False).start()

    flows = []
    for f in range(2):
        place = last - t if f == 0 else t
        nxt = t - 1 if f == 0 else t + 1
        prv = t + 1 if f == 0 else t - 1
        flows.append((f, place, nxt, prv, f * half))

    def part(k, col):
        first = pl.multiple_of((k % SUBS) * sub, 8)
        return acc.at[(k // SUBS) % ACCS, pl.ds(first, sub), pl.ds(col, half)]

    def out_rows(k, col):
        return out_hbm.at[pl.ds(pl.multiple_of(k * sub, 8), sub), pl.ds(col, half)]

    def rs_copy(f, k, col, device):
        return pltpu.make_async_remote_copy(
            src_ref=part(k, col), dst_ref=slot.at[f, k % SLOTS], send_sem=rs_send.at[f, k % SLOTS],
            recv_sem=rs_recv.at[f, k % SLOTS], device_id={'tp': device}, device_id_type=MESH)

    def ag_copy(f, k, col, device, first):
        return pltpu.make_async_remote_copy(
            src_ref=fin.at[f, k % SLOTS] if first else out_rows(k, col), dst_ref=out_rows(k, col), send_sem=ag_send.at[f, k],
            recv_sem=ag_recv.at[f, k], device_id={'tp': device}, device_id_type=MESH)

    def fin_copy(f, k, col):
        return pltpu.make_async_copy(fin.at[f, k % SLOTS], out_rows(k, col), fin_sem.at[f, k % SLOTS])

    def res_copy(f, k, col):
        rows_k = hid_hbm.at[pl.ds(pl.multiple_of(k * sub, 8), sub), pl.ds(col, half)]
        return pltpu.make_async_copy(rows_k, res.at[f, k % SLOTS], res_sem.at[f, k % SLOTS])

    def collect(m):
        for f, place, nxt, prv, col in flows:
            k = m - place

            @at((k >= 0) & (k < total) & (place > 0))
            def _(f=f, place=place, nxt=nxt, prv=prv, col=col, k=k):
                rs_copy(f, k, col, nxt).wait_recv()
                mine = part(k, col)

                @at(place < last)
                def _():
                    mine[...] += slot[f, k % SLOTS]

                @at(place == last)
                def _():
                    res_copy(f, k, col).wait()

                    @at(k >= SLOTS)
                    def _():
                        fin_copy(f, k, col).wait()
                        ag_copy(f, k - SLOTS, col, prv, True).wait_send()

                    both = mine[...] + slot[f, k % SLOTS]
                    fin[f, k % SLOTS] = (res[f, k % SLOTS].astype(F32) + both).astype(BF)

                @at(k + SLOTS < total)
                def _():
                    pl.semaphore_signal(credit.at[f], inc=1, device_id={'tp': prv}, device_id_type=MESH)

    def send(m):
        for f, place, nxt, prv, col in flows:
            k = m - place

            @at((k >= 0) & (k < total) & (place < last))
            def _(f=f, nxt=nxt, col=col, k=k):
                @at(k >= SLOTS)
                def _():
                    pl.semaphore_wait(credit.at[f], 1)
                    rs_copy(f, k - SLOTS, col, nxt).wait_send()

                rs_copy(f, k, col, nxt).start()

            @at((k >= 0) & (k < total) & (place == last))
            def _(f=f, prv=prv, col=col, k=k):
                fin_copy(f, k, col).start()
                ag_copy(f, k, col, prv, True).start()

            ahead = k + 1

            @at((ahead >= 0) & (ahead < total) & (place == last))
            def _(f=f, col=col, ahead=ahead):
                res_copy(f, ahead, col).start()

            a = m - 2 * last + place

            @at((a >= 0) & (a < total) & (place < last))
            def _(f=f, place=place, prv=prv, col=col, a=a):
                ag_copy(f, a, col, prv, False).wait_recv()

                @at(place > 0)
                def _():
                    ag_copy(f, a, col, prv, False).start()

    @at((c == 0) & (j == 0))
    def _():
        barrier = pltpu.get_barrier_semaphore()

        @at(t > 0)
        def _():
            pl.semaphore_signal(barrier, inc=1, device_id={'tp': t - 1}, device_id_type=MESH)

        @at(t < last)
        def _():
            pl.semaphore_signal(barrier, inc=1, device_id={'tp': t + 1}, device_id_type=MESH)

        @at((t > 0) & (t < last))
        def _():
            pl.semaphore_wait(barrier, 2)

        @at((t == 0) | (t == last))
        def _():
            pl.semaphore_wait(barrier, 1)

        ctx_first(0)
        cx[...] = jnp.zeros_like(cx)
        hid[...] = jnp.zeros_like(hid)
        for hop in range(1, last):
            ctx_hop(0, hop)
        ctx_first(1)
        ctx_hop(0, last)

    for i in range(SUBS):
        @at((c > 0) & (j == stride * i + 1))
        def _(i=i):
            collect(SUBS * (c - 1) + i)

        @at((c > 0) & (j == stride * i + 2))
        def _(i=i):
            send(SUBS * (c - 1) + i)

    for hop in range(1, last + 1):
        @at((c + 1 < CHUNKS) & (j == stride * hop + 3))
        def _(hop=hop):
            ctx_hop(c + 1, hop)
            if hop == last:
                @at(c + 2 < CHUNKS)
                def _():
                    ctx_first(c + 2)

    @at(j == 0)
    def _():
        loads = [
            pltpu.make_async_copy(x_hbm.at[pl.ds(pl.multiple_of(c * step, 8), step)], hid.at[pl.ds(0, step)], load_sem.at[tp]),
            pltpu.make_async_copy(y_hbm.at[pl.ds(pl.multiple_of(c * dec, 8), dec)], hid.at[pl.ds(step, dec)], load_sem.at[tp + 1]),
        ]
        for copy in loads:
            copy.start()
        for s in range(tp):
            where = cx.at[pl.ds(0, rows), pl.ds(s * head_cols, head_cols)]

            @at(t == s)
            def _(s=s, where=where):
                pltpu.make_async_copy(ctx_hbm.at[c], where, load_sem.at[s]).start()

            @at(t != s)
            def _(s=s, where=where):
                pltpu.make_async_copy(full_hbm.at[s, c], where, load_sem.at[s]).start()

        for s in range(tp):
            where = cx.at[pl.ds(0, rows), pl.ds(s * head_cols, head_cols)]
            pltpu.make_async_copy(ctx_hbm.at[c], where, load_sem.at[s]).wait()
        for copy in loads:
            copy.wait()

    @at(j < out_tiles)
    def _():
        heads = head_cols // 128
        mixed = None
        for s in range(tp):
            w = wo_ref[:heads, s].reshape(head_cols, TILE_OUT)
            one = jnp.dot(cx[:, s * head_cols:(s + 1) * head_cols], w, preferred_element_type=F32)
            mixed = one if mixed is None else mixed + one
        cols = pl.ds(pl.multiple_of(j * TILE_OUT, TILE_OUT), TILE_OUT)
        hid[:, cols] = (hid[:, cols].astype(F32) + mixed).astype(BF)

    hid_copy = pltpu.make_async_copy(hid.at[pl.ds(0, rows)], hid_hbm.at[pl.ds(pl.multiple_of(c * rows, 8), rows)], hid_sem)

    @at(j == out_tiles)
    def _():
        hid_copy.start()
        block = hid.shape[0] // 11

        @pl.loop(0, 11)
        def _(b):
            some = pl.ds(pl.multiple_of(b * block, 16), block)
            h = hid[some].astype(F32)
            inv = lax.rsqrt(jnp.mean(h * h, axis=-1, keepdims=True) + NORM_EPS)
            cx[some] = (h * inv * gain_ref[...].astype(F32)).astype(BF)
            acc[c % ACCS, some] = jnp.zeros((block, width), F32)

    @at(j >= out_tiles)
    def _():
        gate = jnp.dot(cx[...], wg_ref[0], preferred_element_type=F32)
        up = jnp.dot(cx[...], wu_ref[0], preferred_element_type=F32)
        act = (jax.nn.silu(gate) * up).astype(BF)
        which = c % ACCS

        @at(j < ticks - 1)
        def _():
            acc[which] += jnp.dot(act, wd_ref[...], preferred_element_type=F32)

        @at(j == ticks - 1)
        def _():
            acc[which] += jnp.dot(act[:, :tail], wd_ref[:tail], preferred_element_type=F32)
            hid_copy.wait()

    @at((c == CHUNKS - 1) & (j == ticks - 1))
    def _():
        @pl.loop(SUBS * (CHUNKS - 1), total + 2 * last)
        def _(m):
            collect(m)
            send(m)

        for f, place, nxt, prv, col in flows:
            @at(place < last)
            def _(f=f, nxt=nxt, col=col):
                for k in range(total - SLOTS, total):
                    rs_copy(f, k, col, nxt).wait_send()

            @at(place == last)
            def _(f=f, prv=prv, col=col):
                for k in range(total - SLOTS, total):
                    fin_copy(f, k, col).wait()
                    ag_copy(f, k, col, prv, True).wait_send()

            @at((place < last) & (place > 0))
            def _(f=f, prv=prv, col=col):
                @pl.loop(0, total)
                def _(k):
                    ag_copy(f, k, col, prv, False).wait_send()

        for source in range(tp):
            @at((source <= t) & (t < last))
            def _(source=source):
                for chunk in range(CHUNKS):
                    ctx_copy(chunk, source, True).wait_send()

            @at((source >= t) & (t > 0))
            def _(source=source):
                for chunk in range(CHUNKS):
                    ctx_copy(chunk, source, False).wait_send()


def layer_sums(ctx, x, y, gain, w_full, w_gate_up, w_down):
    _, rows, head_cols = ctx.shape
    seq, width = x.shape
    step, dec = seq // CHUNKS, y.shape[0] // CHUNKS
    ff = w_down.shape[0]
    ff_tiles = pl.cdiv(ff, TILE)
    tail = ff - (ff_tiles - 1) * TILE
    out_tiles = width // TILE_OUT
    tp = width // head_cols
    pad = (rows + 15) // 16 * 16
    half = width // 2
    sub = rows // SUBS
    total = CHUNKS * SUBS
    geo = (width, head_cols, step, dec, ff_tiles, tail)
    heads = head_cols // 128

    def ff_index(j):
        return jnp.maximum(j - out_tiles, 0)

    any_spec = pl.BlockSpec(memory_space=pl.ANY)
    flops = 2 * CHUNKS * rows * width * (width + 3 * ff)
    moved = 2 * CHUNKS * (width * width + 3 * width * ff)
    return pl.pallas_call(
        functools.partial(layer_kernel, geo),
        grid=(CHUNKS, out_tiles + ff_tiles),
        in_specs=[
            any_spec, any_spec, any_spec,
            pl.BlockSpec((1, width), lambda c, j: (0, 0)),
            pl.BlockSpec((heads, tp, 128, TILE_OUT), lambda c, j: (0, 0, 0, jnp.minimum(j, out_tiles - 1))),
            pl.BlockSpec((1, width, TILE), lambda c, j: (0, 0, ff_index(j))),
            pl.BlockSpec((1, width, TILE), lambda c, j: (1, 0, ff_index(j))),
            pl.BlockSpec((TILE, width), lambda c, j: (ff_index(j), 0)),
        ],
        out_specs=[any_spec, any_spec, any_spec],
        out_shape=[
            jax.ShapeDtypeStruct((CHUNKS * rows, width), BF),
            jax.ShapeDtypeStruct((tp, CHUNKS, rows, head_cols), BF),
            jax.ShapeDtypeStruct((CHUNKS * rows, width), BF),
        ],
        scratch_shapes=[
            pltpu.VMEM((pad, width), BF),
            pltpu.VMEM((pad, width), BF),
            pltpu.VMEM((ACCS, pad, width), F32),
            pltpu.VMEM((2, SLOTS, sub, half), F32),
            pltpu.VMEM((2, SLOTS, sub, half), BF),
            pltpu.VMEM((2, SLOTS, sub, half), BF),
            pltpu.SemaphoreType.DMA((2, SLOTS)),
            pltpu.SemaphoreType.DMA((2, SLOTS)),
            pltpu.SemaphoreType.REGULAR((2,)),
            pltpu.SemaphoreType.DMA((2, total)),
            pltpu.SemaphoreType.DMA((2, total)),
            pltpu.SemaphoreType.DMA((2, SLOTS)),
            pltpu.SemaphoreType.DMA((2, SLOTS)),
            pltpu.SemaphoreType.DMA((CHUNKS, tp)),
            pltpu.SemaphoreType.DMA((CHUNKS, tp, 2)),
            pltpu.SemaphoreType.DMA((tp + 2,)),
            pltpu.SemaphoreType.DMA(()),
        ],
        compiler_params=pltpu.CompilerParams(collective_id=0, has_side_effects=True, vmem_limit_bytes=67000000, dimension_semantics=('arbitrary', 'arbitrary')),
        cost_estimate=pl.CostEstimate(flops=flops, bytes_accessed=moved, transcendentals=0),
        name='layer_sums',
    )(ctx, x, y, gain, w_full, w_gate_up, w_gate_up, w_down)[0]


def decode_context(tokens, cache_lens, k_cache, v_cache, gain, w_qkv):
    group_q = w_qkv.shape[2] - 2
    head_dim = w_qkv.shape[3]
    cache_local = k_cache.shape[1]
    cache_pos = lax.axis_index('tp') * cache_local + jnp.arange(cache_local)
    write_mask = (cache_pos[None, :] == cache_lens[:, None])[:, :, None, None]
    allowed = (cache_pos[None, :] <= cache_lens[:, None])[:, None, None, :]
    normed = rms_norm(tokens, gain)
    projected = jnp.einsum('bd,dkjh->bkjh', normed, w_qkv, preferred_element_type=F32)
    rotated = rope_rotate(projected[:, :, :group_q + 1], cache_lens)
    local_qkv = jnp.concatenate([rotated, projected[:, :, group_q + 1:]], axis=2).astype(BF)
    full_qkv = lax.all_gather(local_qkv, 'tp', axis=1, tiled=True)
    key_now = jnp.where(write_mask, full_qkv[:, None, :, group_q], k_cache)
    value_now = jnp.where(write_mask, full_qkv[:, None, :, group_q + 1], v_cache)
    scores = jnp.einsum('bkgh,btkh->bkgt', full_qkv[:, :, :group_q], key_now, preferred_element_type=F32) * head_dim ** -0.5
    scores = jnp.where(allowed, scores, -1e30)
    score_max = lax.pmax(jnp.max(scores, axis=-1, keepdims=True), 'tp')
    weights = jnp.exp(scores - score_max)
    sum_own = lax.psum_scatter(jnp.sum(weights, axis=-1), 'tp', scatter_dimension=1, tiled=True)
    mixed_sum = jnp.einsum('bkgt,btkh->bkgh', weights.astype(BF), value_now, preferred_element_type=F32)
    mixed_own = lax.psum_scatter(mixed_sum, 'tp', scatter_dimension=1, tiled=True)
    context = (mixed_own / sum_own[..., None]).astype(BF)
    return context, key_now, value_now


def gather_w_out(w_out, mesh):
    index = lax.axis_index('pair') * mesh.shape['side'] + lax.axis_index('side')
    own = lax.dynamic_index_in_dim(w_out, jnp.minimum(index, w_out.shape[0] - 1), 0, keepdims=False)
    column = lax.all_gather(own, 'tp')
    return lax.all_gather(column, ('pair', 'side'))


def solution(mesh):
    side_size = mesh.shape['side']
    tp = mesh.shape['tp']
    send_pairs = [(source, (source + 1) % side_size) for source in range(side_size)]
    group_axes = ('pair', 'side')

    def device_fn(x_prompt, s_len, y_tok, c_len, k_cache, v_cache, attn_gain, w_qkv, w_out, mlp_gain, w_gate_up, w_down):
        x = x_prompt[0]
        seq_len, width = x.shape
        group_q, head = w_qkv.shape[3] - 2, w_qkv.shape[4]
        positions = jnp.arange(seq_len)
        keep_mask = (positions < s_len[0])[:, None].astype(BF)
        cos, sin = rope_tables(positions, head)
        cos, sin = jnp.concatenate([cos, cos], -1), jnp.concatenate([-sin, sin], -1)

        w_full = gather_w_out(w_out[0, 0], mesh)
        gate_up = jnp.transpose(w_gate_up[0], (1, 0, 2))

        dctx, key_now, value_now = decode_context(y_tok, c_len, k_cache[0], v_cache[0], attn_gain[0], w_qkv[0])
        dctx = dctx.reshape(dctx.shape[0], group_q * head)

        w_slots = jnp.transpose(w_qkv[0, :, 0], (1, 0, 2))
        qkv = project_qkv(x, attn_gain, cos, sin, w_slots)
        ctx = attend(s_len, qkv)

        step, dec = seq_len // CHUNKS, y_tok.shape[0] // CHUNKS
        ctx_all = jnp.concatenate([ctx.reshape(CHUNKS, step, -1), dctx.reshape(CHUNKS, dec, -1)], axis=1)
        done = layer_sums(ctx_all, x, y_tok, mlp_gain, w_full, gate_up, w_down[0])
        done = done.reshape(CHUNKS, step + dec, width)
        hidden = done[:, :step].reshape(seq_len, width)
        tokens = done[:, step:].reshape(CHUNKS * dec, width)

        kv_pair = (qkv[group_q:] * keep_mask)[:, :, None]
        kv_by_pos = lax.all_to_all(kv_pair, 'tp', 1, 2, tiled=True)
        kv_recv = lax.ppermute(kv_by_pos, 'side', send_pairs)
        return (hidden[None], tokens, kv_recv[0][None, None], kv_recv[1][None, None], key_now[None], value_now[None])

    cache_spec = P(None, group_axes, 'tp', None, None)
    in_specs = (P(group_axes, None, None), P(group_axes), P(group_axes, None), P(group_axes), cache_spec, cache_spec, P(), P(None, None, 'tp', None, None), P(None, 'tp', None, None, None), P(), P(None, None, None, 'tp'), P(None, 'tp', None))
    out_specs = (P(group_axes, None, None), P(group_axes, None), cache_spec, cache_spec, cache_spec, cache_spec)
    return jax.shard_map(device_fn, mesh=mesh, in_specs=in_specs, out_specs=out_specs, check_vma=False)
```

```python
import functools

import jax
import jax.numpy as jnp
from jax import lax
from jax.experimental import pallas as pl
from jax.experimental.pallas import tpu as pltpu
from jax.sharding import PartitionSpec as P

ROPE_BASE = 10000.0
NORM_EPS = 1e-5
LOG2E = 1.4426950408889634
BF = jnp.bfloat16
F32 = jnp.float32


def rms_norm(hidden, norm_gain):
    hidden_f32 = hidden.astype(F32)
    inv_rms = lax.rsqrt(jnp.mean(hidden_f32 * hidden_f32, axis=-1, keepdims=True) + NORM_EPS)
    return (hidden_f32 * inv_rms * norm_gain.astype(F32)).astype(BF)


def rope_tables(positions, head_dim):
    half_dim = head_dim // 2
    inv_freq = ROPE_BASE ** (-2.0 * jnp.arange(half_dim, dtype=F32) / head_dim)
    angles = positions.astype(F32)[:, None] * inv_freq[None, :]
    return jnp.cos(angles), jnp.sin(angles)


def rope_rotate(vals_f32, positions):
    half_dim = vals_f32.shape[-1] // 2
    cos_table, sin_table = rope_tables(positions, vals_f32.shape[-1])
    cos_table, sin_table = cos_table[:, None, None, :], sin_table[:, None, None, :]
    first_half = vals_f32[..., :half_dim]
    second_half = vals_f32[..., half_dim:]
    return jnp.concatenate([first_half * cos_table - second_half * sin_table, second_half * cos_table + first_half * sin_table], axis=-1)


def qkv_kernel(x_ref, gain_ref, cos_ref, sin_ref, w_ref, o_ref):
    slots = w_ref.shape[0]
    x = x_ref[...].astype(F32)
    inv = lax.rsqrt(jnp.mean(x * x, axis=-1, keepdims=True) + NORM_EPS)
    normed = (x * inv * gain_ref[...].astype(F32)).astype(BF)
    cos, sin = cos_ref[...], sin_ref[...]
    for first in range(0, slots, 2):
        group = range(first, min(first + 2, slots))
        w = jnp.concatenate([w_ref[s] for s in group], axis=-1)
        y = jnp.dot(normed, w, preferred_element_type=F32)
        for n, s in enumerate(group):
            part = y[:, n * 128:(n + 1) * 128]
            if s < slots - 1:
                part = part * cos + pltpu.roll(part, 64, 1) * sin
            o_ref[s] = part.astype(BF)


def project_qkv(x, gain, cos, sin, w, rows_block=256):
    rows, width = x.shape
    slots, _, head = w.shape
    return pl.pallas_call(
        qkv_kernel,
        grid=(rows // rows_block,),
        in_specs=[
            pl.BlockSpec((rows_block, width), lambda i: (i, 0)),
            pl.BlockSpec((1, width), lambda i: (0, 0)),
            pl.BlockSpec((rows_block, head), lambda i: (i, 0)),
            pl.BlockSpec((rows_block, head), lambda i: (i, 0)),
            pl.BlockSpec((slots, width, head), lambda i: (0, 0, 0), pipeline_mode=pl.Buffered(1)),
        ],
        out_specs=pl.BlockSpec((slots, rows_block, head), lambda i: (0, i, 0)),
        out_shape=jax.ShapeDtypeStruct((slots, rows, head), BF),
        cost_estimate=pl.CostEstimate(flops=2 * rows * width * slots * head, bytes_accessed=2 * (rows * width + slots * head * (width + rows)), transcendentals=0),
        name="project_qkv",
    )(x, gain, cos, sin, w)


def flash_kernel(block_q, block_k, some, slen_ref, q_ref, k_ref, v_ref, o_ref, s_ref, m_ref, l_ref, p_ref, acc_ref):
    i = pl.program_id(0)
    heads, _, head = q_ref.shape
    rows = heads * block_q
    pieces = rows // some
    lanes = block_k // 128
    slen = slen_ref[0]
    scale = head ** -0.5 * LOG2E
    count = (i * block_q + block_q - 1) // block_k + 1

    def cols(j):
        return pl.ds(pl.multiple_of(j * block_k, block_k), block_k)

    @pl.loop(0, count)
    def _(j):
        k = k_ref[0, cols(j), :]
        s_ref[:, cols(j)] = lax.dot_general(q_ref[...].reshape(rows, head), k, (((1,), (1,)), ((), ())), preferred_element_type=F32)
        edge = ((j + 1) * block_k > i * block_q) | ((j + 1) * block_k > slen)

        @pl.when(edge)
        def _():
            @pl.loop(0, pieces)
            def _(r):
                here = pl.ds(pl.multiple_of(r * some, some), some)
                q_pos = i * block_q + (r * some) % block_q + lax.broadcasted_iota(jnp.int32, (some, block_k), 0)
                k_pos = j * block_k + lax.broadcasted_iota(jnp.int32, (some, block_k), 1)
                s_ref[here, cols(j)] = jnp.where((k_pos <= q_pos) & (k_pos < slen), s_ref[here, cols(j)], -1e30)

    tall = rows // heads

    @pl.loop(0, heads)
    def _(r):
        here = pl.ds(pl.multiple_of(r * tall, tall), tall)

        def more(j, top):
            s = s_ref[here, cols(j)]
            for n in range(lanes):
                top = jnp.maximum(top, s[:, n * 128:(n + 1) * 128])
            return top

        top = lax.fori_loop(0, count, more, jnp.full((tall, 128), -jnp.inf, F32))
        m_ref[here] = jnp.broadcast_to(jnp.max(top, axis=-1, keepdims=True), (tall, 128))

    l_ref[...] = jnp.zeros_like(l_ref)
    acc_ref[...] = jnp.zeros_like(acc_ref)

    @pl.loop(0, count)
    def _(j):
        @pl.loop(0, pieces, unroll=2)
        def _(r):
            here = pl.ds(pl.multiple_of(r * some, some), some)
            s = s_ref[here, cols(j)]
            m = m_ref[here]
            total = l_ref[here]
            for n in range(lanes):
                w = jnp.exp2((s[:, n * 128:(n + 1) * 128] - m) * scale)
                total = total + w
                p_ref[here, n * 128:(n + 1) * 128] = w.astype(BF)
            l_ref[here] = total

        acc_ref[...] += jnp.dot(p_ref[...], v_ref[0, cols(j), :], preferred_element_type=F32)

    for h in range(heads):
        here = slice(h * block_q, (h + 1) * block_q)
        o_ref[:, h * head:(h + 1) * head] = (acc_ref[here] / jnp.sum(l_ref[here], axis=-1, keepdims=True)).astype(BF)


def attend(slen, qkv, block_q=256, block_k=512, some=32):
    slots, rows, head = qkv.shape
    heads = slots - 2
    tall = heads * block_q
    return pl.pallas_call(
        functools.partial(flash_kernel, block_q, block_k, some),
        grid_spec=pltpu.PrefetchScalarGridSpec(
            num_scalar_prefetch=1,
            grid=(rows // block_q,),
            in_specs=[
                pl.BlockSpec((heads, block_q, head), lambda i, _: (0, i, 0)),
                pl.BlockSpec((1, rows, head), lambda i, _: (heads, 0, 0)),
                pl.BlockSpec((1, rows, head), lambda i, _: (heads + 1, 0, 0)),
            ],
            out_specs=pl.BlockSpec((block_q, heads * head), lambda i, _: (i, 0)),
            scratch_shapes=[
                pltpu.VMEM((tall, rows), F32),
                pltpu.VMEM((tall, 128), F32),
                pltpu.VMEM((tall, 128), F32),
                pltpu.VMEM((tall, block_k), BF),
                pltpu.VMEM((tall, head), F32),
            ],
        ),
        out_shape=jax.ShapeDtypeStruct((rows, heads * head), BF),
        cost_estimate=pl.CostEstimate(flops=3 * heads * rows * rows * head, bytes_accessed=2 * (2 * heads + 2) * rows * head, transcendentals=heads * rows * rows // 2),
        name='attend',
    )(slen, qkv, qkv, qkv)


MESH = pl.DeviceIdType.MESH
CHUNKS = 4
SUBS = 13
SLOTS = 2
ACCS = 3
TILE = 256
TILE_OUT = 512
OWNED = (10, 4, 4, 10)


def layer_kernel(geo, ctx_hbm, x_hbm, y_hbm, gain_ref, wo_ref, wg_ref, wu_ref, wd_ref, out_hbm, full_hbm, hid_hbm,
                 cx, hid, acc, slots, fins, ress, rs_recv, rs_send, credit, ag_recv, ag_send, fin_sem, res_sem,
                 ctx_recv, ctx_send, load_sem, hid_sem):
    width, head_cols, step, dec, ff_tiles, tail = geo
    rows = step + dec
    sub = rows // SUBS
    total = CHUNKS * SUBS
    out_tiles = width // TILE_OUT
    ticks = out_tiles + ff_tiles
    stride = ticks // SUBS
    tp = width // head_cols
    last = tp - 1
    c, j = pl.program_id(0), pl.program_id(1)
    t = lax.axis_index('tp')

    def at(cond):
        return pl.when(cond)

    def ctx_copy(chunk, source, right):
        src = full_hbm.at[source, chunk]
        return pltpu.make_async_remote_copy(
            src_ref=src, dst_ref=full_hbm.at[source, chunk], send_sem=ctx_send.at[chunk, source, 0 if right else 1],
            recv_sem=ctx_recv.at[chunk, source], device_id={'tp': t + 1 if right else t - 1}, device_id_type=MESH)

    def ctx_first(chunk):
        def own(right):
            return pltpu.make_async_remote_copy(
                src_ref=ctx_hbm.at[chunk], dst_ref=full_hbm.at[t, chunk], send_sem=ctx_send.at[chunk, t, 0 if right else 1],
                recv_sem=ctx_recv.at[chunk, t], device_id={'tp': t + 1 if right else t - 1}, device_id_type=MESH)

        @at(t < last)
        def _():
            own(True).start()

        @at(t > 0)
        def _():
            own(False).start()

    def ctx_hop(chunk, hop):
        @at(t >= hop)
        def _():
            ctx_copy(chunk, t - hop, True).wait_recv()

            @at(t < last)
            def _():
                ctx_copy(chunk, t - hop, True).start()

        @at(t + hop <= last)
        def _():
            ctx_copy(chunk, t + hop, False).wait_recv()

            @at(t > 0)
            def _():
                ctx_copy(chunk, t + hop, False).start()

    flows = []
    for f, groups in enumerate(OWNED):
        flows.append((f, sum(OWNED[:f]) * 128, groups * 128, max(f, last - f)))

    def to(device):
        return dict(device_id={'tp': device}, device_id_type=MESH)

    def rows_of(k):
        return pl.ds(pl.multiple_of(k * sub, 8), sub)

    def part(f, k):
        _, col, cols, _ = flows[f]
        first = pl.multiple_of((k % SUBS) * sub, 8)
        return acc.at[(k // SUBS) % ACCS, pl.ds(first, sub), pl.ds(col, cols)]

    def out_part(f, k):
        _, col, cols, _ = flows[f]
        return out_hbm.at[rows_of(k), pl.ds(col, cols)]

    def rs_copy(f, k, side, device):
        return pltpu.make_async_remote_copy(
            src_ref=part(f, k), dst_ref=slots[f].at[side, k % SLOTS], send_sem=rs_send.at[f, k % SLOTS],
            recv_sem=rs_recv.at[f, side, k % SLOTS], **to(device))

    def ag_copy(f, k, way, first):
        return pltpu.make_async_remote_copy(
            src_ref=fins[f].at[k % SLOTS] if first else out_part(f, k), dst_ref=out_part(f, k), send_sem=ag_send.at[f, way, k % SLOTS],
            recv_sem=ag_recv.at[f, k], **to(t + 1 if way == 0 else t - 1))

    def fin_copy(f, k):
        return pltpu.make_async_copy(fins[f].at[k % SLOTS], out_part(f, k), fin_sem.at[f, k % SLOTS])

    def res_copy(f, k):
        _, col, cols, _ = flows[f]
        return pltpu.make_async_copy(hid_hbm.at[rows_of(k), pl.ds(col, cols)], ress[f].at[k % SLOTS], res_sem.at[f, k % SLOTS])

    def sides(f):
        found = []
        if f < last:
            found.append((0, t > f, t - f, t + 1, t - 1, t < last))
        if f > 0:
            found.append((1, t < f, f - t, t - 1, t + 1, t > 0))
        return found

    def inside(k):
        return (k >= 0) & (k < total)

    def collect(m):
        for f, col, cols, peak in flows:
            for side, there, dist, outer, inner, more in sides(f):
                k = m - peak + dist

                @at(inside(k) & there & more)
                def _(f=f, side=side, outer=outer, inner=inner, k=k):
                    rs_copy(f, k, side, inner).wait_recv()
                    mine = part(f, k)
                    mine[...] += slots[f][side, k % SLOTS]

                    @at(k + SLOTS < total)
                    def _():
                        pl.semaphore_signal(credit.at[f], inc=1, **to(outer))

            k = m - peak

            @at(inside(k) & (t == f))
            def _(f=f, k=k):
                both = part(f, k)[...]
                for side, _, _, outer, inner, _ in sides(f):
                    rs_copy(f, k, side, inner).wait_recv()
                    both = both + slots[f][side, k % SLOTS]
                res_copy(f, k).wait()

                @at(k >= SLOTS)
                def _():
                    fin_copy(f, k - SLOTS).wait()
                    for side, _, _, _, _, _ in sides(f):
                        ag_copy(f, k - SLOTS, side, True).wait_send()

                fins[f][k % SLOTS] = (ress[f][k % SLOTS].astype(F32) + both).astype(BF)

                @at(k + SLOTS < total)
                def _():
                    for side, _, _, outer, _, _ in sides(f):
                        pl.semaphore_signal(credit.at[f], inc=1, **to(outer))

    def send(m):
        for f, col, cols, peak in flows:
            for side, there, dist, outer, inner, more in sides(f):
                k = m - peak + dist

                @at(inside(k) & there)
                def _(f=f, side=side, inner=inner, k=k):
                    @at(k >= SLOTS)
                    def _():
                        pl.semaphore_wait(credit.at[f], 1)
                        rs_copy(f, k - SLOTS, side, inner).wait_send()

                    rs_copy(f, k, side, inner).start()

            k = m - peak

            @at(inside(k) & (t == f))
            def _(f=f, k=k):
                fin_copy(f, k).start()
                for side, _, _, _, _, _ in sides(f):
                    ag_copy(f, k, side, True).start()

            @at(inside(k + 1) & (t == f))
            def _(f=f, k=k):
                res_copy(f, k + 1).start()

            for side, there, dist, outer, inner, more in sides(f):
                a = m - peak - dist

                @at(inside(a) & there)
                def _(f=f, side=side, more=more, a=a):
                    ag_copy(f, a, side, False).wait_recv()

                    @at(more)
                    def _():
                        @at(a >= SLOTS)
                        def _():
                            ag_copy(f, a - SLOTS, side, False).wait_send()

                        ag_copy(f, a, side, False).start()

    @at((c == 0) & (j == 0))
    def _():
        barrier = pltpu.get_barrier_semaphore()

        @at(t > 0)
        def _():
            pl.semaphore_signal(barrier, inc=1, device_id={'tp': t - 1}, device_id_type=MESH)

        @at(t < last)
        def _():
            pl.semaphore_signal(barrier, inc=1, device_id={'tp': t + 1}, device_id_type=MESH)

        @at((t > 0) & (t < last))
        def _():
            pl.semaphore_wait(barrier, 2)

        @at((t == 0) | (t == last))
        def _():
            pl.semaphore_wait(barrier, 1)

        ctx_first(0)
        cx[...] = jnp.zeros_like(cx)
        hid[...] = jnp.zeros_like(hid)
        for hop in range(1, last):
            ctx_hop(0, hop)
        ctx_first(1)
        ctx_hop(0, last)

    @at((c > 0) & (j % stride == 0) & (j < stride * SUBS))
    def _():
        collect(SUBS * (c - 1) + j // stride)

    @at((c > 0) & (j % stride == 1) & (j < stride * SUBS))
    def _():
        send(SUBS * (c - 1) + j // stride)

    for hop in range(1, last + 1):
        @at((c + 1 < CHUNKS) & (j == ticks * hop // (last + 1) + 2))
        def _(hop=hop):
            ctx_hop(c + 1, hop)
            if hop == last:
                @at(c + 2 < CHUNKS)
                def _():
                    ctx_first(c + 2)

    @at(j == 0)
    def _():
        loads = [
            pltpu.make_async_copy(x_hbm.at[pl.ds(pl.multiple_of(c * step, 8), step)], hid.at[pl.ds(0, step)], load_sem.at[tp]),
            pltpu.make_async_copy(y_hbm.at[pl.ds(pl.multiple_of(c * dec, 8), dec)], hid.at[pl.ds(step, dec)], load_sem.at[tp + 1]),
        ]
        for copy in loads:
            copy.start()
        for s in range(tp):
            where = cx.at[pl.ds(0, rows), pl.ds(s * head_cols, head_cols)]

            @at(t == s)
            def _(s=s, where=where):
                pltpu.make_async_copy(ctx_hbm.at[c], where, load_sem.at[s]).start()

            @at(t != s)
            def _(s=s, where=where):
                pltpu.make_async_copy(full_hbm.at[s, c], where, load_sem.at[s]).start()

        for s in range(tp):
            where = cx.at[pl.ds(0, rows), pl.ds(s * head_cols, head_cols)]
            pltpu.make_async_copy(ctx_hbm.at[c], where, load_sem.at[s]).wait()
        for copy in loads:
            copy.wait()

    @at(j < out_tiles)
    def _():
        heads = head_cols // 128
        mixed = None
        for s in range(tp):
            w = wo_ref[s].reshape(head_cols, TILE_OUT)
            one = jnp.dot(cx[:, s * head_cols:(s + 1) * head_cols], w, preferred_element_type=F32)
            mixed = one if mixed is None else mixed + one
        cols = pl.ds(pl.multiple_of(j * TILE_OUT, TILE_OUT), TILE_OUT)
        hid[:, cols] = (hid[:, cols].astype(F32) + mixed).astype(BF)

    hid_copy = pltpu.make_async_copy(hid.at[pl.ds(0, rows)], hid_hbm.at[pl.ds(pl.multiple_of(c * rows, 8), rows)], hid_sem)

    @at(j == out_tiles)
    def _():
        hid_copy.start()
        block = hid.shape[0] // 11

        @pl.loop(0, 11)
        def _(b):
            some = pl.ds(pl.multiple_of(b * block, 16), block)
            h = hid[some].astype(F32)
            inv = lax.rsqrt(jnp.mean(h * h, axis=-1, keepdims=True) + NORM_EPS)
            cx[some] = (h * inv * gain_ref[...].astype(F32)).astype(BF)
            acc[c % ACCS, some] = jnp.zeros((block, width), F32)

    @at(j >= out_tiles)
    def _():
        gate = jnp.dot(cx[...], wg_ref[0], preferred_element_type=F32)
        up = jnp.dot(cx[...], wu_ref[0], preferred_element_type=F32)
        act = (jax.nn.silu(gate) * up).astype(BF)
        which = c % ACCS

        @at(j < ticks - 1)
        def _():
            acc[which] += jnp.dot(act, wd_ref[...], preferred_element_type=F32)

        @at(j == ticks - 1)
        def _():
            acc[which] += jnp.dot(act[:, :tail], wd_ref[:tail], preferred_element_type=F32)
            hid_copy.wait()

    @at((c == CHUNKS - 1) & (j == ticks - 1))
    def _():
        @pl.loop(SUBS * (CHUNKS - 1), total + 2 * last)
        def _(m):
            collect(m)
            send(m)

        for f, col, cols, peak in flows:
            for side, there, dist, outer, inner, more in sides(f):
                @at(there)
                def _(f=f, side=side, inner=inner, more=more):
                    for k in range(total - SLOTS, total):
                        rs_copy(f, k, side, inner).wait_send()

                    @at(more)
                    def _():
                        for k in range(total - SLOTS, total):
                            ag_copy(f, k, side, False).wait_send()

            @at(t == f)
            def _(f=f):
                for k in range(total - SLOTS, total):
                    fin_copy(f, k).wait()
                    for side, _, _, _, _, _ in sides(f):
                        ag_copy(f, k, side, True).wait_send()

        for source in range(tp):
            @at((source <= t) & (t < last))
            def _(source=source):
                for chunk in range(CHUNKS):
                    ctx_copy(chunk, source, True).wait_send()

            @at((source >= t) & (t > 0))
            def _(source=source):
                for chunk in range(CHUNKS):
                    ctx_copy(chunk, source, False).wait_send()


def layer_sums(ctx, x, y, gain, w_full, w_gate_up, w_down):
    _, rows, head_cols = ctx.shape
    seq, width = x.shape
    step, dec = seq // CHUNKS, y.shape[0] // CHUNKS
    ff = w_down.shape[0]
    ff_tiles = pl.cdiv(ff, TILE)
    tail = ff - (ff_tiles - 1) * TILE
    out_tiles = width // TILE_OUT
    tp = width // head_cols
    pad = (rows + 15) // 16 * 16
    sub = rows // SUBS
    total = CHUNKS * SUBS
    geo = (width, head_cols, step, dec, ff_tiles, tail)
    heads = head_cols // 128

    def ff_index(j):
        return jnp.maximum(j - out_tiles, 0)

    any_spec = pl.BlockSpec(memory_space=pl.ANY)
    flops = 2 * CHUNKS * rows * width * (width + 3 * ff)
    moved = 2 * CHUNKS * (width * width + 3 * width * ff)
    return pl.pallas_call(
        functools.partial(layer_kernel, geo),
        grid=(CHUNKS, out_tiles + ff_tiles),
        in_specs=[
            any_spec, any_spec, any_spec,
            pl.BlockSpec((1, width), lambda c, j: (0, 0)),
            pl.BlockSpec((tp, heads, 128, TILE_OUT), lambda c, j: (0, 0, 0, jnp.minimum(j, out_tiles - 1))),
            pl.BlockSpec((1, width, TILE), lambda c, j: (0, 0, ff_index(j))),
            pl.BlockSpec((1, width, TILE), lambda c, j: (1, 0, ff_index(j))),
            pl.BlockSpec((TILE, width), lambda c, j: (ff_index(j), 0)),
        ],
        out_specs=[any_spec, any_spec, any_spec],
        out_shape=[
            jax.ShapeDtypeStruct((CHUNKS * rows, width), BF),
            jax.ShapeDtypeStruct((tp, CHUNKS, rows, head_cols), BF),
            jax.ShapeDtypeStruct((CHUNKS * rows, width), BF),
        ],
        scratch_shapes=[
            pltpu.VMEM((pad, width), BF),
            pltpu.VMEM((pad, width), BF),
            pltpu.VMEM((ACCS, pad, width), F32),
            [pltpu.VMEM((2, SLOTS, sub, groups * 128), F32) for groups in OWNED],
            [pltpu.VMEM((SLOTS, sub, groups * 128), BF) for groups in OWNED],
            [pltpu.VMEM((SLOTS, sub, groups * 128), BF) for groups in OWNED],
            pltpu.SemaphoreType.DMA((tp, 2, SLOTS)),
            pltpu.SemaphoreType.DMA((tp, SLOTS)),
            pltpu.SemaphoreType.REGULAR((tp,)),
            pltpu.SemaphoreType.DMA((tp, total)),
            pltpu.SemaphoreType.DMA((tp, 2, SLOTS)),
            pltpu.SemaphoreType.DMA((tp, SLOTS)),
            pltpu.SemaphoreType.DMA((tp, SLOTS)),
            pltpu.SemaphoreType.DMA((CHUNKS, tp)),
            pltpu.SemaphoreType.DMA((CHUNKS, tp, 2)),
            pltpu.SemaphoreType.DMA((tp + 2,)),
            pltpu.SemaphoreType.DMA(()),
        ],
        compiler_params=pltpu.CompilerParams(collective_id=0, has_side_effects=True, vmem_limit_bytes=67000000, dimension_semantics=('arbitrary', 'arbitrary')),
        cost_estimate=pl.CostEstimate(flops=flops, bytes_accessed=moved, transcendentals=0),
        name='layer_sums',
    )(ctx, x, y, gain, w_full, w_gate_up, w_gate_up, w_down)[0]


def decode_local(tokens, cache_lens, k_cache, v_cache, gain, w_qkv):
    group_q = w_qkv.shape[2] - 2
    head_dim = w_qkv.shape[3]
    cache_local = k_cache.shape[1]
    cache_pos = lax.axis_index('tp') * cache_local + jnp.arange(cache_local)
    write_mask = (cache_pos[None, :] == cache_lens[:, None])[:, :, None, None]
    allowed = (cache_pos[None, :] <= cache_lens[:, None])[None, :, None, :]
    normed = rms_norm(tokens, gain)
    projected = jnp.einsum('bd,dkjh->bkjh', normed, w_qkv, preferred_element_type=F32)
    rotated = rope_rotate(projected[:, :, :group_q + 1], cache_lens)
    local_qkv = jnp.concatenate([rotated, projected[:, :, group_q + 1:]], axis=2).astype(BF)[:, 0]
    tp = k_cache.shape[2]
    full_qkv = lax.all_to_all(jnp.broadcast_to(local_qkv, (tp,) + local_qkv.shape), 'tp', 0, 0)
    key_now = jnp.where(write_mask, jnp.moveaxis(full_qkv[:, :, group_q], 0, 1)[:, None], k_cache)
    value_now = jnp.where(write_mask, jnp.moveaxis(full_qkv[:, :, group_q + 1], 0, 1)[:, None], v_cache)
    scores = jnp.einsum('kbgh,btkh->kbgt', full_qkv[:, :, :group_q], key_now, preferred_element_type=F32) * head_dim ** -0.5
    scores = jnp.where(allowed, scores, -1e30)
    top = jnp.max(scores, axis=-1)
    weights = jnp.exp(scores - top[..., None])
    mixed = jnp.einsum('kbgt,btkh->kbgh', weights.astype(BF), value_now, preferred_element_type=F32)
    stats = jnp.concatenate([top, jnp.sum(weights, axis=-1)], axis=-1)
    stats = jnp.pad(stats, ((0, 0), (0, 0), (0, head_dim - stats.shape[-1])))
    return jnp.concatenate([mixed, stats[:, :, None]], axis=2), key_now, value_now


def decode_combine(mixed):
    heads = mixed.shape[2] - 1
    own = lax.all_to_all(mixed, 'tp', 0, 0)
    top, total = own[:, :, heads, :heads], own[:, :, heads, heads:2 * heads]
    factor = jnp.exp(top - jnp.max(top, axis=0))
    return (jnp.sum(own[:, :, :heads] * factor[..., None], axis=0) / jnp.sum(total * factor, axis=0)[..., None]).astype(BF)


def gather_w_out(w_out, mesh):
    index = lax.axis_index('pair') * mesh.shape['side'] + lax.axis_index('side')
    own = lax.dynamic_index_in_dim(w_out, jnp.minimum(index, w_out.shape[0] - 1), 0, keepdims=False)
    return lax.all_gather(own, ('tp', 'pair', 'side'))


def solution(mesh):
    side_size = mesh.shape['side']
    tp = mesh.shape['tp']
    send_pairs = [(source, (source + 1) % side_size) for source in range(side_size)]
    group_axes = ('pair', 'side')

    def device_fn(x_prompt, s_len, y_tok, c_len, k_cache, v_cache, attn_gain, w_qkv, w_out, mlp_gain, w_gate_up, w_down):
        x = x_prompt[0]
        seq_len, width = x.shape
        group_q, head = w_qkv.shape[3] - 2, w_qkv.shape[4]
        positions = jnp.arange(seq_len)
        keep_mask = (positions < s_len[0])[:, None].astype(BF)
        cos, sin = rope_tables(positions, head)
        cos, sin = jnp.concatenate([cos, cos], -1), jnp.concatenate([-sin, sin], -1)

        w_full = gather_w_out(w_out[0, 0], mesh).reshape(tp, -1, head, width)
        gate_up = jnp.transpose(w_gate_up[0], (1, 0, 2))

        mixed, key_now, value_now = decode_local(y_tok, c_len, k_cache[0], v_cache[0], attn_gain[0], w_qkv[0])

        w_slots = jnp.transpose(w_qkv[0, :, 0], (1, 0, 2))
        qkv = project_qkv(x, attn_gain, cos, sin, w_slots)
        mixed, qkv = lax.optimization_barrier((mixed, qkv))
        dctx = decode_combine(mixed)
        ctx = attend(s_len, qkv)

        step, dec = seq_len // CHUNKS, y_tok.shape[0] // CHUNKS
        ctx_all = jnp.concatenate([ctx.reshape(CHUNKS, step, -1), dctx.reshape(CHUNKS, dec, -1)], axis=1)
        done = layer_sums(ctx_all, x, y_tok, mlp_gain, w_full, gate_up, w_down[0])
        done = done.reshape(CHUNKS, step + dec, width)
        hidden = done[:, :step].reshape(seq_len, width)
        tokens = done[:, step:].reshape(CHUNKS * dec, width)

        kv_pair = (qkv[group_q:] * keep_mask)[:, :, None]
        kv_by_pos = lax.all_to_all(kv_pair, 'tp', 1, 2, tiled=True)
        kv_recv = lax.ppermute(kv_by_pos, 'side', send_pairs)
        return (hidden[None], tokens, kv_recv[0][None, None], kv_recv[1][None, None], key_now[None], value_now[None])

    cache_spec = P(None, group_axes, 'tp', None, None)
    in_specs = (P(group_axes, None, None), P(group_axes), P(group_axes, None), P(group_axes), cache_spec, cache_spec, P(), P(None, None, 'tp', None, None), P(None, 'tp', None, None, None), P(), P(None, None, None, 'tp'), P(None, 'tp', None))
    out_specs = (P(group_axes, None, None), P(group_axes, None), cache_spec, cache_spec, cache_spec, cache_spec)
    return jax.shard_map(device_fn, mesh=mesh, in_specs=in_specs, out_specs=out_specs, check_vma=False)
```

```python
import functools

import jax
import jax.numpy as jnp
from jax import lax
from jax.experimental import pallas as pl
from jax.experimental.pallas import tpu as pltpu
from jax.sharding import PartitionSpec as P

ROPE_BASE = 10000.0
NORM_EPS = 1e-5
LOG2E = 1.4426950408889634
BF = jnp.bfloat16
F32 = jnp.float32


def rms_norm(hidden, norm_gain):
    hidden_f32 = hidden.astype(F32)
    inv_rms = lax.rsqrt(jnp.mean(hidden_f32 * hidden_f32, axis=-1, keepdims=True) + NORM_EPS)
    return (hidden_f32 * inv_rms * norm_gain.astype(F32)).astype(BF)


def rope_tables(positions, head_dim):
    half_dim = head_dim // 2
    inv_freq = ROPE_BASE ** (-2.0 * jnp.arange(half_dim, dtype=F32) / head_dim)
    angles = positions.astype(F32)[:, None] * inv_freq[None, :]
    return jnp.cos(angles), jnp.sin(angles)


def rope_rotate(vals_f32, positions):
    half_dim = vals_f32.shape[-1] // 2
    cos_table, sin_table = rope_tables(positions, vals_f32.shape[-1])
    cos_table, sin_table = cos_table[:, None, None, :], sin_table[:, None, None, :]
    first_half = vals_f32[..., :half_dim]
    second_half = vals_f32[..., half_dim:]
    return jnp.concatenate([first_half * cos_table - second_half * sin_table, second_half * cos_table + first_half * sin_table], axis=-1)


def qkv_kernel(x_ref, gain_ref, cos_ref, sin_ref, w_ref, o_ref):
    slots = w_ref.shape[0]
    x = x_ref[...].astype(F32)
    inv = lax.rsqrt(jnp.mean(x * x, axis=-1, keepdims=True) + NORM_EPS)
    normed = (x * inv * gain_ref[...].astype(F32)).astype(BF)
    cos, sin = cos_ref[...], sin_ref[...]
    for first in range(0, slots, 2):
        group = range(first, min(first + 2, slots))
        w = jnp.concatenate([w_ref[s] for s in group], axis=-1)
        y = jnp.dot(normed, w, preferred_element_type=F32)
        for n, s in enumerate(group):
            part = y[:, n * 128:(n + 1) * 128]
            if s < slots - 1:
                part = part * cos + pltpu.roll(part, 64, 1) * sin
            o_ref[s] = part.astype(BF)


def project_qkv(x, gain, cos, sin, w, rows_block=256):
    rows, width = x.shape
    slots, _, head = w.shape
    return pl.pallas_call(
        qkv_kernel,
        grid=(rows // rows_block,),
        in_specs=[
            pl.BlockSpec((rows_block, width), lambda i: (i, 0)),
            pl.BlockSpec((1, width), lambda i: (0, 0)),
            pl.BlockSpec((rows_block, head), lambda i: (i, 0)),
            pl.BlockSpec((rows_block, head), lambda i: (i, 0)),
            pl.BlockSpec((slots, width, head), lambda i: (0, 0, 0), pipeline_mode=pl.Buffered(1)),
        ],
        out_specs=pl.BlockSpec((slots, rows_block, head), lambda i: (0, i, 0)),
        out_shape=jax.ShapeDtypeStruct((slots, rows, head), BF),
        cost_estimate=pl.CostEstimate(flops=2 * rows * width * slots * head, bytes_accessed=2 * (rows * width + slots * head * (width + rows)), transcendentals=0),
        name="project_qkv",
    )(x, gain, cos, sin, w)


MESH = pl.DeviceIdType.MESH


def to(device):
    return dict(device_id={'tp': device}, device_id_type=MESH)


def meet_neighbours(t, last):
    barrier = pltpu.get_barrier_semaphore()

    @pl.when(t > 0)
    def _():
        pl.semaphore_signal(barrier, inc=1, **to(t - 1))

    @pl.when(t < last)
    def _():
        pl.semaphore_signal(barrier, inc=1, **to(t + 1))

    @pl.when((t > 0) & (t < last))
    def _():
        pl.semaphore_wait(barrier, 2)

    @pl.when((t == 0) | (t == last))
    def _():
        pl.semaphore_wait(barrier, 1)


class Spread:
    def __init__(self, t, last, own, place, send_sem, recv_sem):
        self.t, self.last, self.own, self.place, self.send_sem, self.recv_sem = t, last, own, place, send_sem, recv_sem

    def copy(self, source, way, first=False):
        return pltpu.make_async_remote_copy(
            src_ref=self.own if first else self.place(source), dst_ref=self.place(source), send_sem=self.send_sem(source, way),
            recv_sem=self.recv_sem(source), **to(self.t + 1 if way == 0 else self.t - 1))

    def start(self):
        @pl.when(self.t < self.last)
        def _():
            self.copy(self.t, 0, True).start()

        @pl.when(self.t > 0)
        def _():
            self.copy(self.t, 1, True).start()

    def hop(self, n):
        t, last = self.t, self.last

        @pl.when(t >= n)
        def _():
            self.copy(t - n, 0).wait_recv()

            @pl.when(t < last)
            def _():
                self.copy(t - n, 0).start()

        @pl.when(t + n <= last)
        def _():
            self.copy(t + n, 1).wait_recv()

            @pl.when(t > 0)
            def _():
                self.copy(t + n, 1).start()

    def finish(self):
        for source in range(self.last + 1):
            @pl.when((source <= self.t) & (self.t < self.last))
            def _(source=source):
                self.copy(source, 0).wait_send()

            @pl.when((source >= self.t) & (self.t > 0))
            def _(source=source):
                self.copy(source, 1).wait_send()


def flash_kernel(block_q, block_k, some, base, slen_ref, q_ref, k_ref, v_ref, *refs):
    o_ref, s_ref, m_ref, l_ref, p_ref, acc_ref = refs[-6:]
    i = pl.program_id(0) + base
    heads, _, head = q_ref.shape
    rows = heads * block_q
    pieces = rows // some
    lanes = block_k // 128
    slen = slen_ref[0]
    scale = head ** -0.5 * LOG2E
    count = (i * block_q + block_q - 1) // block_k + 1

    def cols(j):
        return pl.ds(pl.multiple_of(j * block_k, block_k), block_k)

    @pl.loop(0, count)
    def _(j):
        k = k_ref[0, cols(j), :]
        s_ref[:, cols(j)] = lax.dot_general(q_ref[...].reshape(rows, head), k, (((1,), (1,)), ((), ())), preferred_element_type=F32)
        edge = ((j + 1) * block_k > i * block_q) | ((j + 1) * block_k > k_ref.shape[1] // 2)

        @pl.when(edge)
        def _():
            @pl.loop(0, pieces)
            def _(r):
                here = pl.ds(pl.multiple_of(r * some, some), some)
                q_pos = i * block_q + (r * some) % block_q + lax.broadcasted_iota(jnp.int32, (some, block_k), 0)
                k_pos = j * block_k + lax.broadcasted_iota(jnp.int32, (some, block_k), 1)
                s_ref[here, cols(j)] = jnp.where((k_pos <= q_pos) & (k_pos < slen), s_ref[here, cols(j)], -1e30)

    tall = rows // heads

    @pl.loop(0, heads)
    def _(r):
        here = pl.ds(pl.multiple_of(r * tall, tall), tall)

        def more(j, top):
            s = s_ref[here, cols(j)]
            for n in range(lanes):
                top = jnp.maximum(top, s[:, n * 128:(n + 1) * 128])
            return top

        top = lax.fori_loop(0, count, more, jnp.full((tall, 128), -jnp.inf, F32))
        m_ref[here] = jnp.broadcast_to(jnp.max(top, axis=-1, keepdims=True), (tall, 128))

    l_ref[...] = jnp.zeros_like(l_ref)
    acc_ref[...] = jnp.zeros_like(acc_ref)

    @pl.loop(0, count)
    def _(j):
        @pl.loop(0, pieces, unroll=2)
        def _(r):
            here = pl.ds(pl.multiple_of(r * some, some), some)
            s = s_ref[here, cols(j)]
            m = m_ref[here]
            total = l_ref[here]
            for n in range(lanes):
                w = jnp.exp2((s[:, n * 128:(n + 1) * 128] - m) * scale)
                total = total + w
                p_ref[here, n * 128:(n + 1) * 128] = w.astype(BF)
            l_ref[here] = total

        acc_ref[...] += jnp.dot(p_ref[...], v_ref[0, cols(j), :], preferred_element_type=F32)

    for h in range(heads):
        here = slice(h * block_q, (h + 1) * block_q)
        o_ref[:, h * head:(h + 1) * head] = (acc_ref[here] / jnp.sum(l_ref[here], axis=-1, keepdims=True)).astype(BF)


def attend(slen, qkv, first, count, total, into=None, block_q=256, block_k=512, some=32):
    slots, rows, head = qkv.shape
    heads = slots - 2
    tall = heads * block_q
    base = first // block_q
    place = 0 if into is None else (total - count) // block_q
    more = [] if into is None else [into]
    share = (first + count) ** 2 - first ** 2
    return pl.pallas_call(
        functools.partial(flash_kernel, block_q, block_k, some, base),
        grid_spec=pltpu.PrefetchScalarGridSpec(
            num_scalar_prefetch=1,
            grid=(count // block_q,),
            in_specs=[
                pl.BlockSpec((heads, block_q, head), lambda i, _: (0, i + base, 0)),
                pl.BlockSpec((1, rows, head), lambda i, _: (heads, 0, 0)),
                pl.BlockSpec((1, rows, head), lambda i, _: (heads + 1, 0, 0)),
            ] + [pl.BlockSpec(memory_space=pl.ANY) for _ in more],
            out_specs=pl.BlockSpec((block_q, heads * head), lambda i, _: (i + place, 0)),
            scratch_shapes=[
                pltpu.VMEM((tall, rows), F32),
                pltpu.VMEM((tall, 128), F32),
                pltpu.VMEM((tall, 128), F32),
                pltpu.VMEM((tall, block_k), BF),
                pltpu.VMEM((tall, head), F32),
            ],
        ),
        out_shape=jax.ShapeDtypeStruct((total, heads * head), BF),
        input_output_aliases={4: 0} if more else {},
        cost_estimate=pl.CostEstimate(flops=3 * heads * share * head, bytes_accessed=2 * (2 * heads + 2) * count * head, transcendentals=heads * share // 2),
        name='attend',
    )(slen, qkv, qkv, qkv, *more)


CHUNKS = 4
SUBS = 13
SLOTS = 2
ACCS = 3
TILE = 256
TILE_OUT = 512
OWNED = (10, 4, 4, 10)


def layer_kernel(geo, ctx_hbm, dctx_hbm, mine_hbm, right_hbm, left_hbm, x_hbm, y_hbm, gain_ref, wo_ref, wg_ref, wu_ref, wd_ref, out_hbm, full_hbm, dfull_hbm, hid_hbm,
                 cx, hid, acc, slots, fins, ress, rs_recv, rs_send, credit, ag_recv, ag_send, fin_sem, res_sem,
                 ctx_recv, ctx_send, load_sem, hid_sem):
    width, head_cols, step, dec, ff_tiles, tail = geo
    rows = step + dec
    sub = rows // SUBS
    total = CHUNKS * SUBS
    out_tiles = width // TILE_OUT
    ticks = out_tiles + ff_tiles
    stride = ticks // SUBS
    tp = width // head_cols
    last = tp - 1
    c, j = pl.program_id(0), pl.program_id(1)
    t = lax.axis_index('tp')

    def at(cond):
        return pl.when(cond)

    def step_rows(chunk):
        return pl.ds(pl.multiple_of(chunk * step, 8), step)

    def dec_rows(chunk):
        return pl.ds(pl.multiple_of(chunk * dec, 8), dec)

    def spread(chunk):
        return Spread(t, last, ctx_hbm.at[step_rows(chunk - 1)], lambda source: full_hbm.at[source, chunk - 1],
                      lambda source, way: ctx_send.at[chunk, source, way], lambda source: ctx_recv.at[chunk, source])

    tokens = Spread(t, last, dctx_hbm, lambda source: dfull_hbm.at[source],
                    lambda source, way: ctx_send.at[0, source, way], lambda source: ctx_recv.at[0, source])

    flows = []
    for f, groups in enumerate(OWNED):
        flows.append((f, sum(OWNED[:f]) * 128, groups * 128, max(f, last - f)))

    def rows_of(k):
        return pl.ds(pl.multiple_of(k * sub, 8), sub)

    def part(f, k):
        _, col, cols, _ = flows[f]
        first = pl.multiple_of((k % SUBS) * sub, 8)
        return acc.at[(k // SUBS) % ACCS, pl.ds(first, sub), pl.ds(col, cols)]

    def out_part(f, k):
        _, col, cols, _ = flows[f]
        return out_hbm.at[rows_of(k), pl.ds(col, cols)]

    def rs_copy(f, k, side, device):
        return pltpu.make_async_remote_copy(
            src_ref=part(f, k), dst_ref=slots[f].at[side, k % SLOTS], send_sem=rs_send.at[f, k % SLOTS],
            recv_sem=rs_recv.at[f, side, k % SLOTS], **to(device))

    def ag_copy(f, k, way, first):
        return pltpu.make_async_remote_copy(
            src_ref=fins[f].at[k % SLOTS] if first else out_part(f, k), dst_ref=out_part(f, k), send_sem=ag_send.at[f, way, k % SLOTS],
            recv_sem=ag_recv.at[f, k], **to(t + 1 if way == 0 else t - 1))

    def fin_copy(f, k):
        return pltpu.make_async_copy(fins[f].at[k % SLOTS], out_part(f, k), fin_sem.at[f, k % SLOTS])

    def res_copy(f, k):
        _, col, cols, _ = flows[f]
        return pltpu.make_async_copy(hid_hbm.at[rows_of(k), pl.ds(col, cols)], ress[f].at[k % SLOTS], res_sem.at[f, k % SLOTS])

    def sides(f):
        found = []
        if f < last:
            found.append((0, t > f, t - f, t + 1, t - 1, t < last))
        if f > 0:
            found.append((1, t < f, f - t, t - 1, t + 1, t > 0))
        return found

    def inside(k):
        return (k >= 0) & (k < total)

    def collect(m):
        for f, col, cols, peak in flows:
            for side, there, dist, outer, inner, more in sides(f):
                k = m - peak + dist

                @at(inside(k) & there & more)
                def _(f=f, side=side, outer=outer, inner=inner, k=k):
                    rs_copy(f, k, side, inner).wait_recv()
                    mine = part(f, k)
                    mine[...] += slots[f][side, k % SLOTS]

                    @at(k + SLOTS < total)
                    def _():
                        pl.semaphore_signal(credit.at[f], inc=1, **to(outer))

            k = m - peak

            @at(inside(k) & (t == f))
            def _(f=f, k=k):
                both = part(f, k)[...]
                for side, _, _, outer, inner, _ in sides(f):
                    rs_copy(f, k, side, inner).wait_recv()
                    both = both + slots[f][side, k % SLOTS]
                res_copy(f, k).wait()

                @at(k >= SLOTS)
                def _():
                    fin_copy(f, k - SLOTS).wait()
                    for side, _, _, _, _, _ in sides(f):
                        ag_copy(f, k - SLOTS, side, True).wait_send()

                fins[f][k % SLOTS] = (ress[f][k % SLOTS].astype(F32) + both).astype(BF)

                @at(k + SLOTS < total)
                def _():
                    for side, _, _, outer, _, _ in sides(f):
                        pl.semaphore_signal(credit.at[f], inc=1, **to(outer))

    def send(m):
        for f, col, cols, peak in flows:
            for side, there, dist, outer, inner, more in sides(f):
                k = m - peak + dist

                @at(inside(k) & there)
                def _(f=f, side=side, inner=inner, k=k):
                    @at(k >= SLOTS)
                    def _():
                        pl.semaphore_wait(credit.at[f], 1)
                        rs_copy(f, k - SLOTS, side, inner).wait_send()

                    rs_copy(f, k, side, inner).start()

        for f, col, cols, peak in flows:
            k = m - peak

            @at(inside(k) & (t == f))
            def _(f=f, k=k):
                for side, _, _, _, _, _ in sides(f):
                    ag_copy(f, k, side, True).start()
                fin_copy(f, k).start()

            @at(inside(k + 1) & (t == f))
            def _(f=f, k=k):
                res_copy(f, k + 1).start()

        for f, col, cols, peak in flows:
            for side, there, dist, outer, inner, more in sides(f):
                a = m - peak - dist

                @at(inside(a) & there)
                def _(f=f, side=side, more=more, a=a):
                    ag_copy(f, a, side, False).wait_recv()

                    @at(more)
                    def _():
                        @at(a >= SLOTS)
                        def _():
                            ag_copy(f, a - SLOTS, side, False).wait_send()

                        ag_copy(f, a, side, False).start()

    @at((c == 0) & (j == 0))
    def _():
        meet_neighbours(t, last)
        tokens.start()
        spread(1).start()
        cx[...] = jnp.zeros_like(cx)
        hid[...] = jnp.zeros_like(hid)
        for n in range(1, last + 1):
            tokens.hop(n)

    @at((c > 0) & (j % stride == 0) & (j < stride * SUBS))
    def _():
        period = SUBS * (c - 1) + j // stride
        collect(period)
        send(period)

    for n in range(1, last + 1):
        @at((c + 1 < CHUNKS) & (j == ticks * n // (last + 1) + 2))
        def _(n=n):
            spread(c + 1).hop(n)
            if n == last:
                @at(c + 2 < CHUNKS)
                def _():
                    spread(c + 2).start()

    @at(j == 0)
    def _():
        loads = [
            pltpu.make_async_copy(x_hbm.at[step_rows(c)], hid.at[pl.ds(0, step)], load_sem.at[2 * tp]),
            pltpu.make_async_copy(y_hbm.at[dec_rows(c)], hid.at[pl.ds(step, dec)], load_sem.at[2 * tp + 1]),
        ]
        for copy in loads:
            copy.start()
        for s in range(tp):
            head_range = pl.ds(s * head_cols, head_cols)
            where, tail_rows = cx.at[pl.ds(0, step), head_range], cx.at[pl.ds(step, dec), head_range]

            for device in range(tp):
                piece = mine_hbm if device == s else right_hbm[device - s - 1] if device > s else left_hbm[s - device - 1]

                @at((c == 0) & (t == device))
                def _(s=s, where=where, piece=piece):
                    pltpu.make_async_copy(piece, where, load_sem.at[s]).start()

            @at((c > 0) & (t == s))
            def _(s=s, where=where):
                pltpu.make_async_copy(ctx_hbm.at[step_rows(c - 1)], where, load_sem.at[s]).start()

            @at((c > 0) & (t != s))
            def _(s=s, where=where):
                pltpu.make_async_copy(full_hbm.at[s, c - 1], where, load_sem.at[s]).start()

            @at(t == s)
            def _(s=s, tail_rows=tail_rows):
                pltpu.make_async_copy(dctx_hbm.at[dec_rows(c)], tail_rows, load_sem.at[tp + s]).start()

            @at(t != s)
            def _(s=s, tail_rows=tail_rows):
                pltpu.make_async_copy(dfull_hbm.at[s, dec_rows(c)], tail_rows, load_sem.at[tp + s]).start()

        for s in range(tp):
            head_range = pl.ds(s * head_cols, head_cols)
            pltpu.make_async_copy(mine_hbm, cx.at[pl.ds(0, step), head_range], load_sem.at[s]).wait()
            pltpu.make_async_copy(dctx_hbm.at[dec_rows(c)], cx.at[pl.ds(step, dec), head_range], load_sem.at[tp + s]).wait()
        for copy in loads:
            copy.wait()

    @at(j < out_tiles)
    def _():
        heads = head_cols // 128
        mixed = None
        for s in range(tp):
            w = wo_ref[s].reshape(head_cols, TILE_OUT)
            one = jnp.dot(cx[:, s * head_cols:(s + 1) * head_cols], w, preferred_element_type=F32)
            mixed = one if mixed is None else mixed + one
        cols = pl.ds(pl.multiple_of(j * TILE_OUT, TILE_OUT), TILE_OUT)
        hid[:, cols] = (hid[:, cols].astype(F32) + mixed).astype(BF)

    hid_copy = pltpu.make_async_copy(hid.at[pl.ds(0, rows)], hid_hbm.at[pl.ds(pl.multiple_of(c * rows, 8), rows)], hid_sem)

    @at(j == out_tiles)
    def _():
        hid_copy.start()
        block = hid.shape[0] // 11

        @pl.loop(0, 11)
        def _(b):
            some = pl.ds(pl.multiple_of(b * block, 16), block)
            h = hid[some].astype(F32)
            inv = lax.rsqrt(jnp.mean(h * h, axis=-1, keepdims=True) + NORM_EPS)
            cx[some] = (h * inv * gain_ref[...].astype(F32)).astype(BF)
            acc[c % ACCS, some] = jnp.zeros((block, width), F32)

    @at(j >= out_tiles)
    def _():
        gate = jnp.dot(cx[...], wg_ref[0], preferred_element_type=F32)
        up = jnp.dot(cx[...], wu_ref[0], preferred_element_type=F32)
        act = (jax.nn.silu(gate) * up).astype(BF)
        which = c % ACCS

        @at(j < ticks - 1)
        def _():
            acc[which] += jnp.dot(act, wd_ref[...], preferred_element_type=F32)

        @at(j == ticks - 1)
        def _():
            acc[which] += jnp.dot(act[:, :tail], wd_ref[:tail], preferred_element_type=F32)
            hid_copy.wait()

    @at((c == CHUNKS - 1) & (j == ticks - 1))
    def _():
        @pl.loop(SUBS * (CHUNKS - 1), total + 2 * last)
        def _(m):
            collect(m)
            send(m)

        for f, col, cols, peak in flows:
            for side, there, dist, outer, inner, more in sides(f):
                @at(there)
                def _(f=f, side=side, inner=inner, more=more):
                    for k in range(total - SLOTS, total):
                        rs_copy(f, k, side, inner).wait_send()

                    @at(more)
                    def _():
                        for k in range(total - SLOTS, total):
                            ag_copy(f, k, side, False).wait_send()

            @at(t == f)
            def _(f=f):
                for k in range(total - SLOTS, total):
                    fin_copy(f, k).wait()
                    for side, _, _, _, _, _ in sides(f):
                        ag_copy(f, k, side, True).wait_send()

        tokens.finish()
        for chunk in range(1, CHUNKS):
            spread(chunk).finish()


def layer_sums(ctx, dctx, mine, right, left, x, y, gain, w_full, w_gate_up, w_down):
    head_cols = ctx.shape[1]
    seq, width = x.shape
    step, dec = seq // CHUNKS, y.shape[0] // CHUNKS
    rows = step + dec
    ff = w_down.shape[0]
    ff_tiles = pl.cdiv(ff, TILE)
    tail = ff - (ff_tiles - 1) * TILE
    out_tiles = width // TILE_OUT
    tp = width // head_cols
    pad = (rows + 15) // 16 * 16
    sub = rows // SUBS
    total = CHUNKS * SUBS
    geo = (width, head_cols, step, dec, ff_tiles, tail)
    heads = head_cols // 128

    def ff_index(j):
        return jnp.maximum(j - out_tiles, 0)

    any_spec = pl.BlockSpec(memory_space=pl.ANY)
    flops = 2 * CHUNKS * rows * width * (width + 3 * ff)
    moved = 2 * CHUNKS * (width * width + 3 * width * ff)
    return pl.pallas_call(
        functools.partial(layer_kernel, geo),
        grid=(CHUNKS, out_tiles + ff_tiles),
        in_specs=[
            any_spec, any_spec, any_spec, [any_spec] * (tp - 1), [any_spec] * (tp - 1), any_spec, any_spec,
            pl.BlockSpec((1, width), lambda c, j: (0, 0)),
            pl.BlockSpec((tp, heads, 128, TILE_OUT), lambda c, j: (0, 0, 0, jnp.minimum(j, out_tiles - 1))),
            pl.BlockSpec((1, width, TILE), lambda c, j: (0, 0, ff_index(j))),
            pl.BlockSpec((1, width, TILE), lambda c, j: (1, 0, ff_index(j))),
            pl.BlockSpec((TILE, width), lambda c, j: (ff_index(j), 0)),
        ],
        out_specs=[any_spec, any_spec, any_spec, any_spec],
        out_shape=[
            jax.ShapeDtypeStruct((CHUNKS * rows, width), BF),
            jax.ShapeDtypeStruct((tp, CHUNKS - 1, step, head_cols), BF),
            jax.ShapeDtypeStruct((tp,) + dctx.shape, BF),
            jax.ShapeDtypeStruct((CHUNKS * rows, width), BF),
        ],
        scratch_shapes=[
            pltpu.VMEM((pad, width), BF),
            pltpu.VMEM((pad, width), BF),
            pltpu.VMEM((ACCS, pad, width), F32),
            [pltpu.VMEM((2, SLOTS, sub, groups * 128), F32) for groups in OWNED],
            [pltpu.VMEM((SLOTS, sub, groups * 128), BF) for groups in OWNED],
            [pltpu.VMEM((SLOTS, sub, groups * 128), BF) for groups in OWNED],
            pltpu.SemaphoreType.DMA((tp, 2, SLOTS)),
            pltpu.SemaphoreType.DMA((tp, SLOTS)),
            pltpu.SemaphoreType.REGULAR((tp,)),
            pltpu.SemaphoreType.DMA((tp, total)),
            pltpu.SemaphoreType.DMA((tp, 2, SLOTS)),
            pltpu.SemaphoreType.DMA((tp, SLOTS)),
            pltpu.SemaphoreType.DMA((tp, SLOTS)),
            pltpu.SemaphoreType.DMA((CHUNKS, tp)),
            pltpu.SemaphoreType.DMA((CHUNKS, tp, 2)),
            pltpu.SemaphoreType.DMA((2 * tp + 2,)),
            pltpu.SemaphoreType.DMA(()),
        ],
        compiler_params=pltpu.CompilerParams(collective_id=0, has_side_effects=True, vmem_limit_bytes=67000000, dimension_semantics=('arbitrary', 'arbitrary')),
        cost_estimate=pl.CostEstimate(flops=flops, bytes_accessed=moved, transcendentals=0),
        name='layer_sums',
    )(ctx, dctx, mine, right, left, x, y, gain, w_full, w_gate_up, w_gate_up, w_down)[0]


def decode_local(tokens, cache_lens, k_cache, v_cache, gain, w_qkv):
    group_q = w_qkv.shape[2] - 2
    head_dim = w_qkv.shape[3]
    cache_local = k_cache.shape[1]
    cache_pos = lax.axis_index('tp') * cache_local + jnp.arange(cache_local)
    write_mask = (cache_pos[None, :] == cache_lens[:, None])[:, :, None, None]
    allowed = (cache_pos[None, :] <= cache_lens[:, None])[None, :, None, :]
    normed = rms_norm(tokens, gain)
    projected = jnp.einsum('bd,dkjh->bkjh', normed, w_qkv, preferred_element_type=F32)
    rotated = rope_rotate(projected[:, :, :group_q + 1], cache_lens)
    local_qkv = jnp.concatenate([rotated, projected[:, :, group_q + 1:]], axis=2).astype(BF)[:, 0]
    tp = k_cache.shape[2]
    full_qkv = lax.all_to_all(jnp.broadcast_to(local_qkv, (tp,) + local_qkv.shape), 'tp', 0, 0)
    key_now = jnp.where(write_mask, jnp.moveaxis(full_qkv[:, :, group_q], 0, 1)[:, None], k_cache)
    value_now = jnp.where(write_mask, jnp.moveaxis(full_qkv[:, :, group_q + 1], 0, 1)[:, None], v_cache)
    scores = jnp.einsum('kbgh,btkh->kbgt', full_qkv[:, :, :group_q], key_now, preferred_element_type=F32) * head_dim ** -0.5
    scores = jnp.where(allowed, scores, -1e30)
    top = jnp.max(scores, axis=-1)
    weights = jnp.exp(scores - top[..., None])
    mixed = jnp.einsum('kbgt,btkh->kbgh', weights.astype(BF), value_now, preferred_element_type=F32)
    stats = jnp.concatenate([top, jnp.sum(weights, axis=-1)], axis=-1)
    stats = jnp.pad(stats, ((0, 0), (0, 0), (0, head_dim - stats.shape[-1])))
    return jnp.concatenate([mixed, stats[:, :, None]], axis=2), key_now, value_now


def decode_combine(mixed):
    heads = mixed.shape[2] - 1
    own = lax.all_to_all(mixed, 'tp', 0, 0)
    top, total = own[:, :, heads, :heads], own[:, :, heads, heads:2 * heads]
    factor = jnp.exp(top - jnp.max(top, axis=0))
    return (jnp.sum(own[:, :, :heads] * factor[..., None], axis=0) / jnp.sum(total * factor, axis=0)[..., None]).astype(BF)


def pass_on(right, left, hop, tp):
    return (lax.ppermute(right, 'tp', [(place, place + 1) for place in range(hop - 1, tp - 1)]),
            lax.ppermute(left, 'tp', [(place, place - 1) for place in range(tp - hop, 0, -1)]))


def gather_w_out(w_out, mesh):
    index = lax.axis_index('pair') * mesh.shape['side'] + lax.axis_index('side')
    own = lax.dynamic_index_in_dim(w_out, jnp.minimum(index, w_out.shape[0] - 1), 0, keepdims=False)
    return lax.all_gather(own, ('tp', 'pair', 'side'))


def solution(mesh):
    side_size = mesh.shape['side']
    tp = mesh.shape['tp']
    send_pairs = [(source, (source + 1) % side_size) for source in range(side_size)]
    group_axes = ('pair', 'side')

    def device_fn(x_prompt, s_len, y_tok, c_len, k_cache, v_cache, attn_gain, w_qkv, w_out, mlp_gain, w_gate_up, w_down):
        x = x_prompt[0]
        seq_len, width = x.shape
        group_q, head = w_qkv.shape[3] - 2, w_qkv.shape[4]
        positions = jnp.arange(seq_len)
        keep_mask = (positions < s_len[0])[:, None].astype(BF)
        cos, sin = rope_tables(positions, head)
        cos, sin = jnp.concatenate([cos, cos], -1), jnp.concatenate([-sin, sin], -1)

        w_full = gather_w_out(w_out[0, 0], mesh).reshape(tp, -1, head, width)
        gate_up = jnp.transpose(w_gate_up[0], (1, 0, 2))

        mixed, key_now, value_now = decode_local(y_tok, c_len, k_cache[0], v_cache[0], attn_gain[0], w_qkv[0])

        w_slots = jnp.transpose(w_qkv[0, :, 0], (1, 0, 2))
        qkv = project_qkv(x, attn_gain, cos, sin, w_slots)
        step, dec = seq_len // CHUNKS, y_tok.shape[0] // CHUNKS
        rest = seq_len - step
        mine = attend(s_len, qkv, 0, step, step)
        moved = [pass_on(mine, mine, 1, tp)]
        mixed, qkv, mine = lax.optimization_barrier((mixed, qkv, mine))
        dctx = decode_combine(mixed)
        ctx = attend(s_len, qkv, step, rest - step, rest)
        for hop in range(2, tp):
            pair = pass_on(*moved[-1], hop, tp)
            if hop < tp - 1:
                ctx, pair = lax.optimization_barrier((ctx, pair))
            moved.append(pair)
        ctx = attend(s_len, qkv, rest, step, rest, ctx)

        done = layer_sums(ctx, dctx.reshape(-1, ctx.shape[1]), mine, [r for r, _ in moved], [l for _, l in moved], x, y_tok, mlp_gain, w_full, gate_up, w_down[0])
        done = done.reshape(CHUNKS, step + dec, width)
        hidden = done[:, :step].reshape(seq_len, width)
        tokens = done[:, step:].reshape(CHUNKS * dec, width)

        kv_pair = (qkv[group_q:] * keep_mask)[:, :, None]
        kv_by_pos = lax.all_to_all(kv_pair, 'tp', 1, 2, tiled=True)
        kv_recv = lax.ppermute(kv_by_pos, 'side', send_pairs)
        return (hidden[None], tokens, kv_recv[0][None, None], kv_recv[1][None, None], key_now[None], value_now[None])

    cache_spec = P(None, group_axes, 'tp', None, None)
    in_specs = (P(group_axes, None, None), P(group_axes), P(group_axes, None), P(group_axes), cache_spec, cache_spec, P(), P(None, None, 'tp', None, None), P(None, 'tp', None, None, None), P(), P(None, None, None, 'tp'), P(None, 'tp', None))
    out_specs = (P(group_axes, None, None), P(group_axes, None), cache_spec, cache_spec, cache_spec, cache_spec)
    return jax.shard_map(device_fn, mesh=mesh, in_specs=in_specs, out_specs=out_specs, check_vma=False)
```

```python
import functools

import jax
import jax.numpy as jnp
from jax import lax
from jax.experimental import pallas as pl
from jax.experimental.pallas import tpu as pltpu
from jax.sharding import PartitionSpec as P

ROPE_BASE = 10000.0
NORM_EPS = 1e-5
LOG2E = 1.4426950408889634
BF = jnp.bfloat16
F32 = jnp.float32


def rms_norm(hidden, norm_gain):
    hidden_f32 = hidden.astype(F32)
    inv_rms = lax.rsqrt(jnp.mean(hidden_f32 * hidden_f32, axis=-1, keepdims=True) + NORM_EPS)
    return (hidden_f32 * inv_rms * norm_gain.astype(F32)).astype(BF)


def rope_tables(positions, head_dim):
    half_dim = head_dim // 2
    inv_freq = ROPE_BASE ** (-2.0 * jnp.arange(half_dim, dtype=F32) / head_dim)
    angles = positions.astype(F32)[:, None] * inv_freq[None, :]
    return jnp.cos(angles), jnp.sin(angles)


def rope_rotate(vals_f32, positions):
    half_dim = vals_f32.shape[-1] // 2
    cos_table, sin_table = rope_tables(positions, vals_f32.shape[-1])
    cos_table, sin_table = cos_table[:, None, None, :], sin_table[:, None, None, :]
    first_half = vals_f32[..., :half_dim]
    second_half = vals_f32[..., half_dim:]
    return jnp.concatenate([first_half * cos_table - second_half * sin_table, second_half * cos_table + first_half * sin_table], axis=-1)


def qkv_kernel(x_ref, gain_ref, cos_ref, sin_ref, w_ref, o_ref):
    slots = w_ref.shape[0]
    x = x_ref[...].astype(F32)
    inv = lax.rsqrt(jnp.mean(x * x, axis=-1, keepdims=True) + NORM_EPS)
    normed = (x * inv * gain_ref[...].astype(F32)).astype(BF)
    cos, sin = cos_ref[...], sin_ref[...]
    for first in range(0, slots, 2):
        group = range(first, min(first + 2, slots))
        w = jnp.concatenate([w_ref[s] for s in group], axis=-1)
        y = jnp.dot(normed, w, preferred_element_type=F32)
        for n, s in enumerate(group):
            part = y[:, n * 128:(n + 1) * 128]
            if s < slots - 1:
                part = part * cos + pltpu.roll(part, 64, 1) * sin
            o_ref[s] = part.astype(BF)


def project_qkv(x, gain, cos, sin, w, rows_block=256):
    rows, width = x.shape
    slots, _, head = w.shape
    return pl.pallas_call(
        qkv_kernel,
        grid=(rows // rows_block,),
        in_specs=[
            pl.BlockSpec((rows_block, width), lambda i: (i, 0)),
            pl.BlockSpec((1, width), lambda i: (0, 0)),
            pl.BlockSpec((rows_block, head), lambda i: (i, 0)),
            pl.BlockSpec((rows_block, head), lambda i: (i, 0)),
            pl.BlockSpec((slots, width, head), lambda i: (0, 0, 0), pipeline_mode=pl.Buffered(1)),
        ],
        out_specs=pl.BlockSpec((slots, rows_block, head), lambda i: (0, i, 0)),
        out_shape=jax.ShapeDtypeStruct((slots, rows, head), BF),
        cost_estimate=pl.CostEstimate(flops=2 * rows * width * slots * head, bytes_accessed=2 * (rows * width + slots * head * (width + rows)), transcendentals=0),
        name="project_qkv",
    )(x, gain, cos, sin, w)


MESH = pl.DeviceIdType.MESH


def to(device):
    return dict(device_id={'tp': device}, device_id_type=MESH)


def meet_neighbours(t, last):
    barrier = pltpu.get_barrier_semaphore()

    @pl.when(t > 0)
    def _():
        pl.semaphore_signal(barrier, inc=1, **to(t - 1))

    @pl.when(t < last)
    def _():
        pl.semaphore_signal(barrier, inc=1, **to(t + 1))

    @pl.when((t > 0) & (t < last))
    def _():
        pl.semaphore_wait(barrier, 2)

    @pl.when((t == 0) | (t == last))
    def _():
        pl.semaphore_wait(barrier, 1)


class Spread:
    def __init__(self, t, last, own, place, send_sem, recv_sem):
        self.t, self.last, self.own, self.place, self.send_sem, self.recv_sem = t, last, own, place, send_sem, recv_sem

    def copy(self, source, way, first=False):
        return pltpu.make_async_remote_copy(
            src_ref=self.own if first else self.place(source), dst_ref=self.place(source), send_sem=self.send_sem(source, way),
            recv_sem=self.recv_sem(source), **to(self.t + 1 if way == 0 else self.t - 1))

    def start(self):
        @pl.when(self.t < self.last)
        def _():
            self.copy(self.t, 0, True).start()

        @pl.when(self.t > 0)
        def _():
            self.copy(self.t, 1, True).start()

    def hop(self, n):
        t, last = self.t, self.last

        @pl.when(t >= n)
        def _():
            self.copy(t - n, 0).wait_recv()

            @pl.when(t < last)
            def _():
                self.copy(t - n, 0).start()

        @pl.when(t + n <= last)
        def _():
            self.copy(t + n, 1).wait_recv()

            @pl.when(t > 0)
            def _():
                self.copy(t + n, 1).start()

    def finish(self):
        for source in range(self.last + 1):
            @pl.when((source <= self.t) & (self.t < self.last))
            def _(source=source):
                self.copy(source, 0).wait_send()

            @pl.when((source >= self.t) & (self.t > 0))
            def _(source=source):
                self.copy(source, 1).wait_send()


def flash_kernel(block_q, block_k, some, base, slen_ref, q_ref, k_ref, v_ref, *refs):
    o_ref, s_ref, m_ref, l_ref, p_ref, acc_ref = refs[-6:]
    i = pl.program_id(0) + base
    heads, _, head = q_ref.shape
    rows = heads * block_q
    pieces = rows // some
    lanes = block_k // 128
    slen = slen_ref[0]
    scale = head ** -0.5 * LOG2E
    count = (i * block_q + block_q - 1) // block_k + 1

    def cols(j):
        return pl.ds(pl.multiple_of(j * block_k, block_k), block_k)

    @pl.loop(0, count)
    def _(j):
        k = k_ref[0, cols(j), :]
        s_ref[:, cols(j)] = lax.dot_general(q_ref[...].reshape(rows, head), k, (((1,), (1,)), ((), ())), preferred_element_type=F32)
        edge = ((j + 1) * block_k > i * block_q) | ((j + 1) * block_k > k_ref.shape[1] // 2)

        @pl.when(edge)
        def _():
            @pl.loop(0, pieces)
            def _(r):
                here = pl.ds(pl.multiple_of(r * some, some), some)
                q_pos = i * block_q + (r * some) % block_q + lax.broadcasted_iota(jnp.int32, (some, block_k), 0)
                k_pos = j * block_k + lax.broadcasted_iota(jnp.int32, (some, block_k), 1)
                s_ref[here, cols(j)] = jnp.where((k_pos <= q_pos) & (k_pos < slen), s_ref[here, cols(j)], -1e30)

    tall = rows // heads

    @pl.loop(0, heads)
    def _(r):
        here = pl.ds(pl.multiple_of(r * tall, tall), tall)

        def more(j, top):
            s = s_ref[here, cols(j)]
            for n in range(lanes):
                top = jnp.maximum(top, s[:, n * 128:(n + 1) * 128])
            return top

        top = lax.fori_loop(0, count, more, jnp.full((tall, 128), -jnp.inf, F32))
        m_ref[here] = jnp.broadcast_to(jnp.max(top, axis=-1, keepdims=True), (tall, 128))

    l_ref[...] = jnp.zeros_like(l_ref)
    acc_ref[...] = jnp.zeros_like(acc_ref)

    @pl.loop(0, count)
    def _(j):
        @pl.loop(0, pieces, unroll=2)
        def _(r):
            here = pl.ds(pl.multiple_of(r * some, some), some)
            s = s_ref[here, cols(j)]
            m = m_ref[here]
            total = l_ref[here]
            for n in range(lanes):
                w = jnp.exp2((s[:, n * 128:(n + 1) * 128] - m) * scale)
                total = total + w
                p_ref[here, n * 128:(n + 1) * 128] = w.astype(BF)
            l_ref[here] = total

        acc_ref[...] += jnp.dot(p_ref[...], v_ref[0, cols(j), :], preferred_element_type=F32)

    for h in range(heads):
        here = slice(h * block_q, (h + 1) * block_q)
        o_ref[:, h * head:(h + 1) * head] = (acc_ref[here] / jnp.sum(l_ref[here], axis=-1, keepdims=True)).astype(BF)


def attend(slen, qkv, first, count, total, into=None, block_q=256, block_k=512, some=32):
    slots, rows, head = qkv.shape
    heads = slots - 2
    tall = heads * block_q
    base = first // block_q
    place = 0 if into is None else (total - count) // block_q
    more = [] if into is None else [into]
    share = (first + count) ** 2 - first ** 2
    return pl.pallas_call(
        functools.partial(flash_kernel, block_q, block_k, some, base),
        grid_spec=pltpu.PrefetchScalarGridSpec(
            num_scalar_prefetch=1,
            grid=(count // block_q,),
            in_specs=[
                pl.BlockSpec((heads, block_q, head), lambda i, _: (0, i + base, 0)),
                pl.BlockSpec((1, rows, head), lambda i, _: (heads, 0, 0)),
                pl.BlockSpec((1, rows, head), lambda i, _: (heads + 1, 0, 0)),
            ] + [pl.BlockSpec(memory_space=pl.ANY) for _ in more],
            out_specs=pl.BlockSpec((block_q, heads * head), lambda i, _: (i + place, 0)),
            scratch_shapes=[
                pltpu.VMEM((tall, rows), F32),
                pltpu.VMEM((tall, 128), F32),
                pltpu.VMEM((tall, 128), F32),
                pltpu.VMEM((tall, block_k), BF),
                pltpu.VMEM((tall, head), F32),
            ],
        ),
        out_shape=jax.ShapeDtypeStruct((total, heads * head), BF),
        input_output_aliases={4: 0} if more else {},
        cost_estimate=pl.CostEstimate(flops=3 * heads * share * head, bytes_accessed=2 * (2 * heads + 2) * count * head, transcendentals=heads * share // 2),
        name='attend',
    )(slen, qkv, qkv, qkv, *more)


CHUNKS = 4
SUBS = 5
SLOTS = 2
ACCS = 3
TILE = 256
TILE_OUT = 512
OWNED = (11, 3, 3, 11)


def layer_kernel(geo, ctx_hbm, dctx_hbm, mine_hbm, right_hbm, left_hbm, x_hbm, y_hbm, gain_ref, wo_ref, wg_ref, wu_ref, wd_ref, out_hbm, full_hbm, dfull_hbm, hid_hbm,
                 cx, hid, acc, slots, fins, ress, rs_recv, rs_send, credit, ag_recv, ag_send, fin_sem, res_sem,
                 ctx_recv, ctx_send, load_sem, hid_sem):
    width, head_cols, step, dec, ff_tiles, tail = geo
    rows = step + dec
    sub = rows // SUBS
    total = CHUNKS * SUBS
    out_tiles = width // TILE_OUT
    ticks = out_tiles + ff_tiles
    stride = ticks // SUBS
    tp = width // head_cols
    last = tp - 1
    c, j = pl.program_id(0), pl.program_id(1)
    t = lax.axis_index('tp')

    def at(cond):
        return pl.when(cond)

    def step_rows(chunk):
        return pl.ds(pl.multiple_of(chunk * step, 8), step)

    def dec_rows(chunk):
        return pl.ds(pl.multiple_of(chunk * dec, 8), dec)

    def spread(chunk):
        return Spread(t, last, ctx_hbm.at[step_rows(chunk - 1)], lambda source: full_hbm.at[source, chunk - 1],
                      lambda source, way: ctx_send.at[chunk, source, way], lambda source: ctx_recv.at[chunk, source])

    tokens = Spread(t, last, dctx_hbm, lambda source: dfull_hbm.at[source],
                    lambda source, way: ctx_send.at[0, source, way], lambda source: ctx_recv.at[0, source])

    flows = []
    for f, groups in enumerate(OWNED):
        flows.append((f, sum(OWNED[:f]) * 128, groups * 128, max(f, last - f)))

    def rows_of(k):
        return pl.ds(pl.multiple_of(k * sub, 8), sub)

    def part(f, k):
        _, col, cols, _ = flows[f]
        first = pl.multiple_of((k % SUBS) * sub, 8)
        return acc.at[(k // SUBS) % ACCS, pl.ds(first, sub), pl.ds(col, cols)]

    def out_part(f, k):
        _, col, cols, _ = flows[f]
        return out_hbm.at[rows_of(k), pl.ds(col, cols)]

    def rs_copy(f, k, side, device):
        return pltpu.make_async_remote_copy(
            src_ref=part(f, k), dst_ref=slots[f].at[side, k % SLOTS], send_sem=rs_send.at[f, k % SLOTS],
            recv_sem=rs_recv.at[f, side, k % SLOTS], **to(device))

    def ag_copy(f, k, way, first):
        return pltpu.make_async_remote_copy(
            src_ref=fins[f].at[k % SLOTS] if first else out_part(f, k), dst_ref=out_part(f, k), send_sem=ag_send.at[f, way, k % SLOTS],
            recv_sem=ag_recv.at[f, k], **to(t + 1 if way == 0 else t - 1))

    def fin_copy(f, k):
        return pltpu.make_async_copy(fins[f].at[k % SLOTS], out_part(f, k), fin_sem.at[f, k % SLOTS])

    def res_copy(f, k):
        _, col, cols, _ = flows[f]
        return pltpu.make_async_copy(hid_hbm.at[rows_of(k), pl.ds(col, cols)], ress[f].at[k % SLOTS], res_sem.at[f, k % SLOTS])

    def sides(f):
        found = []
        if f < last:
            found.append((0, t > f, t - f, t + 1, t - 1, t < last))
        if f > 0:
            found.append((1, t < f, f - t, t - 1, t + 1, t > 0))
        return found

    def inside(k):
        return (k >= 0) & (k < total)

    def advance(m):
        for f, col, cols, peak in flows:
            for side, there, dist, outer, inner, more in sides(f):
                k = m - peak + dist

                @at(inside(k) & there)
                def _(f=f, side=side, outer=outer, inner=inner, more=more, k=k):
                    @at(more)
                    def _():
                        rs_copy(f, k, side, inner).wait_recv()
                        mine = part(f, k)
                        mine[...] += slots[f][side, k % SLOTS]

                        @at(k + SLOTS < total)
                        def _():
                            pl.semaphore_signal(credit.at[f], inc=1, **to(outer))

                    @at(k >= SLOTS)
                    def _():
                        pl.semaphore_wait(credit.at[f], 1)
                        rs_copy(f, k - SLOTS, side, inner).wait_send()

                    rs_copy(f, k, side, inner).start()

            k = m - peak

            @at(inside(k) & (t == f))
            def _(f=f, k=k):
                both = part(f, k)[...]
                for side, _, _, outer, inner, _ in sides(f):
                    rs_copy(f, k, side, inner).wait_recv()
                    both = both + slots[f][side, k % SLOTS]
                res_copy(f, k).wait()

                @at(k >= SLOTS)
                def _():
                    fin_copy(f, k - SLOTS).wait()
                    for side, _, _, _, _, _ in sides(f):
                        ag_copy(f, k - SLOTS, side, True).wait_send()

                fins[f][k % SLOTS] = (ress[f][k % SLOTS].astype(F32) + both).astype(BF)

                @at(k + SLOTS < total)
                def _():
                    for side, _, _, outer, _, _ in sides(f):
                        pl.semaphore_signal(credit.at[f], inc=1, **to(outer))

        for f, col, cols, peak in flows:
            k = m - peak

            @at(inside(k) & (t == f))
            def _(f=f, k=k):
                for side, _, _, _, _, _ in sides(f):
                    ag_copy(f, k, side, True).start()
                fin_copy(f, k).start()

            @at(inside(k + 1) & (t == f))
            def _(f=f, k=k):
                res_copy(f, k + 1).start()

        for f, col, cols, peak in flows:
            for side, there, dist, outer, inner, more in sides(f):
                a = m - peak - dist

                @at(inside(a) & there)
                def _(f=f, side=side, more=more, a=a):
                    ag_copy(f, a, side, False).wait_recv()

                    @at(more)
                    def _():
                        @at(a >= SLOTS)
                        def _():
                            ag_copy(f, a - SLOTS, side, False).wait_send()

                        ag_copy(f, a, side, False).start()

    @at((c == 0) & (j == 0))
    def _():
        meet_neighbours(t, last)
        tokens.start()
        spread(1).start()
        cx[...] = jnp.zeros_like(cx)
        hid[...] = jnp.zeros_like(hid)
        for n in range(1, last + 1):
            tokens.hop(n)

    @at((c > 0) & (j % stride == 0) & (j < stride * SUBS))
    def _():
        advance(SUBS * (c - 1) + j // stride)

    for n in range(1, last + 1):
        @at((c + 1 < CHUNKS) & (j == ticks * n // (last + 1) + 1))
        def _(n=n):
            spread(c + 1).hop(n)
            if n == last:
                @at(c + 2 < CHUNKS)
                def _():
                    spread(c + 2).start()

    @at(j == 0)
    def _():
        loads = [
            pltpu.make_async_copy(x_hbm.at[step_rows(c)], hid.at[pl.ds(0, step)], load_sem.at[2 * tp]),
            pltpu.make_async_copy(y_hbm.at[dec_rows(c)], hid.at[pl.ds(step, dec)], load_sem.at[2 * tp + 1]),
        ]
        for copy in loads:
            copy.start()
        for s in range(tp):
            head_range = pl.ds(s * head_cols, head_cols)
            where, tail_rows = cx.at[pl.ds(0, step), head_range], cx.at[pl.ds(step, dec), head_range]

            for device in range(tp):
                piece = mine_hbm if device == s else right_hbm[device - s - 1] if device > s else left_hbm[s - device - 1]

                @at((c == 0) & (t == device))
                def _(s=s, where=where, piece=piece):
                    pltpu.make_async_copy(piece, where, load_sem.at[s]).start()

            @at((c > 0) & (t == s))
            def _(s=s, where=where):
                pltpu.make_async_copy(ctx_hbm.at[step_rows(c - 1)], where, load_sem.at[s]).start()

            @at((c > 0) & (t != s))
            def _(s=s, where=where):
                pltpu.make_async_copy(full_hbm.at[s, c - 1], where, load_sem.at[s]).start()

            @at(t == s)
            def _(s=s, tail_rows=tail_rows):
                pltpu.make_async_copy(dctx_hbm.at[dec_rows(c)], tail_rows, load_sem.at[tp + s]).start()

            @at(t != s)
            def _(s=s, tail_rows=tail_rows):
                pltpu.make_async_copy(dfull_hbm.at[s, dec_rows(c)], tail_rows, load_sem.at[tp + s]).start()

        for s in range(tp):
            head_range = pl.ds(s * head_cols, head_cols)
            pltpu.make_async_copy(mine_hbm, cx.at[pl.ds(0, step), head_range], load_sem.at[s]).wait()
            pltpu.make_async_copy(dctx_hbm.at[dec_rows(c)], cx.at[pl.ds(step, dec), head_range], load_sem.at[tp + s]).wait()
        for copy in loads:
            copy.wait()

    @at(j < out_tiles)
    def _():
        mixed = None
        for s in range(tp):
            one = jnp.dot(cx[:, s * head_cols:(s + 1) * head_cols], wo_ref[s], preferred_element_type=F32)
            mixed = one if mixed is None else mixed + one
        cols = pl.ds(pl.multiple_of(j * TILE_OUT, TILE_OUT), TILE_OUT)
        hid[:, cols] = (hid[:, cols].astype(F32) + mixed).astype(BF)

    hid_copy = pltpu.make_async_copy(hid.at[pl.ds(0, rows)], hid_hbm.at[pl.ds(pl.multiple_of(c * rows, 8), rows)], hid_sem)

    @at(j == out_tiles)
    def _():
        hid_copy.start()
        block = hid.shape[0] // 11

        @pl.loop(0, 11)
        def _(b):
            some = pl.ds(pl.multiple_of(b * block, 16), block)
            h = hid[some].astype(F32)
            inv = lax.rsqrt(jnp.mean(h * h, axis=-1, keepdims=True) + NORM_EPS)
            cx[some] = (h * inv * gain_ref[...].astype(F32)).astype(BF)
            acc[c % ACCS, some] = jnp.zeros((block, width), F32)

    @at(j >= out_tiles)
    def _():
        gate = jnp.dot(cx[...], wg_ref[0], preferred_element_type=F32)
        up = jnp.dot(cx[...], wu_ref[0], preferred_element_type=F32)
        act = (jax.nn.silu(gate) * up).astype(BF)
        which = c % ACCS

        @at(j < ticks - 1)
        def _():
            acc[which] += jnp.dot(act, wd_ref[...], preferred_element_type=F32)

        @at(j == ticks - 1)
        def _():
            acc[which] += jnp.dot(act[:, :tail], wd_ref[:tail], preferred_element_type=F32)
            hid_copy.wait()

    @at((c == CHUNKS - 1) & (j == ticks - 1))
    def _():
        @pl.loop(SUBS * (CHUNKS - 1), total + 2 * last)
        def _(m):
            advance(m)

        for f, col, cols, peak in flows:
            for side, there, dist, outer, inner, more in sides(f):
                @at(there)
                def _(f=f, side=side, inner=inner, more=more):
                    for k in range(total - SLOTS, total):
                        rs_copy(f, k, side, inner).wait_send()

                    @at(more)
                    def _():
                        for k in range(total - SLOTS, total):
                            ag_copy(f, k, side, False).wait_send()

            @at(t == f)
            def _(f=f):
                for k in range(total - SLOTS, total):
                    fin_copy(f, k).wait()
                    for side, _, _, _, _, _ in sides(f):
                        ag_copy(f, k, side, True).wait_send()

        tokens.finish()
        for chunk in range(1, CHUNKS):
            spread(chunk).finish()


def layer_sums(ctx, dctx, mine, right, left, x, y, gain, w_full, w_gate_up, w_down):
    head_cols = ctx.shape[1]
    seq, width = x.shape
    step, dec = seq // CHUNKS, y.shape[0] // CHUNKS
    rows = step + dec
    ff = w_down.shape[0]
    ff_tiles = pl.cdiv(ff, TILE)
    tail = ff - (ff_tiles - 1) * TILE
    out_tiles = width // TILE_OUT
    tp = width // head_cols
    pad = (rows + 15) // 16 * 16
    sub = rows // SUBS
    total = CHUNKS * SUBS
    geo = (width, head_cols, step, dec, ff_tiles, tail)
    def ff_index(j):
        return jnp.maximum(j - out_tiles, 0)

    any_spec = pl.BlockSpec(memory_space=pl.ANY)
    flops = 2 * CHUNKS * rows * width * (width + 3 * ff)
    moved = 2 * CHUNKS * (width * width + 3 * width * ff)
    return pl.pallas_call(
        functools.partial(layer_kernel, geo),
        grid=(CHUNKS, out_tiles + ff_tiles),
        in_specs=[
            any_spec, any_spec, any_spec, [any_spec] * (tp - 1), [any_spec] * (tp - 1), any_spec, any_spec,
            pl.BlockSpec((1, width), lambda c, j: (0, 0)),
            pl.BlockSpec((tp, head_cols, TILE_OUT), lambda c, j: (0, 0, jnp.minimum(j, out_tiles - 1))),
            pl.BlockSpec((1, width, TILE), lambda c, j: (0, 0, ff_index(j))),
            pl.BlockSpec((1, width, TILE), lambda c, j: (1, 0, ff_index(j))),
            pl.BlockSpec((TILE, width), lambda c, j: (ff_index(j), 0)),
        ],
        out_specs=[any_spec, any_spec, any_spec, any_spec],
        out_shape=[
            jax.ShapeDtypeStruct((CHUNKS * rows, width), BF),
            jax.ShapeDtypeStruct((tp, CHUNKS - 1, step, head_cols), BF),
            jax.ShapeDtypeStruct((tp,) + dctx.shape, BF),
            jax.ShapeDtypeStruct((CHUNKS * rows, width), BF),
        ],
        scratch_shapes=[
            pltpu.VMEM((pad, width), BF),
            pltpu.VMEM((pad, width), BF),
            pltpu.VMEM((ACCS, pad, width), F32),
            [pltpu.VMEM((2, SLOTS, sub, groups * 128), F32) for groups in OWNED],
            [pltpu.VMEM((SLOTS, sub, groups * 128), BF) for groups in OWNED],
            [pltpu.VMEM((SLOTS, sub, groups * 128), BF) for groups in OWNED],
            pltpu.SemaphoreType.DMA((tp, 2, SLOTS)),
            pltpu.SemaphoreType.DMA((tp, SLOTS)),
            pltpu.SemaphoreType.REGULAR((tp,)),
            pltpu.SemaphoreType.DMA((tp, total)),
            pltpu.SemaphoreType.DMA((tp, 2, SLOTS)),
            pltpu.SemaphoreType.DMA((tp, SLOTS)),
            pltpu.SemaphoreType.DMA((tp, SLOTS)),
            pltpu.SemaphoreType.DMA((CHUNKS, tp)),
            pltpu.SemaphoreType.DMA((CHUNKS, tp, 2)),
            pltpu.SemaphoreType.DMA((2 * tp + 2,)),
            pltpu.SemaphoreType.DMA(()),
        ],
        compiler_params=pltpu.CompilerParams(collective_id=0, has_side_effects=True, vmem_limit_bytes=67000000, dimension_semantics=('arbitrary', 'arbitrary')),
        cost_estimate=pl.CostEstimate(flops=flops, bytes_accessed=moved, transcendentals=0),
        name='layer_sums',
    )(ctx, dctx, mine, right, left, x, y, gain, w_full, w_gate_up, w_gate_up, w_down)[0]


def decode_local(tokens, cache_lens, k_cache, v_cache, gain, w_qkv):
    group_q = w_qkv.shape[2] - 2
    head_dim = w_qkv.shape[3]
    cache_local = k_cache.shape[1]
    cache_pos = lax.axis_index('tp') * cache_local + jnp.arange(cache_local)
    write_mask = (cache_pos[None, :] == cache_lens[:, None])[:, :, None, None]
    allowed = (cache_pos[None, :] <= cache_lens[:, None])[None, :, None, :]
    normed = rms_norm(tokens, gain)
    projected = jnp.einsum('bd,dkjh->bkjh', normed, w_qkv, preferred_element_type=F32)
    rotated = rope_rotate(projected[:, :, :group_q + 1], cache_lens)
    local_qkv = jnp.concatenate([rotated, projected[:, :, group_q + 1:]], axis=2).astype(BF)[:, 0]
    tp = k_cache.shape[2]
    full_qkv = lax.all_to_all(jnp.broadcast_to(local_qkv, (tp,) + local_qkv.shape), 'tp', 0, 0)
    key_now = jnp.where(write_mask, jnp.moveaxis(full_qkv[:, :, group_q], 0, 1)[:, None], k_cache)
    value_now = jnp.where(write_mask, jnp.moveaxis(full_qkv[:, :, group_q + 1], 0, 1)[:, None], v_cache)
    scores = jnp.einsum('kbgh,btkh->kbgt', full_qkv[:, :, :group_q], key_now, preferred_element_type=F32) * head_dim ** -0.5
    scores = jnp.where(allowed, scores, -1e30)
    top = jnp.max(scores, axis=-1)
    weights = jnp.exp(scores - top[..., None])
    mixed = jnp.einsum('kbgt,btkh->kbgh', weights.astype(BF), value_now, preferred_element_type=F32)
    stats = jnp.concatenate([top, jnp.sum(weights, axis=-1)], axis=-1)
    stats = jnp.pad(stats, ((0, 0), (0, 0), (0, head_dim - stats.shape[-1])))
    return jnp.concatenate([mixed, stats[:, :, None]], axis=2), key_now, value_now


def decode_combine(mixed):
    heads = mixed.shape[2] - 1
    own = lax.all_to_all(mixed, 'tp', 0, 0)
    top, total = own[:, :, heads, :heads], own[:, :, heads, heads:2 * heads]
    factor = jnp.exp(top - jnp.max(top, axis=0))
    return (jnp.sum(own[:, :, :heads] * factor[..., None], axis=0) / jnp.sum(total * factor, axis=0)[..., None]).astype(BF)


def pass_on(right, left, hop, tp):
    return (lax.ppermute(right, 'tp', [(place, place + 1) for place in range(hop - 1, tp - 1)]),
            lax.ppermute(left, 'tp', [(place, place - 1) for place in range(tp - hop, 0, -1)]))


def gather_w_out(w_out, mesh):
    rows = w_out.shape[0] // (mesh.shape['pair'] * mesh.shape['side'])
    index = lax.axis_index('pair') * mesh.shape['side'] + lax.axis_index('side')
    own = lax.dynamic_slice_in_dim(w_out, index * rows, rows, 0)
    return lax.all_gather(own, ('tp', 'pair', 'side'))


def solution(mesh):
    side_size = mesh.shape['side']
    tp = mesh.shape['tp']
    send_pairs = [(source, (source + 1) % side_size) for source in range(side_size)]
    group_axes = ('pair', 'side')

    def device_fn(x_prompt, s_len, y_tok, c_len, k_cache, v_cache, attn_gain, w_qkv, w_out, mlp_gain, w_gate_up, w_down):
        x = x_prompt[0]
        seq_len, width = x.shape
        group_q, head = w_qkv.shape[3] - 2, w_qkv.shape[4]
        positions = jnp.arange(seq_len)
        keep_mask = (positions < s_len[0])[:, None].astype(BF)
        cos, sin = rope_tables(positions, head)
        cos, sin = jnp.concatenate([cos, cos], -1), jnp.concatenate([-sin, sin], -1)

        w_full = gather_w_out(w_out[0, 0].reshape(group_q * head, width), mesh).reshape(tp, group_q * head, width)
        mixed, key_now, value_now = decode_local(y_tok, c_len, k_cache[0], v_cache[0], attn_gain[0], w_qkv[0])

        w_slots = jnp.transpose(w_qkv[0, :, 0], (1, 0, 2))
        qkv = project_qkv(x, attn_gain, cos, sin, w_slots)
        step, dec = seq_len // CHUNKS, y_tok.shape[0] // CHUNKS
        mine = attend(s_len, qkv, 0, step, step)
        moved = [pass_on(mine, mine, 1, tp)]
        kv_pair = (qkv[group_q:] * keep_mask)[:, :, None]
        kv_by_pos = lax.all_to_all(kv_pair, 'tp', 1, 2, tiled=True)
        w_gate_up, moved[0] = lax.optimization_barrier((w_gate_up, moved[0]))
        moved.append(pass_on(*moved[0], 2, tp))
        gate_up = jnp.transpose(w_gate_up[0], (1, 0, 2))
        qkv, gate_up, moved[1], kv_by_pos, mixed = lax.optimization_barrier((qkv, gate_up, moved[1], kv_by_pos, mixed))
        dctx = decode_combine(mixed)
        moved.append(pass_on(*moved[1], 3, tp))
        ctx = attend(s_len, qkv, step, seq_len - step, seq_len - step)
        ctx, moved[2] = lax.optimization_barrier((ctx, moved[2]))

        done = layer_sums(ctx, dctx.reshape(-1, ctx.shape[1]), mine, [r for r, _ in moved], [l for _, l in moved], x, y_tok, mlp_gain, w_full, gate_up, w_down[0])
        done = done.reshape(CHUNKS, step + dec, width)
        hidden = done[:, :step].reshape(seq_len, width)
        tokens = done[:, step:].reshape(CHUNKS * dec, width)

        kv_recv = lax.ppermute(kv_by_pos, 'side', send_pairs)
        return (hidden[None], tokens, kv_recv[0][None, None], kv_recv[1][None, None], key_now[None], value_now[None])

    cache_spec = P(None, group_axes, 'tp', None, None)
    in_specs = (P(group_axes, None, None), P(group_axes), P(group_axes, None), P(group_axes), cache_spec, cache_spec, P(), P(None, None, 'tp', None, None), P(None, 'tp', None, None, None), P(), P(None, None, None, 'tp'), P(None, 'tp', None))
    out_specs = (P(group_axes, None, None), P(group_axes, None), cache_spec, cache_spec, cache_spec, cache_spec)
    return jax.shard_map(device_fn, mesh=mesh, in_specs=in_specs, out_specs=out_specs, check_vma=False)
```

```python
import functools

import jax
import jax.numpy as jnp
from jax import lax
from jax.experimental import pallas as pl
from jax.experimental.pallas import tpu as pltpu
from jax.sharding import PartitionSpec as P

ROPE_BASE = 10000.0
NORM_EPS = 1e-5
LOG2E = 1.4426950408889634
BF = jnp.bfloat16
F32 = jnp.float32


def rms_norm(hidden, norm_gain):
    hidden_f32 = hidden.astype(F32)
    inv_rms = lax.rsqrt(jnp.mean(hidden_f32 * hidden_f32, axis=-1, keepdims=True) + NORM_EPS)
    return (hidden_f32 * inv_rms * norm_gain.astype(F32)).astype(BF)


def rope_tables(positions, head_dim):
    half_dim = head_dim // 2
    inv_freq = ROPE_BASE ** (-2.0 * jnp.arange(half_dim, dtype=F32) / head_dim)
    angles = positions.astype(F32)[:, None] * inv_freq[None, :]
    return jnp.cos(angles), jnp.sin(angles)


def rope_rotate(vals_f32, positions):
    half_dim = vals_f32.shape[-1] // 2
    cos_table, sin_table = rope_tables(positions, vals_f32.shape[-1])
    cos_table, sin_table = cos_table[:, None, None, :], sin_table[:, None, None, :]
    first_half = vals_f32[..., :half_dim]
    second_half = vals_f32[..., half_dim:]
    return jnp.concatenate([first_half * cos_table - second_half * sin_table, second_half * cos_table + first_half * sin_table], axis=-1)


def qkv_kernel(x_ref, gain_ref, cos_ref, sin_ref, w_ref, o_ref):
    slots = w_ref.shape[0]
    x = x_ref[...].astype(F32)
    inv = lax.rsqrt(jnp.mean(x * x, axis=-1, keepdims=True) + NORM_EPS)
    normed = (x * inv * gain_ref[...].astype(F32)).astype(BF)
    cos, sin = cos_ref[...], sin_ref[...]
    for first in range(0, slots, 2):
        group = range(first, min(first + 2, slots))
        w = jnp.concatenate([w_ref[s] for s in group], axis=-1)
        y = jnp.dot(normed, w, preferred_element_type=F32)
        for n, s in enumerate(group):
            part = y[:, n * 128:(n + 1) * 128]
            if s < slots - 1:
                part = part * cos + pltpu.roll(part, 64, 1) * sin
            o_ref[s] = part.astype(BF)


def project_qkv(x, gain, cos, sin, w, rows_block=256):
    rows, width = x.shape
    slots, _, head = w.shape
    return pl.pallas_call(
        qkv_kernel,
        grid=(rows // rows_block,),
        in_specs=[
            pl.BlockSpec((rows_block, width), lambda i: (i, 0)),
            pl.BlockSpec((1, width), lambda i: (0, 0)),
            pl.BlockSpec((rows_block, head), lambda i: (i, 0)),
            pl.BlockSpec((rows_block, head), lambda i: (i, 0)),
            pl.BlockSpec((slots, width, head), lambda i: (0, 0, 0), pipeline_mode=pl.Buffered(1)),
        ],
        out_specs=pl.BlockSpec((slots, rows_block, head), lambda i: (0, i, 0)),
        out_shape=jax.ShapeDtypeStruct((slots, rows, head), BF),
        cost_estimate=pl.CostEstimate(flops=2 * rows * width * slots * head, bytes_accessed=2 * (rows * width + slots * head * (width + rows)), transcendentals=0),
        name="project_qkv",
    )(x, gain, cos, sin, w)


MESH = pl.DeviceIdType.MESH


def to(device):
    return dict(device_id={'tp': device}, device_id_type=MESH)


def meet_neighbours(t, last):
    barrier = pltpu.get_barrier_semaphore()

    @pl.when(t > 0)
    def _():
        pl.semaphore_signal(barrier, inc=1, **to(t - 1))

    @pl.when(t < last)
    def _():
        pl.semaphore_signal(barrier, inc=1, **to(t + 1))

    @pl.when((t > 0) & (t < last))
    def _():
        pl.semaphore_wait(barrier, 2)

    @pl.when((t == 0) | (t == last))
    def _():
        pl.semaphore_wait(barrier, 1)


class Spread:
    def __init__(self, t, last, own, place, send_sem, recv_sem):
        self.t, self.last, self.own, self.place, self.send_sem, self.recv_sem = t, last, own, place, send_sem, recv_sem

    def copy(self, source, way, first=False):
        return pltpu.make_async_remote_copy(
            src_ref=self.own if first else self.place(source), dst_ref=self.place(source), send_sem=self.send_sem(source, way),
            recv_sem=self.recv_sem(source), **to(self.t + 1 if way == 0 else self.t - 1))

    def start(self):
        @pl.when(self.t < self.last)
        def _():
            self.copy(self.t, 0, True).start()

        @pl.when(self.t > 0)
        def _():
            self.copy(self.t, 1, True).start()

    def hop(self, n):
        t, last = self.t, self.last

        @pl.when(t >= n)
        def _():
            self.copy(t - n, 0).wait_recv()

            @pl.when(t < last)
            def _():
                self.copy(t - n, 0).start()

        @pl.when(t + n <= last)
        def _():
            self.copy(t + n, 1).wait_recv()

            @pl.when(t > 0)
            def _():
                self.copy(t + n, 1).start()

    def finish(self):
        for source in range(self.last + 1):
            @pl.when((source <= self.t) & (self.t < self.last))
            def _(source=source):
                self.copy(source, 0).wait_send()

            @pl.when((source >= self.t) & (self.t > 0))
            def _(source=source):
                self.copy(source, 1).wait_send()


def flash_kernel(block_q, block_k, some, base, slen_ref, q_ref, k_ref, v_ref, *refs):
    o_ref, s_ref, m_ref, l_ref, p_ref, acc_ref = refs[-6:]
    i = pl.program_id(0) + base
    heads, _, head = q_ref.shape
    rows = heads * block_q
    pieces = rows // some
    lanes = block_k // 128
    slen = slen_ref[0]
    scale = head ** -0.5 * LOG2E
    count = (i * block_q + block_q - 1) // block_k + 1

    def cols(j):
        return pl.ds(pl.multiple_of(j * block_k, block_k), block_k)

    @pl.loop(0, count)
    def _(j):
        k = k_ref[0, cols(j), :]
        s_ref[:, cols(j)] = lax.dot_general(q_ref[...].reshape(rows, head), k, (((1,), (1,)), ((), ())), preferred_element_type=F32)
        edge = ((j + 1) * block_k > i * block_q) | ((j + 1) * block_k > k_ref.shape[1] // 2)

        @pl.when(edge)
        def _():
            @pl.loop(0, pieces)
            def _(r):
                here = pl.ds(pl.multiple_of(r * some, some), some)
                q_pos = i * block_q + (r * some) % block_q + lax.broadcasted_iota(jnp.int32, (some, block_k), 0)
                k_pos = j * block_k + lax.broadcasted_iota(jnp.int32, (some, block_k), 1)
                s_ref[here, cols(j)] = jnp.where((k_pos <= q_pos) & (k_pos < slen), s_ref[here, cols(j)], -1e30)

    tall = rows // heads

    @pl.loop(0, heads)
    def _(r):
        here = pl.ds(pl.multiple_of(r * tall, tall), tall)

        def more(j, top):
            s = s_ref[here, cols(j)]
            for n in range(lanes):
                top = jnp.maximum(top, s[:, n * 128:(n + 1) * 128])
            return top

        top = lax.fori_loop(0, count, more, jnp.full((tall, 128), -jnp.inf, F32))
        m_ref[here] = jnp.broadcast_to(jnp.max(top, axis=-1, keepdims=True), (tall, 128))

    l_ref[...] = jnp.zeros_like(l_ref)
    acc_ref[...] = jnp.zeros_like(acc_ref)

    @pl.loop(0, count)
    def _(j):
        @pl.loop(0, pieces, unroll=2)
        def _(r):
            here = pl.ds(pl.multiple_of(r * some, some), some)
            s = s_ref[here, cols(j)]
            m = m_ref[here]
            total = l_ref[here]
            for n in range(lanes):
                w = jnp.exp2((s[:, n * 128:(n + 1) * 128] - m) * scale)
                total = total + w
                p_ref[here, n * 128:(n + 1) * 128] = w.astype(BF)
            l_ref[here] = total

        acc_ref[...] += jnp.dot(p_ref[...], v_ref[0, cols(j), :], preferred_element_type=F32)

    for h in range(heads):
        here = slice(h * block_q, (h + 1) * block_q)
        o_ref[:, h * head:(h + 1) * head] = (acc_ref[here] / jnp.sum(l_ref[here], axis=-1, keepdims=True)).astype(BF)


def attend(slen, qkv, first, count, total, into=None, block_q=256, block_k=512, some=32):
    slots, rows, head = qkv.shape
    heads = slots - 2
    tall = heads * block_q
    base = first // block_q
    place = 0 if into is None else (total - count) // block_q
    more = [] if into is None else [into]
    share = (first + count) ** 2 - first ** 2
    return pl.pallas_call(
        functools.partial(flash_kernel, block_q, block_k, some, base),
        grid_spec=pltpu.PrefetchScalarGridSpec(
            num_scalar_prefetch=1,
            grid=(count // block_q,),
            in_specs=[
                pl.BlockSpec((heads, block_q, head), lambda i, _: (0, i + base, 0)),
                pl.BlockSpec((1, rows, head), lambda i, _: (heads, 0, 0)),
                pl.BlockSpec((1, rows, head), lambda i, _: (heads + 1, 0, 0)),
            ] + [pl.BlockSpec(memory_space=pl.ANY) for _ in more],
            out_specs=pl.BlockSpec((block_q, heads * head), lambda i, _: (i + place, 0)),
            scratch_shapes=[
                pltpu.VMEM((tall, rows), F32),
                pltpu.VMEM((tall, 128), F32),
                pltpu.VMEM((tall, 128), F32),
                pltpu.VMEM((tall, block_k), BF),
                pltpu.VMEM((tall, head), F32),
            ],
        ),
        out_shape=jax.ShapeDtypeStruct((total, heads * head), BF),
        input_output_aliases={4: 0} if more else {},
        cost_estimate=pl.CostEstimate(flops=3 * heads * share * head, bytes_accessed=2 * (2 * heads + 2) * count * head, transcendentals=heads * share // 2),
        name='attend',
    )(slen, qkv, qkv, qkv, *more)


CHUNKS = 4
SUBS = 5
SLOTS = 2
ACCS = 3
TILE = 256
TILE_OUT = 512
OWNED = (11, 3, 3, 11)


def layer_kernel(geo, ctx_hbm, dctx_hbm, mine_hbm, right_hbm, left_hbm, x_hbm, y_hbm, gain_ref, wo_ref, wg_ref, wu_ref, wd_ref, out_hbm, full_hbm, dfull_hbm, hid_hbm,
                 cx, hid, acc, slots, fins, ress, rs_recv, rs_send, credit, ag_recv, ag_send, fin_sem, res_sem,
                 ctx_recv, ctx_send, load_sem, hid_sem):
    width, head_cols, step, dec, ff_tiles, tail = geo
    rows = step + dec
    sub = rows // SUBS
    total = CHUNKS * SUBS
    out_tiles = width // TILE_OUT
    ticks = out_tiles + ff_tiles
    stride = ticks // SUBS
    tp = width // head_cols
    last = tp - 1
    c, j = pl.program_id(0), pl.program_id(1)
    t = lax.axis_index('tp')

    def at(cond):
        return pl.when(cond)

    def step_rows(chunk):
        return pl.ds(pl.multiple_of(chunk * step, 8), step)

    def dec_rows(chunk):
        return pl.ds(pl.multiple_of(chunk * dec, 8), dec)

    def spread(chunk):
        return Spread(t, last, ctx_hbm.at[step_rows(chunk - 1)], lambda source: full_hbm.at[source, chunk - 1],
                      lambda source, way: ctx_send.at[chunk, source, way], lambda source: ctx_recv.at[chunk, source])

    tokens = Spread(t, last, dctx_hbm, lambda source: dfull_hbm.at[source],
                    lambda source, way: ctx_send.at[0, source, way], lambda source: ctx_recv.at[0, source])

    flows = []
    for f, groups in enumerate(OWNED):
        flows.append((f, sum(OWNED[:f]) * 128, groups * 128, max(f, last - f)))

    def rows_of(k):
        return pl.ds(pl.multiple_of(k * sub, 8), sub)

    def part(f, k):
        _, col, cols, _ = flows[f]
        first = pl.multiple_of((k % SUBS) * sub, 8)
        return acc.at[(k // SUBS) % ACCS, pl.ds(first, sub), pl.ds(col, cols)]

    def out_part(f, k):
        _, col, cols, _ = flows[f]
        return out_hbm.at[rows_of(k), pl.ds(col, cols)]

    def rs_copy(f, k, side, device):
        return pltpu.make_async_remote_copy(
            src_ref=part(f, k), dst_ref=slots[f].at[side, k % SLOTS], send_sem=rs_send.at[f, k % SLOTS],
            recv_sem=rs_recv.at[f, side, k % SLOTS], **to(device))

    def ag_copy(f, k, way, first):
        return pltpu.make_async_remote_copy(
            src_ref=fins[f].at[k % SLOTS] if first else out_part(f, k), dst_ref=out_part(f, k), send_sem=ag_send.at[f, way, k % SLOTS],
            recv_sem=ag_recv.at[f, k], **to(t + 1 if way == 0 else t - 1))

    def fin_copy(f, k):
        return pltpu.make_async_copy(fins[f].at[k % SLOTS], out_part(f, k), fin_sem.at[f, k % SLOTS])

    def res_copy(f, k):
        _, col, cols, _ = flows[f]
        return pltpu.make_async_copy(hid_hbm.at[rows_of(k), pl.ds(col, cols)], ress[f].at[k % SLOTS], res_sem.at[f, k % SLOTS])

    def sides(f):
        found = []
        if f < last:
            found.append((0, t > f, t - f, t + 1, t - 1, t < last))
        if f > 0:
            found.append((1, t < f, f - t, t - 1, t + 1, t > 0))
        return found

    def inside(k):
        return (k >= 0) & (k < total)

    def advance(m):
        for f, col, cols, peak in flows:
            for side, there, dist, outer, inner, more in sides(f):
                k = m - peak + dist

                @at(inside(k) & there)
                def _(f=f, side=side, outer=outer, inner=inner, more=more, k=k):
                    @at(more)
                    def _():
                        rs_copy(f, k, side, inner).wait_recv()
                        mine = part(f, k)
                        mine[...] += slots[f][side, k % SLOTS]

                        @at(k + SLOTS < total)
                        def _():
                            pl.semaphore_signal(credit.at[f], inc=1, **to(outer))

                    @at(k >= SLOTS)
                    def _():
                        pl.semaphore_wait(credit.at[f], 1)
                        rs_copy(f, k - SLOTS, side, inner).wait_send()

                    rs_copy(f, k, side, inner).start()

            k = m - peak

            @at(inside(k) & (t == f))
            def _(f=f, k=k):
                both = part(f, k)[...]
                for side, _, _, outer, inner, _ in sides(f):
                    rs_copy(f, k, side, inner).wait_recv()
                    both = both + slots[f][side, k % SLOTS]
                res_copy(f, k).wait()

                @at(k >= SLOTS)
                def _():
                    fin_copy(f, k - SLOTS).wait()
                    for side, _, _, _, _, _ in sides(f):
                        ag_copy(f, k - SLOTS, side, True).wait_send()

                fins[f][k % SLOTS] = (ress[f][k % SLOTS].astype(F32) + both).astype(BF)

                @at(k + SLOTS < total)
                def _():
                    for side, _, _, outer, _, _ in sides(f):
                        pl.semaphore_signal(credit.at[f], inc=1, **to(outer))

        for f, col, cols, peak in flows:
            k = m - peak

            @at(inside(k) & (t == f))
            def _(f=f, k=k):
                for side, _, _, _, _, _ in sides(f):
                    ag_copy(f, k, side, True).start()
                fin_copy(f, k).start()

            @at(inside(k + 1) & (t == f))
            def _(f=f, k=k):
                res_copy(f, k + 1).start()

        for f, col, cols, peak in flows:
            for side, there, dist, outer, inner, more in sides(f):
                a = m - peak - dist

                @at(inside(a) & there)
                def _(f=f, side=side, more=more, a=a):
                    ag_copy(f, a, side, False).wait_recv()

                    @at(more)
                    def _():
                        @at(a >= SLOTS)
                        def _():
                            ag_copy(f, a - SLOTS, side, False).wait_send()

                        ag_copy(f, a, side, False).start()

    @at((c == 0) & (j == 0))
    def _():
        meet_neighbours(t, last)
        tokens.start()
        spread(1).start()
        cx[...] = jnp.zeros_like(cx)
        hid[...] = jnp.zeros_like(hid)
    @at((c > 0) & (j % stride == 0) & (j < stride * SUBS))
    def _():
        advance(SUBS * (c - 1) + j // stride)

    for n in range(1, last + 1):
        @at((c + 1 < CHUNKS) & (j == ticks * n // (last + 1) + 1))
        def _(n=n):
            spread(c + 1).hop(n)
            if n == last:
                @at(c + 2 < CHUNKS)
                def _():
                    spread(c + 2).start()

    @at(j == 0)
    def _():
        loads = [
            pltpu.make_async_copy(x_hbm.at[step_rows(c)], hid.at[pl.ds(0, step)], load_sem.at[2 * tp]),
            pltpu.make_async_copy(y_hbm.at[dec_rows(c)], hid.at[pl.ds(step, dec)], load_sem.at[2 * tp + 1]),
        ]
        for copy in loads:
            copy.start()
        for s in range(tp):
            head_range = pl.ds(s * head_cols, head_cols)
            where = cx.at[pl.ds(0, step), head_range]

            for device in range(tp):
                piece = mine_hbm if device == s else right_hbm[device - s - 1] if device > s else left_hbm[s - device - 1]

                @at((c == 0) & (t == device))
                def _(s=s, where=where, piece=piece):
                    pltpu.make_async_copy(piece, where, load_sem.at[s]).start()

            @at((c > 0) & (t == s))
            def _(s=s, where=where):
                pltpu.make_async_copy(ctx_hbm.at[step_rows(c - 1)], where, load_sem.at[s]).start()

            @at((c > 0) & (t != s))
            def _(s=s, where=where):
                pltpu.make_async_copy(full_hbm.at[s, c - 1], where, load_sem.at[s]).start()

        @at(c == 0)
        def _():
            for n in range(1, last + 1):
                tokens.hop(n)

        for s in range(tp):
            head_range = pl.ds(s * head_cols, head_cols)
            tail_rows = cx.at[pl.ds(step, dec), head_range]

            @at(t == s)
            def _(s=s, tail_rows=tail_rows):
                pltpu.make_async_copy(dctx_hbm.at[dec_rows(c)], tail_rows, load_sem.at[tp + s]).start()

            @at(t != s)
            def _(s=s, tail_rows=tail_rows):
                pltpu.make_async_copy(dfull_hbm.at[s, dec_rows(c)], tail_rows, load_sem.at[tp + s]).start()

        for s in range(tp):
            head_range = pl.ds(s * head_cols, head_cols)
            pltpu.make_async_copy(mine_hbm, cx.at[pl.ds(0, step), head_range], load_sem.at[s]).wait()
            pltpu.make_async_copy(dctx_hbm.at[dec_rows(c)], cx.at[pl.ds(step, dec), head_range], load_sem.at[tp + s]).wait()
        for copy in loads:
            copy.wait()

    @at(j < out_tiles)
    def _():
        mixed = None
        for s in range(tp):
            one = jnp.dot(cx[:, s * head_cols:(s + 1) * head_cols], wo_ref[s], preferred_element_type=F32)
            mixed = one if mixed is None else mixed + one
        cols = pl.ds(pl.multiple_of(j * TILE_OUT, TILE_OUT), TILE_OUT)
        hid[:, cols] = (hid[:, cols].astype(F32) + mixed).astype(BF)

    hid_copy = pltpu.make_async_copy(hid.at[pl.ds(0, rows)], hid_hbm.at[pl.ds(pl.multiple_of(c * rows, 8), rows)], hid_sem)

    @at(j == out_tiles)
    def _():
        hid_copy.start()
        block = hid.shape[0] // 11

        @pl.loop(0, 11)
        def _(b):
            some = pl.ds(pl.multiple_of(b * block, 16), block)
            h = hid[some].astype(F32)
            inv = lax.rsqrt(jnp.mean(h * h, axis=-1, keepdims=True) + NORM_EPS)
            cx[some] = (h * inv * gain_ref[...].astype(F32)).astype(BF)
            acc[c % ACCS, some] = jnp.zeros((block, width), F32)

    @at(j >= out_tiles)
    def _():
        gate = jnp.dot(cx[...], wg_ref[0], preferred_element_type=F32)
        up = jnp.dot(cx[...], wu_ref[0], preferred_element_type=F32)
        act = (jax.nn.silu(gate) * up).astype(BF)
        which = c % ACCS

        @at(j < ticks - 1)
        def _():
            acc[which] += jnp.dot(act, wd_ref[...], preferred_element_type=F32)

        @at(j == ticks - 1)
        def _():
            acc[which] += jnp.dot(act[:, :tail], wd_ref[:tail], preferred_element_type=F32)
            hid_copy.wait()

    @at((c == CHUNKS - 1) & (j == ticks - 1))
    def _():
        @pl.loop(SUBS * (CHUNKS - 1), total + 2 * last)
        def _(m):
            advance(m)

        for f, col, cols, peak in flows:
            for side, there, dist, outer, inner, more in sides(f):
                @at(there)
                def _(f=f, side=side, inner=inner, more=more):
                    for k in range(total - SLOTS, total):
                        rs_copy(f, k, side, inner).wait_send()

                    @at(more)
                    def _():
                        for k in range(total - SLOTS, total):
                            ag_copy(f, k, side, False).wait_send()

            @at(t == f)
            def _(f=f):
                for k in range(total - SLOTS, total):
                    fin_copy(f, k).wait()
                    for side, _, _, _, _, _ in sides(f):
                        ag_copy(f, k, side, True).wait_send()

        tokens.finish()
        for chunk in range(1, CHUNKS):
            spread(chunk).finish()


def layer_sums(ctx, dctx, mine, right, left, x, y, gain, w_full, w_gate_up, w_down):
    head_cols = ctx.shape[1]
    seq, width = x.shape
    step, dec = seq // CHUNKS, y.shape[0] // CHUNKS
    rows = step + dec
    ff = w_down.shape[0]
    ff_tiles = pl.cdiv(ff, TILE)
    tail = ff - (ff_tiles - 1) * TILE
    out_tiles = width // TILE_OUT
    tp = width // head_cols
    pad = (rows + 15) // 16 * 16
    sub = rows // SUBS
    total = CHUNKS * SUBS
    geo = (width, head_cols, step, dec, ff_tiles, tail)
    def ff_index(j):
        return jnp.maximum(j - out_tiles, 0)

    any_spec = pl.BlockSpec(memory_space=pl.ANY)
    flops = 2 * CHUNKS * rows * width * (width + 3 * ff)
    moved = 2 * CHUNKS * (width * width + 3 * width * ff)
    return pl.pallas_call(
        functools.partial(layer_kernel, geo),
        grid=(CHUNKS, out_tiles + ff_tiles),
        in_specs=[
            any_spec, any_spec, any_spec, [any_spec] * (tp - 1), [any_spec] * (tp - 1), any_spec, any_spec,
            pl.BlockSpec((1, width), lambda c, j: (0, 0)),
            pl.BlockSpec((tp, head_cols, TILE_OUT), lambda c, j: (0, 0, jnp.minimum(j, out_tiles - 1))),
            pl.BlockSpec((1, width, TILE), lambda c, j: (0, 0, ff_index(j))),
            pl.BlockSpec((1, width, TILE), lambda c, j: (1, 0, ff_index(j))),
            pl.BlockSpec((TILE, width), lambda c, j: (ff_index(j), 0)),
        ],
        out_specs=[any_spec, any_spec, any_spec, any_spec],
        out_shape=[
            jax.ShapeDtypeStruct((CHUNKS * rows, width), BF),
            jax.ShapeDtypeStruct((tp, CHUNKS - 1, step, head_cols), BF),
            jax.ShapeDtypeStruct((tp,) + dctx.shape, BF),
            jax.ShapeDtypeStruct((CHUNKS * rows, width), BF),
        ],
        scratch_shapes=[
            pltpu.VMEM((pad, width), BF),
            pltpu.VMEM((pad, width), BF),
            pltpu.VMEM((ACCS, pad, width), F32),
            [pltpu.VMEM((2, SLOTS, sub, groups * 128), F32) for groups in OWNED],
            [pltpu.VMEM((SLOTS, sub, groups * 128), BF) for groups in OWNED],
            [pltpu.VMEM((SLOTS, sub, groups * 128), BF) for groups in OWNED],
            pltpu.SemaphoreType.DMA((tp, 2, SLOTS)),
            pltpu.SemaphoreType.DMA((tp, SLOTS)),
            pltpu.SemaphoreType.REGULAR((tp,)),
            pltpu.SemaphoreType.DMA((tp, total)),
            pltpu.SemaphoreType.DMA((tp, 2, SLOTS)),
            pltpu.SemaphoreType.DMA((tp, SLOTS)),
            pltpu.SemaphoreType.DMA((tp, SLOTS)),
            pltpu.SemaphoreType.DMA((CHUNKS, tp)),
            pltpu.SemaphoreType.DMA((CHUNKS, tp, 2)),
            pltpu.SemaphoreType.DMA((2 * tp + 2,)),
            pltpu.SemaphoreType.DMA(()),
        ],
        compiler_params=pltpu.CompilerParams(collective_id=0, has_side_effects=True, vmem_limit_bytes=67000000, dimension_semantics=('arbitrary', 'arbitrary')),
        cost_estimate=pl.CostEstimate(flops=flops, bytes_accessed=moved, transcendentals=0),
        name='layer_sums',
    )(ctx, dctx, mine, right, left, x, y, gain, w_full, w_gate_up, w_gate_up, w_down)[0]


def decode_project(tokens, cache_lens, gain, w_qkv):
    group_q = w_qkv.shape[2] - 2
    normed = rms_norm(tokens, gain)
    projected = jnp.einsum('bd,dkjh->bkjh', normed, w_qkv, preferred_element_type=F32)
    rotated = rope_rotate(projected[:, :, :group_q + 1], cache_lens)
    local_qkv = jnp.concatenate([rotated, projected[:, :, group_q + 1:]], axis=2).astype(BF)[:, 0]
    return local_qkv


def decode_local(full_qkv, cache_lens, k_cache, v_cache):
    group_q, head_dim = full_qkv.shape[2] - 2, full_qkv.shape[3]
    cache_local = k_cache.shape[1]
    cache_pos = lax.axis_index('tp') * cache_local + jnp.arange(cache_local)
    write_mask = (cache_pos[None, :] == cache_lens[:, None])[:, :, None, None]
    allowed = (cache_pos[None, :] <= cache_lens[:, None])[None, :, None, :]
    key_now = jnp.where(write_mask, jnp.moveaxis(full_qkv[:, :, group_q], 0, 1)[:, None], k_cache)
    value_now = jnp.where(write_mask, jnp.moveaxis(full_qkv[:, :, group_q + 1], 0, 1)[:, None], v_cache)
    scores = jnp.einsum('kbgh,btkh->kbgt', full_qkv[:, :, :group_q], key_now, preferred_element_type=F32) * head_dim ** -0.5
    scores = jnp.where(allowed, scores, -1e30)
    top = jnp.max(scores, axis=-1)
    weights = jnp.exp(scores - top[..., None])
    mixed = jnp.einsum('kbgt,btkh->kbgh', weights.astype(BF), value_now, preferred_element_type=F32)
    stats = jnp.concatenate([top, jnp.sum(weights, axis=-1)], axis=-1)
    stats = jnp.pad(stats, ((0, 0), (0, 0), (0, head_dim - stats.shape[-1])))
    return jnp.concatenate([mixed, stats[:, :, None]], axis=2), key_now, value_now


def decode_combine(own):
    heads = own.shape[2] - 1
    top, total = own[:, :, heads, :heads], own[:, :, heads, heads:2 * heads]
    factor = jnp.exp(top - jnp.max(top, axis=0))
    return (jnp.sum(own[:, :, :heads] * factor[..., None], axis=0) / jnp.sum(total * factor, axis=0)[..., None]).astype(BF)


def pass_on(right, left, hop, tp):
    return (lax.ppermute(right, 'tp', [(place, place + 1) for place in range(hop - 1, tp - 1)]),
            lax.ppermute(left, 'tp', [(place, place - 1) for place in range(tp - hop, 0, -1)]))


def gather_w_out(w_out, mesh):
    rows = w_out.shape[0] // (mesh.shape['pair'] * mesh.shape['side'])
    index = lax.axis_index('pair') * mesh.shape['side'] + lax.axis_index('side')
    own = lax.dynamic_slice_in_dim(w_out, index * rows, rows, 0)
    return lax.all_gather(own, ('tp', 'pair', 'side'))


def solution(mesh):
    side_size = mesh.shape['side']
    tp = mesh.shape['tp']
    send_pairs = [(source, (source + 1) % side_size) for source in range(side_size)]
    group_axes = ('pair', 'side')

    def device_fn(x_prompt, s_len, y_tok, c_len, k_cache, v_cache, attn_gain, w_qkv, w_out, mlp_gain, w_gate_up, w_down):
        x = x_prompt[0]
        seq_len, width = x.shape
        group_q, head = w_qkv.shape[3] - 2, w_qkv.shape[4]
        positions = jnp.arange(seq_len)
        keep_mask = (positions < s_len[0])[:, None].astype(BF)
        cos, sin = rope_tables(positions, head)
        cos, sin = jnp.concatenate([cos, cos], -1), jnp.concatenate([-sin, sin], -1)

        w_full = gather_w_out(w_out[0, 0].reshape(group_q * head, width), mesh).reshape(tp, group_q * head, width)
        local_qkv = decode_project(y_tok, c_len, attn_gain[0], w_qkv[0])
        local_qkv, x = lax.optimization_barrier((local_qkv, x))
        full_qkv = lax.all_to_all(jnp.broadcast_to(local_qkv, (tp,) + local_qkv.shape), 'tp', 0, 0)

        w_slots = jnp.transpose(w_qkv[0, :, 0], (1, 0, 2))
        qkv = project_qkv(x, attn_gain, cos, sin, w_slots)
        qkv, full_qkv = lax.optimization_barrier((qkv, full_qkv))
        step, dec = seq_len // CHUNKS, y_tok.shape[0] // CHUNKS
        mine = attend(s_len, qkv, 0, step, step)
        moved = [pass_on(mine, mine, 1, tp)]
        kv_pair = qkv[group_q:] * keep_mask
        full_qkv, mine = lax.optimization_barrier((full_qkv, mine))
        mixed, key_now, value_now = decode_local(full_qkv, c_len, k_cache[0], v_cache[0])
        kv_near = lax.ppermute(kv_pair, 'side', send_pairs)
        w_gate_up, moved[0], mixed = lax.optimization_barrier((w_gate_up, moved[0], mixed))
        mixed = lax.all_to_all(mixed, 'tp', 0, 0)
        moved.append(pass_on(*moved[0], 2, tp))
        gate_up = jnp.transpose(w_gate_up[0], (1, 0, 2))
        qkv, gate_up, moved[1], mixed, kv_near = lax.optimization_barrier((qkv, gate_up, moved[1], mixed, kv_near))
        dctx = decode_combine(mixed)
        kv_recv = lax.all_to_all(kv_near[:, :, None], 'tp', 1, 2, tiled=True)
        moved.append(pass_on(*moved[1], 3, tp))
        ctx = attend(s_len, qkv, step, seq_len - step, seq_len - step)
        ctx, moved[2], kv_recv = lax.optimization_barrier((ctx, moved[2], kv_recv))

        done = layer_sums(ctx, dctx.reshape(-1, ctx.shape[1]), mine, [r for r, _ in moved], [l for _, l in moved], x, y_tok, mlp_gain, w_full, gate_up, w_down[0])
        done = done.reshape(CHUNKS, step + dec, width)
        hidden = done[:, :step].reshape(seq_len, width)
        tokens = done[:, step:].reshape(CHUNKS * dec, width)

        return (hidden[None], tokens, kv_recv[0][None, None], kv_recv[1][None, None], key_now[None], value_now[None])

    cache_spec = P(None, group_axes, 'tp', None, None)
    in_specs = (P(group_axes, None, None), P(group_axes), P(group_axes, None), P(group_axes), cache_spec, cache_spec, P(), P(None, None, 'tp', None, None), P(None, 'tp', None, None, None), P(), P(None, None, None, 'tp'), P(None, 'tp', None))
    out_specs = (P(group_axes, None, None), P(group_axes, None), cache_spec, cache_spec, cache_spec, cache_spec)
    return jax.shard_map(device_fn, mesh=mesh, in_specs=in_specs, out_specs=out_specs, check_vma=False)
```

```python
import functools

import jax
import jax.numpy as jnp
from jax import lax
from jax.experimental import pallas as pl
from jax.experimental.pallas import tpu as pltpu
from jax.sharding import PartitionSpec as P

ROPE_BASE = 10000.0
NORM_EPS = 1e-5
LOG2E = 1.4426950408889634
BF = jnp.bfloat16
F32 = jnp.float32


def rms_norm(hidden, norm_gain):
    hidden_f32 = hidden.astype(F32)
    inv_rms = lax.rsqrt(jnp.mean(hidden_f32 * hidden_f32, axis=-1, keepdims=True) + NORM_EPS)
    return (hidden_f32 * inv_rms * norm_gain.astype(F32)).astype(BF)


def rope_tables(positions, head_dim):
    half_dim = head_dim // 2
    inv_freq = ROPE_BASE ** (-2.0 * jnp.arange(half_dim, dtype=F32) / head_dim)
    angles = positions.astype(F32)[:, None] * inv_freq[None, :]
    return jnp.cos(angles), jnp.sin(angles)


def rope_rotate(vals_f32, positions):
    half_dim = vals_f32.shape[-1] // 2
    cos_table, sin_table = rope_tables(positions, vals_f32.shape[-1])
    cos_table, sin_table = cos_table[:, None, None, :], sin_table[:, None, None, :]
    first_half = vals_f32[..., :half_dim]
    second_half = vals_f32[..., half_dim:]
    return jnp.concatenate([first_half * cos_table - second_half * sin_table, second_half * cos_table + first_half * sin_table], axis=-1)


def qkv_kernel(x_ref, gain_ref, cos_ref, sin_ref, w_ref, o_ref):
    slots = w_ref.shape[0]
    x = x_ref[...].astype(F32)
    inv = lax.rsqrt(jnp.mean(x * x, axis=-1, keepdims=True) + NORM_EPS)
    normed = (x * inv * gain_ref[...].astype(F32)).astype(BF)
    cos, sin = cos_ref[...], sin_ref[...]
    for first in range(0, slots, 2):
        group = range(first, min(first + 2, slots))
        w = jnp.concatenate([w_ref[s] for s in group], axis=-1)
        y = jnp.dot(normed, w, preferred_element_type=F32)
        for n, s in enumerate(group):
            part = y[:, n * 128:(n + 1) * 128]
            if s < slots - 1:
                part = part * cos + pltpu.roll(part, 64, 1) * sin
            o_ref[s] = part.astype(BF)


def project_qkv(x, gain, cos, sin, w, rows_block=512):
    rows, width = x.shape
    slots, _, head = w.shape
    return pl.pallas_call(
        qkv_kernel,
        grid=(rows // rows_block,),
        in_specs=[
            pl.BlockSpec((rows_block, width), lambda i: (i, 0)),
            pl.BlockSpec((1, width), lambda i: (0, 0)),
            pl.BlockSpec((rows_block, head), lambda i: (i, 0)),
            pl.BlockSpec((rows_block, head), lambda i: (i, 0)),
            pl.BlockSpec((slots, width, head), lambda i: (0, 0, 0), pipeline_mode=pl.Buffered(1)),
        ],
        out_specs=pl.BlockSpec((slots, rows_block, head), lambda i: (0, i, 0)),
        out_shape=jax.ShapeDtypeStruct((slots, rows, head), BF),
        cost_estimate=pl.CostEstimate(flops=2 * rows * width * slots * head, bytes_accessed=2 * (rows * width + slots * head * (width + rows)), transcendentals=0),
        name="project_qkv",
    )(x, gain, cos, sin, w)


MESH = pl.DeviceIdType.MESH


def to(device):
    return dict(device_id={'tp': device}, device_id_type=MESH)


def meet_neighbours(t, last):
    barrier = pltpu.get_barrier_semaphore()

    @pl.when(t > 0)
    def _():
        pl.semaphore_signal(barrier, inc=1, **to(t - 1))

    @pl.when(t < last)
    def _():
        pl.semaphore_signal(barrier, inc=1, **to(t + 1))

    @pl.when((t > 0) & (t < last))
    def _():
        pl.semaphore_wait(barrier, 2)

    @pl.when((t == 0) | (t == last))
    def _():
        pl.semaphore_wait(barrier, 1)


class Spread:
    def __init__(self, t, last, own, place, send_sem, recv_sem):
        self.t, self.last, self.own, self.place, self.send_sem, self.recv_sem = t, last, own, place, send_sem, recv_sem

    def copy(self, source, way, first=False):
        return pltpu.make_async_remote_copy(
            src_ref=self.own if first else self.place(source), dst_ref=self.place(source), send_sem=self.send_sem(source, way),
            recv_sem=self.recv_sem(source), **to(self.t + 1 if way == 0 else self.t - 1))

    def start(self):
        @pl.when(self.t < self.last)
        def _():
            self.copy(self.t, 0, True).start()

        @pl.when(self.t > 0)
        def _():
            self.copy(self.t, 1, True).start()

    def hop(self, n):
        t, last = self.t, self.last

        @pl.when(t >= n)
        def _():
            self.copy(t - n, 0).wait_recv()

            @pl.when(t < last)
            def _():
                self.copy(t - n, 0).start()

        @pl.when(t + n <= last)
        def _():
            self.copy(t + n, 1).wait_recv()

            @pl.when(t > 0)
            def _():
                self.copy(t + n, 1).start()

    def finish(self):
        for source in range(self.last + 1):
            @pl.when((source <= self.t) & (self.t < self.last))
            def _(source=source):
                self.copy(source, 0).wait_send()

            @pl.when((source >= self.t) & (self.t > 0))
            def _(source=source):
                self.copy(source, 1).wait_send()


def flash_kernel(block_q, block_k, some, base, slen_ref, q_ref, k_ref, v_ref, *refs):
    o_ref, s_ref, m_ref, l_ref, p_ref, acc_ref = refs[-6:]
    i = pl.program_id(0) + base
    heads, _, head = q_ref.shape
    rows = heads * block_q
    pieces = rows // some
    lanes = block_k // 128
    slen = slen_ref[0]
    scale = head ** -0.5 * LOG2E
    count = (i * block_q + block_q - 1) // block_k + 1

    def cols(j):
        return pl.ds(pl.multiple_of(j * block_k, block_k), block_k)

    @pl.loop(0, count)
    def _(j):
        k = k_ref[0, cols(j), :]
        s_ref[:, cols(j)] = lax.dot_general(q_ref[...].reshape(rows, head), k, (((1,), (1,)), ((), ())), preferred_element_type=F32)
        edge = ((j + 1) * block_k > i * block_q) | ((j + 1) * block_k > k_ref.shape[1] // 2)

        @pl.when(edge)
        def _():
            @pl.loop(0, pieces)
            def _(r):
                here = pl.ds(pl.multiple_of(r * some, some), some)
                q_pos = i * block_q + (r * some) % block_q + lax.broadcasted_iota(jnp.int32, (some, block_k), 0)
                k_pos = j * block_k + lax.broadcasted_iota(jnp.int32, (some, block_k), 1)
                s_ref[here, cols(j)] = jnp.where((k_pos <= q_pos) & (k_pos < slen), s_ref[here, cols(j)], -1e30)

    tall = rows // heads

    @pl.loop(0, heads)
    def _(r):
        here = pl.ds(pl.multiple_of(r * tall, tall), tall)

        def more(j, top):
            s = s_ref[here, cols(j)]
            for n in range(lanes):
                top = jnp.maximum(top, s[:, n * 128:(n + 1) * 128])
            return top

        top = lax.fori_loop(0, count, more, jnp.full((tall, 128), -jnp.inf, F32))
        m_ref[here] = jnp.broadcast_to(jnp.max(top, axis=-1, keepdims=True), (tall, 128))

    l_ref[...] = jnp.zeros_like(l_ref)
    acc_ref[...] = jnp.zeros_like(acc_ref)

    @pl.loop(0, count)
    def _(j):
        @pl.loop(0, pieces, unroll=2)
        def _(r):
            here = pl.ds(pl.multiple_of(r * some, some), some)
            s = s_ref[here, cols(j)]
            m = m_ref[here]
            total = l_ref[here]
            for n in range(lanes):
                w = jnp.exp2((s[:, n * 128:(n + 1) * 128] - m) * scale)
                total = total + w
                p_ref[here, n * 128:(n + 1) * 128] = w.astype(BF)
            l_ref[here] = total

        acc_ref[...] += jnp.dot(p_ref[...], v_ref[0, cols(j), :], preferred_element_type=F32)

    for h in range(heads):
        here = slice(h * block_q, (h + 1) * block_q)
        o_ref[:, h * head:(h + 1) * head] = (acc_ref[here] / jnp.sum(l_ref[here], axis=-1, keepdims=True)).astype(BF)


def attend(slen, qkv, first, count, total, into=None, block_q=256, block_k=512, some=32):
    slots, rows, head = qkv.shape
    heads = slots - 2
    tall = heads * block_q
    base = first // block_q
    place = 0 if into is None else (total - count) // block_q
    more = [] if into is None else [into]
    share = (first + count) ** 2 - first ** 2
    return pl.pallas_call(
        functools.partial(flash_kernel, block_q, block_k, some, base),
        grid_spec=pltpu.PrefetchScalarGridSpec(
            num_scalar_prefetch=1,
            grid=(count // block_q,),
            in_specs=[
                pl.BlockSpec((heads, block_q, head), lambda i, _: (0, i + base, 0)),
                pl.BlockSpec((1, rows, head), lambda i, _: (heads, 0, 0)),
                pl.BlockSpec((1, rows, head), lambda i, _: (heads + 1, 0, 0)),
            ] + [pl.BlockSpec(memory_space=pl.ANY) for _ in more],
            out_specs=pl.BlockSpec((block_q, heads * head), lambda i, _: (i + place, 0)),
            scratch_shapes=[
                pltpu.VMEM((tall, rows), F32),
                pltpu.VMEM((tall, 128), F32),
                pltpu.VMEM((tall, 128), F32),
                pltpu.VMEM((tall, block_k), BF),
                pltpu.VMEM((tall, head), F32),
            ],
        ),
        out_shape=jax.ShapeDtypeStruct((total, heads * head), BF),
        input_output_aliases={4: 0} if more else {},
        cost_estimate=pl.CostEstimate(flops=3 * heads * share * head, bytes_accessed=2 * (2 * heads + 2) * count * head, transcendentals=heads * share // 2),
        name='attend',
    )(slen, qkv, qkv, qkv, *more)


CHUNKS = 4
SUBS = 5
SLOTS = 2
ACCS = 3
TILE = 256
TILE_OUT = 512
OWNED = (11, 3, 3, 11)


def layer_kernel(geo, ctx_hbm, dctx_hbm, mine_hbm, right_hbm, left_hbm, x_hbm, y_hbm, gain_ref, wo_ref, wg_ref, wu_ref, wd_ref, out_hbm, full_hbm, dfull_hbm, hid_hbm,
                 cx, hid, acc, slots, fins, ress, rs_recv, rs_send, credit, ag_recv, ag_send, fin_sem, res_sem,
                 ctx_recv, ctx_send, load_sem, hid_sem):
    width, head_cols, step, dec, ff_tiles, tail = geo
    rows = step + dec
    sub = rows // SUBS
    total = CHUNKS * SUBS
    out_tiles = width // TILE_OUT
    ticks = out_tiles + ff_tiles
    stride = ticks // SUBS
    tp = width // head_cols
    last = tp - 1
    c, j = pl.program_id(0), pl.program_id(1)
    t = lax.axis_index('tp')

    def at(cond):
        return pl.when(cond)

    def step_rows(chunk):
        return pl.ds(pl.multiple_of(chunk * step, 8), step)

    def dec_rows(chunk):
        return pl.ds(pl.multiple_of(chunk * dec, 8), dec)

    def spread(chunk):
        return Spread(t, last, ctx_hbm.at[step_rows(chunk - 1)], lambda source: full_hbm.at[source, chunk - 1],
                      lambda source, way: ctx_send.at[chunk, source, way], lambda source: ctx_recv.at[chunk, source])

    tokens = Spread(t, last, dctx_hbm, lambda source: dfull_hbm.at[source],
                    lambda source, way: ctx_send.at[0, source, way], lambda source: ctx_recv.at[0, source])

    flows = []
    for f, groups in enumerate(OWNED):
        flows.append((f, sum(OWNED[:f]) * 128, groups * 128, max(f, last - f)))

    def rows_of(k):
        return pl.ds(pl.multiple_of(k * sub, 8), sub)

    def part(f, k):
        _, col, cols, _ = flows[f]
        first = pl.multiple_of((k % SUBS) * sub, 8)
        return acc.at[(k // SUBS) % ACCS, pl.ds(first, sub), pl.ds(col, cols)]

    def out_part(f, k):
        _, col, cols, _ = flows[f]
        return out_hbm.at[rows_of(k), pl.ds(col, cols)]

    def rs_copy(f, k, side, device):
        return pltpu.make_async_remote_copy(
            src_ref=part(f, k), dst_ref=slots[f].at[side, k % SLOTS], send_sem=rs_send.at[f, k % SLOTS],
            recv_sem=rs_recv.at[f, side, k % SLOTS], **to(device))

    def ag_copy(f, k, way, first):
        return pltpu.make_async_remote_copy(
            src_ref=fins[f].at[k % SLOTS] if first else out_part(f, k), dst_ref=out_part(f, k), send_sem=ag_send.at[f, way, k % SLOTS],
            recv_sem=ag_recv.at[f, k], **to(t + 1 if way == 0 else t - 1))

    def fin_copy(f, k):
        return pltpu.make_async_copy(fins[f].at[k % SLOTS], out_part(f, k), fin_sem.at[f, k % SLOTS])

    def res_copy(f, k):
        _, col, cols, _ = flows[f]
        return pltpu.make_async_copy(hid_hbm.at[rows_of(k), pl.ds(col, cols)], ress[f].at[k % SLOTS], res_sem.at[f, k % SLOTS])

    def sides(f):
        found = []
        if f < last:
            found.append((0, t > f, t - f, t + 1, t - 1, t < last))
        if f > 0:
            found.append((1, t < f, f - t, t - 1, t + 1, t > 0))
        return found

    def inside(k):
        return (k >= 0) & (k < total)

    def advance(m):
        for f, col, cols, peak in flows:
            for side, there, dist, outer, inner, more in sides(f):
                k = m - peak + dist

                @at(inside(k) & there)
                def _(f=f, side=side, outer=outer, inner=inner, more=more, k=k):
                    @at(more)
                    def _():
                        rs_copy(f, k, side, inner).wait_recv()
                        mine = part(f, k)
                        mine[...] += slots[f][side, k % SLOTS]

                        @at(k + SLOTS < total)
                        def _():
                            pl.semaphore_signal(credit.at[f], inc=1, **to(outer))

                    @at(k >= SLOTS)
                    def _():
                        pl.semaphore_wait(credit.at[f], 1)
                        rs_copy(f, k - SLOTS, side, inner).wait_send()

                    rs_copy(f, k, side, inner).start()

            k = m - peak

            @at(inside(k) & (t == f))
            def _(f=f, k=k):
                both = part(f, k)[...]
                for side, _, _, outer, inner, _ in sides(f):
                    rs_copy(f, k, side, inner).wait_recv()
                    both = both + slots[f][side, k % SLOTS]
                res_copy(f, k).wait()

                @at(k >= SLOTS)
                def _():
                    fin_copy(f, k - SLOTS).wait()
                    for side, _, _, _, _, _ in sides(f):
                        ag_copy(f, k - SLOTS, side, True).wait_send()

                fins[f][k % SLOTS] = (ress[f][k % SLOTS].astype(F32) + both).astype(BF)

                @at(k + SLOTS < total)
                def _():
                    for side, _, _, outer, _, _ in sides(f):
                        pl.semaphore_signal(credit.at[f], inc=1, **to(outer))

        for f, col, cols, peak in flows:
            k = m - peak

            @at(inside(k) & (t == f))
            def _(f=f, k=k):
                for side, _, _, _, _, _ in sides(f):
                    ag_copy(f, k, side, True).start()
                fin_copy(f, k).start()

            @at(inside(k + 1) & (t == f))
            def _(f=f, k=k):
                res_copy(f, k + 1).start()

        for f, col, cols, peak in flows:
            for side, there, dist, outer, inner, more in sides(f):
                a = m - peak - dist

                @at(inside(a) & there)
                def _(f=f, side=side, more=more, a=a):
                    ag_copy(f, a, side, False).wait_recv()

                    @at(more)
                    def _():
                        @at(a >= SLOTS)
                        def _():
                            ag_copy(f, a - SLOTS, side, False).wait_send()

                        ag_copy(f, a, side, False).start()

    @at((c == 0) & (j == 0))
    def _():
        meet_neighbours(t, last)
        tokens.start()
        spread(1).start()
        cx[...] = jnp.zeros_like(cx)
        hid[...] = jnp.zeros_like(hid)
    @at((c > 0) & (j % stride == 0) & (j < stride * SUBS))
    def _():
        advance(SUBS * (c - 1) + j // stride)

    for n in range(1, last + 1):
        @at((c + 1 < CHUNKS) & (j == ticks * n // (last + 1) + 1))
        def _(n=n):
            spread(c + 1).hop(n)
            if n == last:
                @at(c + 2 < CHUNKS)
                def _():
                    spread(c + 2).start()

    @at(j == 0)
    def _():
        loads = [
            pltpu.make_async_copy(x_hbm.at[step_rows(c)], hid.at[pl.ds(0, step)], load_sem.at[2 * tp]),
            pltpu.make_async_copy(y_hbm.at[dec_rows(c)], hid.at[pl.ds(step, dec)], load_sem.at[2 * tp + 1]),
        ]
        for copy in loads:
            copy.start()
        for s in range(tp):
            head_range = pl.ds(s * head_cols, head_cols)
            where = cx.at[pl.ds(0, step), head_range]

            for device in range(tp):
                piece = mine_hbm if device == s else right_hbm[device - s - 1] if device > s else left_hbm[s - device - 1]

                @at((c == 0) & (t == device))
                def _(s=s, where=where, piece=piece):
                    pltpu.make_async_copy(piece, where, load_sem.at[s]).start()

            @at((c > 0) & (t == s))
            def _(s=s, where=where):
                pltpu.make_async_copy(ctx_hbm.at[step_rows(c - 1)], where, load_sem.at[s]).start()

            @at((c > 0) & (t != s))
            def _(s=s, where=where):
                pltpu.make_async_copy(full_hbm.at[s, c - 1], where, load_sem.at[s]).start()

        @at(c == 0)
        def _():
            for n in range(1, last + 1):
                tokens.hop(n)

        for s in range(tp):
            head_range = pl.ds(s * head_cols, head_cols)
            tail_rows = cx.at[pl.ds(step, dec), head_range]

            @at(t == s)
            def _(s=s, tail_rows=tail_rows):
                pltpu.make_async_copy(dctx_hbm.at[dec_rows(c)], tail_rows, load_sem.at[tp + s]).start()

            @at(t != s)
            def _(s=s, tail_rows=tail_rows):
                pltpu.make_async_copy(dfull_hbm.at[s, dec_rows(c)], tail_rows, load_sem.at[tp + s]).start()

        for s in range(tp):
            head_range = pl.ds(s * head_cols, head_cols)
            pltpu.make_async_copy(mine_hbm, cx.at[pl.ds(0, step), head_range], load_sem.at[s]).wait()
            pltpu.make_async_copy(dctx_hbm.at[dec_rows(c)], cx.at[pl.ds(step, dec), head_range], load_sem.at[tp + s]).wait()
        for copy in loads:
            copy.wait()

    @at(j < out_tiles)
    def _():
        mixed = None
        for s in range(tp):
            one = jnp.dot(cx[:, s * head_cols:(s + 1) * head_cols], wo_ref[s], preferred_element_type=F32)
            mixed = one if mixed is None else mixed + one
        cols = pl.ds(pl.multiple_of(j * TILE_OUT, TILE_OUT), TILE_OUT)
        hid[:, cols] = (hid[:, cols].astype(F32) + mixed).astype(BF)

    hid_copy = pltpu.make_async_copy(hid.at[pl.ds(0, rows)], hid_hbm.at[pl.ds(pl.multiple_of(c * rows, 8), rows)], hid_sem)

    @at(j == out_tiles)
    def _():
        hid_copy.start()
        block = hid.shape[0] // 11

        @pl.loop(0, 11)
        def _(b):
            some = pl.ds(pl.multiple_of(b * block, 16), block)
            h = hid[some].astype(F32)
            inv = lax.rsqrt(jnp.mean(h * h, axis=-1, keepdims=True) + NORM_EPS)
            cx[some] = (h * inv * gain_ref[...].astype(F32)).astype(BF)
            acc[c % ACCS, some] = jnp.zeros((block, width), F32)

    @at(j >= out_tiles)
    def _():
        gate = jnp.dot(cx[...], wg_ref[0], preferred_element_type=F32)
        up = jnp.dot(cx[...], wu_ref[0], preferred_element_type=F32)
        act = (jax.nn.silu(gate) * up).astype(BF)
        which = c % ACCS

        @at(j < ticks - 1)
        def _():
            acc[which] += jnp.dot(act, wd_ref[...], preferred_element_type=F32)

        @at(j == ticks - 1)
        def _():
            acc[which] += jnp.dot(act[:, :tail], wd_ref[:tail], preferred_element_type=F32)
            hid_copy.wait()

    @at((c == CHUNKS - 1) & (j == ticks - 1))
    def _():
        @pl.loop(SUBS * (CHUNKS - 1), total + 2 * last)
        def _(m):
            advance(m)

        for f, col, cols, peak in flows:
            for side, there, dist, outer, inner, more in sides(f):
                @at(there)
                def _(f=f, side=side, inner=inner, more=more):
                    for k in range(total - SLOTS, total):
                        rs_copy(f, k, side, inner).wait_send()

                    @at(more)
                    def _():
                        for k in range(total - SLOTS, total):
                            ag_copy(f, k, side, False).wait_send()

            @at(t == f)
            def _(f=f):
                for k in range(total - SLOTS, total):
                    fin_copy(f, k).wait()
                    for side, _, _, _, _, _ in sides(f):
                        ag_copy(f, k, side, True).wait_send()

        tokens.finish()
        for chunk in range(1, CHUNKS):
            spread(chunk).finish()


def layer_sums(ctx, dctx, mine, right, left, x, y, gain, w_full, w_gate_up, w_down):
    head_cols = ctx.shape[1]
    seq, width = x.shape
    step, dec = seq // CHUNKS, y.shape[0] // CHUNKS
    rows = step + dec
    ff = w_down.shape[0]
    ff_tiles = pl.cdiv(ff, TILE)
    tail = ff - (ff_tiles - 1) * TILE
    out_tiles = width // TILE_OUT
    tp = width // head_cols
    pad = (rows + 15) // 16 * 16
    sub = rows // SUBS
    total = CHUNKS * SUBS
    geo = (width, head_cols, step, dec, ff_tiles, tail)
    def ff_index(j):
        return jnp.maximum(j - out_tiles, 0)

    any_spec = pl.BlockSpec(memory_space=pl.ANY)
    flops = 2 * CHUNKS * rows * width * (width + 3 * ff)
    moved = 2 * CHUNKS * (width * width + 3 * width * ff)
    return pl.pallas_call(
        functools.partial(layer_kernel, geo),
        grid=(CHUNKS, out_tiles + ff_tiles),
        in_specs=[
            any_spec, any_spec, any_spec, [any_spec] * (tp - 1), [any_spec] * (tp - 1), any_spec, any_spec,
            pl.BlockSpec((1, width), lambda c, j: (0, 0)),
            pl.BlockSpec((tp, head_cols, TILE_OUT), lambda c, j: (0, 0, jnp.minimum(j, out_tiles - 1))),
            pl.BlockSpec((1, width, TILE), lambda c, j: (0, 0, ff_index(j))),
            pl.BlockSpec((1, width, TILE), lambda c, j: (1, 0, ff_index(j))),
            pl.BlockSpec((TILE, width), lambda c, j: (ff_index(j), 0)),
        ],
        out_specs=[any_spec, any_spec, any_spec, any_spec],
        out_shape=[
            jax.ShapeDtypeStruct((CHUNKS * rows, width), BF),
            jax.ShapeDtypeStruct((tp, CHUNKS - 1, step, head_cols), BF),
            jax.ShapeDtypeStruct((tp,) + dctx.shape, BF),
            jax.ShapeDtypeStruct((CHUNKS * rows, width), BF),
        ],
        scratch_shapes=[
            pltpu.VMEM((pad, width), BF),
            pltpu.VMEM((pad, width), BF),
            pltpu.VMEM((ACCS, pad, width), F32),
            [pltpu.VMEM((2, SLOTS, sub, groups * 128), F32) for groups in OWNED],
            [pltpu.VMEM((SLOTS, sub, groups * 128), BF) for groups in OWNED],
            [pltpu.VMEM((SLOTS, sub, groups * 128), BF) for groups in OWNED],
            pltpu.SemaphoreType.DMA((tp, 2, SLOTS)),
            pltpu.SemaphoreType.DMA((tp, SLOTS)),
            pltpu.SemaphoreType.REGULAR((tp,)),
            pltpu.SemaphoreType.DMA((tp, total)),
            pltpu.SemaphoreType.DMA((tp, 2, SLOTS)),
            pltpu.SemaphoreType.DMA((tp, SLOTS)),
            pltpu.SemaphoreType.DMA((tp, SLOTS)),
            pltpu.SemaphoreType.DMA((CHUNKS, tp)),
            pltpu.SemaphoreType.DMA((CHUNKS, tp, 2)),
            pltpu.SemaphoreType.DMA((2 * tp + 2,)),
            pltpu.SemaphoreType.DMA(()),
        ],
        compiler_params=pltpu.CompilerParams(collective_id=0, has_side_effects=True, vmem_limit_bytes=67000000, dimension_semantics=('arbitrary', 'arbitrary')),
        cost_estimate=pl.CostEstimate(flops=flops, bytes_accessed=moved, transcendentals=0),
        name='layer_sums',
    )(ctx, dctx, mine, right, left, x, y, gain, w_full, w_gate_up, w_gate_up, w_down)[0]


def decode_project(tokens, cache_lens, gain, w_qkv):
    group_q = w_qkv.shape[2] - 2
    normed = rms_norm(tokens, gain)
    projected = jnp.einsum('bd,dkjh->bkjh', normed, w_qkv, preferred_element_type=F32)
    rotated = rope_rotate(projected[:, :, :group_q + 1], cache_lens)
    local_qkv = jnp.concatenate([rotated, projected[:, :, group_q + 1:]], axis=2).astype(BF)[:, 0]
    return local_qkv


def decode_local(full_qkv, cache_lens, k_cache, v_cache):
    group_q, head_dim = full_qkv.shape[2] - 2, full_qkv.shape[3]
    cache_local = k_cache.shape[1]
    cache_pos = lax.axis_index('tp') * cache_local + jnp.arange(cache_local)
    write_mask = (cache_pos[None, :] == cache_lens[:, None])[:, :, None, None]
    allowed = (cache_pos[None, :] <= cache_lens[:, None])[None, :, None, :]
    key_now = jnp.where(write_mask, jnp.moveaxis(full_qkv[:, :, group_q], 0, 1)[:, None], k_cache)
    value_now = jnp.where(write_mask, jnp.moveaxis(full_qkv[:, :, group_q + 1], 0, 1)[:, None], v_cache)
    scores = jnp.einsum('kbgh,btkh->kbgt', full_qkv[:, :, :group_q], key_now, preferred_element_type=F32) * head_dim ** -0.5
    scores = jnp.where(allowed, scores, -1e30)
    top = jnp.max(scores, axis=-1)
    weights = jnp.exp(scores - top[..., None])
    mixed = jnp.einsum('kbgt,btkh->kbgh', weights.astype(BF), value_now, preferred_element_type=F32)
    stats = jnp.concatenate([top, jnp.sum(weights, axis=-1)], axis=-1)
    stats = jnp.pad(stats, ((0, 0), (0, 0), (0, head_dim - stats.shape[-1])))
    return jnp.concatenate([mixed, stats[:, :, None]], axis=2), key_now, value_now


def decode_combine(own):
    heads = own.shape[2] - 1
    top, total = own[:, :, heads, :heads], own[:, :, heads, heads:2 * heads]
    factor = jnp.exp(top - jnp.max(top, axis=0))
    return (jnp.sum(own[:, :, :heads] * factor[..., None], axis=0) / jnp.sum(total * factor, axis=0)[..., None]).astype(BF)


def pass_on(right, left, hop, tp):
    return (lax.ppermute(right, 'tp', [(place, place + 1) for place in range(hop - 1, tp - 1)]),
            lax.ppermute(left, 'tp', [(place, place - 1) for place in range(tp - hop, 0, -1)]))


def gather_w_out(w_out, mesh):
    rows = w_out.shape[0] // (mesh.shape['pair'] * mesh.shape['side'])
    index = lax.axis_index('pair') * mesh.shape['side'] + lax.axis_index('side')
    own = lax.dynamic_slice_in_dim(w_out, index * rows, rows, 0)
    return lax.all_gather(own, ('tp', 'pair', 'side'))


def solution(mesh):
    side_size = mesh.shape['side']
    tp = mesh.shape['tp']
    send_pairs = [(source, (source + 1) % side_size) for source in range(side_size)]
    group_axes = ('pair', 'side')

    def device_fn(x_prompt, s_len, y_tok, c_len, k_cache, v_cache, attn_gain, w_qkv, w_out, mlp_gain, w_gate_up, w_down):
        x = x_prompt[0]
        seq_len, width = x.shape
        group_q, head = w_qkv.shape[3] - 2, w_qkv.shape[4]
        positions = jnp.arange(seq_len)
        keep_mask = (positions < s_len[0])[:, None].astype(BF)
        cos, sin = rope_tables(positions, head)
        cos, sin = jnp.concatenate([cos, cos], -1), jnp.concatenate([-sin, sin], -1)

        w_full = gather_w_out(w_out[0, 0].reshape(group_q * head, width), mesh).reshape(tp, group_q * head, width)
        local_qkv = decode_project(y_tok, c_len, attn_gain[0], w_qkv[0])
        local_qkv, x = lax.optimization_barrier((local_qkv, x))
        full_qkv = lax.all_to_all(jnp.broadcast_to(local_qkv, (tp,) + local_qkv.shape), 'tp', 0, 0)

        w_slots = jnp.transpose(w_qkv[0, :, 0], (1, 0, 2))
        qkv = project_qkv(x, attn_gain, cos, sin, w_slots)
        qkv, full_qkv = lax.optimization_barrier((qkv, full_qkv))
        step, dec = seq_len // CHUNKS, y_tok.shape[0] // CHUNKS
        mine = attend(s_len, qkv, 0, step, step)
        moved = [pass_on(mine, mine, 1, tp)]
        kv_pair = qkv[group_q:] * keep_mask
        full_qkv, mine = lax.optimization_barrier((full_qkv, mine))
        mixed, key_now, value_now = decode_local(full_qkv, c_len, k_cache[0], v_cache[0])
        kv_near = lax.ppermute(kv_pair, 'side', send_pairs)
        w_gate_up, moved[0], mixed, value_now = lax.optimization_barrier((w_gate_up, moved[0], mixed, value_now))
        mixed = lax.all_to_all(mixed, 'tp', 0, 0)
        moved.append(pass_on(*moved[0], 2, tp))
        gate_up = jnp.transpose(w_gate_up[0], (1, 0, 2))
        qkv, gate_up = lax.optimization_barrier((qkv, gate_up))
        rest = seq_len - step
        ctx = attend(s_len, qkv, step, rest - step, rest)
        ctx, moved[1], mixed, kv_near = lax.optimization_barrier((ctx, moved[1], mixed, kv_near))
        dctx = decode_combine(mixed)
        kv_recv = lax.all_to_all(kv_near[:, :, None], 'tp', 1, 2, tiled=True)
        moved.append(pass_on(*moved[1], 3, tp))
        ctx = attend(s_len, qkv, rest, step, rest, ctx)
        ctx, moved[2], kv_recv = lax.optimization_barrier((ctx, moved[2], kv_recv))

        done = layer_sums(ctx, dctx.reshape(-1, ctx.shape[1]), mine, [r for r, _ in moved], [l for _, l in moved], x, y_tok, mlp_gain, w_full, gate_up, w_down[0])
        done = done.reshape(CHUNKS, step + dec, width)
        hidden = done[:, :step].reshape(seq_len, width)
        tokens = done[:, step:].reshape(CHUNKS * dec, width)

        return (hidden[None], tokens, kv_recv[0][None, None], kv_recv[1][None, None], key_now[None], value_now[None])

    cache_spec = P(None, group_axes, 'tp', None, None)
    in_specs = (P(group_axes, None, None), P(group_axes), P(group_axes, None), P(group_axes), cache_spec, cache_spec, P(), P(None, None, 'tp', None, None), P(None, 'tp', None, None, None), P(), P(None, None, None, 'tp'), P(None, 'tp', None))
    out_specs = (P(group_axes, None, None), P(group_axes, None), cache_spec, cache_spec, cache_spec, cache_spec)
    return jax.shard_map(device_fn, mesh=mesh, in_specs=in_specs, out_specs=out_specs, check_vma=False)
```

```python
import functools

import jax
import jax.numpy as jnp
from jax import lax
from jax.experimental import pallas as pl
from jax.experimental.pallas import tpu as pltpu
from jax.sharding import PartitionSpec as P

ROPE_BASE = 10000.0
NORM_EPS = 1e-5
LOG2E = 1.4426950408889634
BF = jnp.bfloat16
F32 = jnp.float32


def rms_norm(hidden, norm_gain):
    hidden_f32 = hidden.astype(F32)
    inv_rms = lax.rsqrt(jnp.mean(hidden_f32 * hidden_f32, axis=-1, keepdims=True) + NORM_EPS)
    return (hidden_f32 * inv_rms * norm_gain.astype(F32)).astype(BF)


def rope_tables(positions, head_dim):
    half_dim = head_dim // 2
    inv_freq = ROPE_BASE ** (-2.0 * jnp.arange(half_dim, dtype=F32) / head_dim)
    angles = positions.astype(F32)[:, None] * inv_freq[None, :]
    return jnp.cos(angles), jnp.sin(angles)


def rope_rotate(vals_f32, positions):
    half_dim = vals_f32.shape[-1] // 2
    cos_table, sin_table = rope_tables(positions, vals_f32.shape[-1])
    cos_table, sin_table = cos_table[:, None, None, :], sin_table[:, None, None, :]
    first_half = vals_f32[..., :half_dim]
    second_half = vals_f32[..., half_dim:]
    return jnp.concatenate([first_half * cos_table - second_half * sin_table, second_half * cos_table + first_half * sin_table], axis=-1)


def qkv_kernel(x_ref, gain_ref, cos_ref, sin_ref, w_ref, o_ref):
    slots = w_ref.shape[0]
    x = x_ref[...].astype(F32)
    inv = lax.rsqrt(jnp.mean(x * x, axis=-1, keepdims=True) + NORM_EPS)
    normed = (x * inv * gain_ref[...].astype(F32)).astype(BF)
    cos, sin = cos_ref[...], sin_ref[...]
    for first in range(0, slots, 2):
        group = range(first, min(first + 2, slots))
        w = jnp.concatenate([w_ref[s] for s in group], axis=-1)
        y = jnp.dot(normed, w, preferred_element_type=F32)
        for n, s in enumerate(group):
            part = y[:, n * 128:(n + 1) * 128]
            if s < slots - 1:
                part = part * cos + pltpu.roll(part, 64, 1) * sin
            o_ref[s] = part.astype(BF)


def project_qkv(x, gain, cos, sin, w, rows_block=256):
    rows, width = x.shape
    slots, _, head = w.shape
    return pl.pallas_call(
        qkv_kernel,
        grid=(rows // rows_block,),
        in_specs=[
            pl.BlockSpec((rows_block, width), lambda i: (i, 0)),
            pl.BlockSpec((1, width), lambda i: (0, 0)),
            pl.BlockSpec((rows_block, head), lambda i: (i, 0)),
            pl.BlockSpec((rows_block, head), lambda i: (i, 0)),
            pl.BlockSpec((slots, width, head), lambda i: (0, 0, 0), pipeline_mode=pl.Buffered(1)),
        ],
        out_specs=pl.BlockSpec((slots, rows_block, head), lambda i: (0, i, 0)),
        out_shape=jax.ShapeDtypeStruct((slots, rows, head), BF),
        cost_estimate=pl.CostEstimate(flops=2 * rows * width * slots * head, bytes_accessed=2 * (rows * width + slots * head * (width + rows)), transcendentals=0),
        name="project_qkv",
    )(x, gain, cos, sin, w)


MESH = pl.DeviceIdType.MESH


def to(device):
    return dict(device_id={'tp': device}, device_id_type=MESH)


def meet_neighbours(t, last):
    barrier = pltpu.get_barrier_semaphore()

    @pl.when(t > 0)
    def _():
        pl.semaphore_signal(barrier, inc=1, **to(t - 1))

    @pl.when(t < last)
    def _():
        pl.semaphore_signal(barrier, inc=1, **to(t + 1))

    @pl.when((t > 0) & (t < last))
    def _():
        pl.semaphore_wait(barrier, 2)

    @pl.when((t == 0) | (t == last))
    def _():
        pl.semaphore_wait(barrier, 1)


class Spread:
    def __init__(self, t, last, own, place, send_sem, recv_sem):
        self.t, self.last, self.own, self.place, self.send_sem, self.recv_sem = t, last, own, place, send_sem, recv_sem

    def copy(self, source, way, first=False):
        return pltpu.make_async_remote_copy(
            src_ref=self.own if first else self.place(source), dst_ref=self.place(source), send_sem=self.send_sem(source, way),
            recv_sem=self.recv_sem(source), **to(self.t + 1 if way == 0 else self.t - 1))

    def start(self):
        @pl.when(self.t < self.last)
        def _():
            self.copy(self.t, 0, True).start()

        @pl.when(self.t > 0)
        def _():
            self.copy(self.t, 1, True).start()

    def hop(self, n):
        t, last = self.t, self.last

        @pl.when(t >= n)
        def _():
            self.copy(t - n, 0).wait_recv()

            @pl.when(t < last)
            def _():
                self.copy(t - n, 0).start()

        @pl.when(t + n <= last)
        def _():
            self.copy(t + n, 1).wait_recv()

            @pl.when(t > 0)
            def _():
                self.copy(t + n, 1).start()

    def finish(self):
        for source in range(self.last + 1):
            @pl.when((source <= self.t) & (self.t < self.last))
            def _(source=source):
                self.copy(source, 0).wait_send()

            @pl.when((source >= self.t) & (self.t > 0))
            def _(source=source):
                self.copy(source, 1).wait_send()


def flash_kernel(block_q, block_k, some, base, slen_ref, q_ref, k_ref, v_ref, *refs):
    o_ref, s_ref, m_ref, l_ref, p_ref, acc_ref = refs[-6:]
    i = pl.program_id(0) + base
    heads, _, head = q_ref.shape
    rows = heads * block_q
    pieces = rows // some
    lanes = block_k // 128
    slen = slen_ref[0]
    scale = head ** -0.5 * LOG2E
    count = (i * block_q + block_q - 1) // block_k + 1

    def cols(j):
        return pl.ds(pl.multiple_of(j * block_k, block_k), block_k)

    @pl.loop(0, count)
    def _(j):
        k = k_ref[0, cols(j), :]
        s_ref[:, cols(j)] = lax.dot_general(q_ref[...].reshape(rows, head), k, (((1,), (1,)), ((), ())), preferred_element_type=F32)
        edge = ((j + 1) * block_k > i * block_q) | ((j + 1) * block_k > k_ref.shape[1] // 2)

        @pl.when(edge)
        def _():
            @pl.loop(0, pieces)
            def _(r):
                here = pl.ds(pl.multiple_of(r * some, some), some)
                q_pos = i * block_q + (r * some) % block_q + lax.broadcasted_iota(jnp.int32, (some, block_k), 0)
                k_pos = j * block_k + lax.broadcasted_iota(jnp.int32, (some, block_k), 1)
                s_ref[here, cols(j)] = jnp.where((k_pos <= q_pos) & (k_pos < slen), s_ref[here, cols(j)], -1e30)

    tall = rows // heads

    @pl.loop(0, heads)
    def _(r):
        here = pl.ds(pl.multiple_of(r * tall, tall), tall)

        def more(j, top):
            s = s_ref[here, cols(j)]
            for n in range(lanes):
                top = jnp.maximum(top, s[:, n * 128:(n + 1) * 128])
            return top

        top = lax.fori_loop(0, count, more, jnp.full((tall, 128), -jnp.inf, F32))
        m_ref[here] = jnp.broadcast_to(jnp.max(top, axis=-1, keepdims=True), (tall, 128))

    l_ref[...] = jnp.zeros_like(l_ref)
    acc_ref[...] = jnp.zeros_like(acc_ref)

    @pl.loop(0, count)
    def _(j):
        @pl.loop(0, pieces, unroll=2)
        def _(r):
            here = pl.ds(pl.multiple_of(r * some, some), some)
            s = s_ref[here, cols(j)]
            m = m_ref[here]
            total = l_ref[here]
            for n in range(lanes):
                w = jnp.exp2((s[:, n * 128:(n + 1) * 128] - m) * scale)
                total = total + w
                p_ref[here, n * 128:(n + 1) * 128] = w.astype(BF)
            l_ref[here] = total

        acc_ref[...] += jnp.dot(p_ref[...], v_ref[0, cols(j), :], preferred_element_type=F32)

    for h in range(heads):
        here = slice(h * block_q, (h + 1) * block_q)
        o_ref[:, h * head:(h + 1) * head] = (acc_ref[here] / jnp.sum(l_ref[here], axis=-1, keepdims=True)).astype(BF)


def attend(slen, qkv, first, count, origin, total, into=None, block_q=256, block_k=512, some=32):
    slots, rows, head = qkv.shape
    heads = slots - 2
    tall = heads * block_q
    base = first // block_q
    place = (first - origin) // block_q
    more = [] if into is None else [into]
    share = (first + count) ** 2 - first ** 2
    return pl.pallas_call(
        functools.partial(flash_kernel, block_q, block_k, some, base),
        grid_spec=pltpu.PrefetchScalarGridSpec(
            num_scalar_prefetch=1,
            grid=(count // block_q,),
            in_specs=[
                pl.BlockSpec((heads, block_q, head), lambda i, _: (0, i + base, 0)),
                pl.BlockSpec((1, rows, head), lambda i, _: (heads, 0, 0)),
                pl.BlockSpec((1, rows, head), lambda i, _: (heads + 1, 0, 0)),
            ] + [pl.BlockSpec(memory_space=pl.ANY) for _ in more],
            out_specs=pl.BlockSpec((block_q, heads * head), lambda i, _: (i + place, 0)),
            scratch_shapes=[
                pltpu.VMEM((tall, rows), F32),
                pltpu.VMEM((tall, 128), F32),
                pltpu.VMEM((tall, 128), F32),
                pltpu.VMEM((tall, block_k), BF),
                pltpu.VMEM((tall, head), F32),
            ],
        ),
        out_shape=jax.ShapeDtypeStruct((total, heads * head), BF),
        input_output_aliases={4: 0} if more else {},
        cost_estimate=pl.CostEstimate(flops=3 * heads * share * head, bytes_accessed=2 * (2 * heads + 2) * count * head, transcendentals=heads * share // 2),
        name='attend',
    )(slen, qkv, qkv, qkv, *more)


CHUNKS = 4
SUBS = 5
SLOTS = 2
ACCS = 3
TILE = 256
TILE_OUT = 512
OWNED = (11, 3, 3, 11)


def layer_kernel(geo, ctx_hbm, dctx_hbm, mine_hbm, right_hbm, left_hbm, x_hbm, y_hbm, gain_ref, wo_ref, wg_ref, wu_ref, wd_ref, out_hbm, full_hbm, dfull_hbm, hid_hbm,
                 cx, hid, acc, slots, fins, ress, rs_recv, rs_send, credit, ag_recv, ag_send, fin_sem, res_sem,
                 ctx_recv, ctx_send, load_sem, hid_sem):
    width, head_cols, step, dec, ff_tiles, tail = geo
    rows = step + dec
    sub = rows // SUBS
    total = CHUNKS * SUBS
    out_tiles = width // TILE_OUT
    ticks = out_tiles + ff_tiles
    stride = ticks // SUBS
    tp = width // head_cols
    last = tp - 1
    c, j = pl.program_id(0), pl.program_id(1)
    t = lax.axis_index('tp')

    def at(cond):
        return pl.when(cond)

    def step_rows(chunk):
        return pl.ds(pl.multiple_of(chunk * step, 8), step)

    def dec_rows(chunk):
        return pl.ds(pl.multiple_of(chunk * dec, 8), dec)

    def spread(chunk):
        return Spread(t, last, ctx_hbm.at[step_rows(chunk - 1)], lambda source: full_hbm.at[source, chunk - 1],
                      lambda source, way: ctx_send.at[chunk, source, way], lambda source: ctx_recv.at[chunk, source])

    tokens = Spread(t, last, dctx_hbm, lambda source: dfull_hbm.at[source],
                    lambda source, way: ctx_send.at[0, source, way], lambda source: ctx_recv.at[0, source])

    flows = []
    for f, groups in enumerate(OWNED):
        flows.append((f, sum(OWNED[:f]) * 128, groups * 128, max(f, last - f)))

    def rows_of(k):
        return pl.ds(pl.multiple_of(k * sub, 8), sub)

    def part(f, k):
        _, col, cols, _ = flows[f]
        first = pl.multiple_of((k % SUBS) * sub, 8)
        return acc.at[(k // SUBS) % ACCS, pl.ds(first, sub), pl.ds(col, cols)]

    def out_part(f, k):
        _, col, cols, _ = flows[f]
        return out_hbm.at[rows_of(k), pl.ds(col, cols)]

    def rs_copy(f, k, side, device):
        return pltpu.make_async_remote_copy(
            src_ref=part(f, k), dst_ref=slots[f].at[side, k % SLOTS], send_sem=rs_send.at[f, k % SLOTS],
            recv_sem=rs_recv.at[f, side, k % SLOTS], **to(device))

    def ag_copy(f, k, way, first):
        return pltpu.make_async_remote_copy(
            src_ref=fins[f].at[k % SLOTS] if first else out_part(f, k), dst_ref=out_part(f, k), send_sem=ag_send.at[f, way, k % SLOTS],
            recv_sem=ag_recv.at[f, k], **to(t + 1 if way == 0 else t - 1))

    def fin_copy(f, k):
        return pltpu.make_async_copy(fins[f].at[k % SLOTS], out_part(f, k), fin_sem.at[f, k % SLOTS])

    def res_copy(f, k):
        _, col, cols, _ = flows[f]
        return pltpu.make_async_copy(hid_hbm.at[rows_of(k), pl.ds(col, cols)], ress[f].at[k % SLOTS], res_sem.at[f, k % SLOTS])

    def sides(f):
        found = []
        if f < last:
            found.append((0, t > f, t - f, t + 1, t - 1, t < last))
        if f > 0:
            found.append((1, t < f, f - t, t - 1, t + 1, t > 0))
        return found

    def inside(k):
        return (k >= 0) & (k < total)

    def advance(m):
        for f, col, cols, peak in flows:
            for side, there, dist, outer, inner, more in sides(f):
                k = m - peak + dist

                @at(inside(k) & there)
                def _(f=f, side=side, outer=outer, inner=inner, more=more, k=k):
                    @at(more)
                    def _():
                        rs_copy(f, k, side, inner).wait_recv()
                        mine = part(f, k)
                        mine[...] += slots[f][side, k % SLOTS]

                        @at(k + SLOTS < total)
                        def _():
                            pl.semaphore_signal(credit.at[f], inc=1, **to(outer))

                    @at(k >= SLOTS)
                    def _():
                        pl.semaphore_wait(credit.at[f], 1)
                        rs_copy(f, k - SLOTS, side, inner).wait_send()

                    rs_copy(f, k, side, inner).start()

            k = m - peak

            @at(inside(k) & (t == f))
            def _(f=f, k=k):
                both = part(f, k)[...]
                for side, _, _, outer, inner, _ in sides(f):
                    rs_copy(f, k, side, inner).wait_recv()
                    both = both + slots[f][side, k % SLOTS]
                res_copy(f, k).wait()

                @at(k >= SLOTS)
                def _():
                    fin_copy(f, k - SLOTS).wait()
                    for side, _, _, _, _, _ in sides(f):
                        ag_copy(f, k - SLOTS, side, True).wait_send()

                fins[f][k % SLOTS] = (ress[f][k % SLOTS].astype(F32) + both).astype(BF)

                @at(k + SLOTS < total)
                def _():
                    for side, _, _, outer, _, _ in sides(f):
                        pl.semaphore_signal(credit.at[f], inc=1, **to(outer))

        for f, col, cols, peak in flows:
            k = m - peak

            @at(inside(k) & (t == f))
            def _(f=f, k=k):
                for side, _, _, _, _, _ in sides(f):
                    ag_copy(f, k, side, True).start()
                fin_copy(f, k).start()

            @at(inside(k + 1) & (t == f))
            def _(f=f, k=k):
                res_copy(f, k + 1).start()

        for f, col, cols, peak in flows:
            for side, there, dist, outer, inner, more in sides(f):
                a = m - peak - dist

                @at(inside(a) & there)
                def _(f=f, side=side, more=more, a=a):
                    ag_copy(f, a, side, False).wait_recv()

                    @at(more)
                    def _():
                        @at(a >= SLOTS)
                        def _():
                            ag_copy(f, a - SLOTS, side, False).wait_send()

                        ag_copy(f, a, side, False).start()

    @at((c == 0) & (j == 0))
    def _():
        meet_neighbours(t, last)
        tokens.start()
        spread(1).start()
        cx[...] = jnp.zeros_like(cx)
        hid[...] = jnp.zeros_like(hid)
    @at((c > 0) & (j % stride == 0) & (j < stride * SUBS))
    def _():
        advance(SUBS * (c - 1) + j // stride)

    for n in range(1, last + 1):
        @at((c + 1 < CHUNKS) & (j == ticks * n // (last + 1) + 1))
        def _(n=n):
            spread(c + 1).hop(n)
            if n == last:
                @at(c + 2 < CHUNKS)
                def _():
                    spread(c + 2).start()

    @at(j == 0)
    def _():
        loads = [
            pltpu.make_async_copy(x_hbm.at[step_rows(c)], hid.at[pl.ds(0, step)], load_sem.at[2 * tp]),
            pltpu.make_async_copy(y_hbm.at[dec_rows(c)], hid.at[pl.ds(step, dec)], load_sem.at[2 * tp + 1]),
        ]
        for copy in loads:
            copy.start()
        for s in range(tp):
            head_range = pl.ds(s * head_cols, head_cols)
            where = cx.at[pl.ds(0, step), head_range]

            for device in range(tp):
                piece = mine_hbm if device == s else right_hbm[device - s - 1] if device > s else left_hbm[s - device - 1]

                @at((c == 0) & (t == device))
                def _(s=s, where=where, piece=piece):
                    pltpu.make_async_copy(piece, where, load_sem.at[s]).start()

            @at((c > 0) & (t == s))
            def _(s=s, where=where):
                pltpu.make_async_copy(ctx_hbm.at[step_rows(c - 1)], where, load_sem.at[s]).start()

            @at((c > 0) & (t != s))
            def _(s=s, where=where):
                pltpu.make_async_copy(full_hbm.at[s, c - 1], where, load_sem.at[s]).start()

        @at(c == 0)
        def _():
            for n in range(1, last + 1):
                tokens.hop(n)

        for s in range(tp):
            head_range = pl.ds(s * head_cols, head_cols)
            tail_rows = cx.at[pl.ds(step, dec), head_range]

            @at(t == s)
            def _(s=s, tail_rows=tail_rows):
                pltpu.make_async_copy(dctx_hbm.at[dec_rows(c)], tail_rows, load_sem.at[tp + s]).start()

            @at(t != s)
            def _(s=s, tail_rows=tail_rows):
                pltpu.make_async_copy(dfull_hbm.at[s, dec_rows(c)], tail_rows, load_sem.at[tp + s]).start()

        for s in range(tp):
            head_range = pl.ds(s * head_cols, head_cols)
            pltpu.make_async_copy(mine_hbm, cx.at[pl.ds(0, step), head_range], load_sem.at[s]).wait()
            pltpu.make_async_copy(dctx_hbm.at[dec_rows(c)], cx.at[pl.ds(step, dec), head_range], load_sem.at[tp + s]).wait()
        for copy in loads:
            copy.wait()

    @at(j < out_tiles)
    def _():
        mixed = None
        for s in range(tp):
            one = jnp.dot(cx[:, s * head_cols:(s + 1) * head_cols], wo_ref[s], preferred_element_type=F32)
            mixed = one if mixed is None else mixed + one
        cols = pl.ds(pl.multiple_of(j * TILE_OUT, TILE_OUT), TILE_OUT)
        hid[:, cols] = (hid[:, cols].astype(F32) + mixed).astype(BF)

    hid_copy = pltpu.make_async_copy(hid.at[pl.ds(0, rows)], hid_hbm.at[pl.ds(pl.multiple_of(c * rows, 8), rows)], hid_sem)

    @at(j == out_tiles)
    def _():
        hid_copy.start()
        block = hid.shape[0] // 11

        @pl.loop(0, 11)
        def _(b):
            some = pl.ds(pl.multiple_of(b * block, 16), block)
            h = hid[some].astype(F32)
            inv = lax.rsqrt(jnp.mean(h * h, axis=-1, keepdims=True) + NORM_EPS)
            cx[some] = (h * inv * gain_ref[...].astype(F32)).astype(BF)
            acc[c % ACCS, some] = jnp.zeros((block, width), F32)

    @at(j >= out_tiles)
    def _():
        gate = jnp.dot(cx[...], wg_ref[0], preferred_element_type=F32)
        up = jnp.dot(cx[...], wu_ref[0], preferred_element_type=F32)
        act = (jax.nn.silu(gate) * up).astype(BF)
        which = c % ACCS

        @at(j < ticks - 1)
        def _():
            acc[which] += jnp.dot(act, wd_ref[...], preferred_element_type=F32)

        @at(j == ticks - 1)
        def _():
            acc[which] += jnp.dot(act[:, :tail], wd_ref[:tail], preferred_element_type=F32)
            hid_copy.wait()

    @at((c == CHUNKS - 1) & (j == ticks - 1))
    def _():
        @pl.loop(SUBS * (CHUNKS - 1), total + 2 * last)
        def _(m):
            advance(m)

        for f, col, cols, peak in flows:
            for side, there, dist, outer, inner, more in sides(f):
                @at(there)
                def _(f=f, side=side, inner=inner, more=more):
                    for k in range(total - SLOTS, total):
                        rs_copy(f, k, side, inner).wait_send()

                    @at(more)
                    def _():
                        for k in range(total - SLOTS, total):
                            ag_copy(f, k, side, False).wait_send()

            @at(t == f)
            def _(f=f):
                for k in range(total - SLOTS, total):
                    fin_copy(f, k).wait()
                    for side, _, _, _, _, _ in sides(f):
                        ag_copy(f, k, side, True).wait_send()

        tokens.finish()
        for chunk in range(1, CHUNKS):
            spread(chunk).finish()


def layer_sums(ctx, dctx, mine, right, left, x, y, gain, w_full, w_gate_up, w_down):
    head_cols = ctx.shape[1]
    seq, width = x.shape
    step, dec = seq // CHUNKS, y.shape[0] // CHUNKS
    rows = step + dec
    ff = w_down.shape[0]
    ff_tiles = pl.cdiv(ff, TILE)
    tail = ff - (ff_tiles - 1) * TILE
    out_tiles = width // TILE_OUT
    tp = width // head_cols
    pad = (rows + 15) // 16 * 16
    sub = rows // SUBS
    total = CHUNKS * SUBS
    geo = (width, head_cols, step, dec, ff_tiles, tail)
    def ff_index(j):
        return jnp.maximum(j - out_tiles, 0)

    any_spec = pl.BlockSpec(memory_space=pl.ANY)
    flops = 2 * CHUNKS * rows * width * (width + 3 * ff)
    moved = 2 * CHUNKS * (width * width + 3 * width * ff)
    return pl.pallas_call(
        functools.partial(layer_kernel, geo),
        grid=(CHUNKS, out_tiles + ff_tiles),
        in_specs=[
            any_spec, any_spec, any_spec, [any_spec] * (tp - 1), [any_spec] * (tp - 1), any_spec, any_spec,
            pl.BlockSpec((1, width), lambda c, j: (0, 0)),
            pl.BlockSpec((tp, head_cols, TILE_OUT), lambda c, j: (0, 0, jnp.minimum(j, out_tiles - 1))),
            pl.BlockSpec((1, width, TILE), lambda c, j: (0, 0, ff_index(j))),
            pl.BlockSpec((1, width, TILE), lambda c, j: (1, 0, ff_index(j))),
            pl.BlockSpec((TILE, width), lambda c, j: (ff_index(j), 0)),
        ],
        out_specs=[any_spec, any_spec, any_spec, any_spec],
        out_shape=[
            jax.ShapeDtypeStruct((CHUNKS * rows, width), BF),
            jax.ShapeDtypeStruct((tp, CHUNKS - 1, step, head_cols), BF),
            jax.ShapeDtypeStruct((tp,) + dctx.shape, BF),
            jax.ShapeDtypeStruct((CHUNKS * rows, width), BF),
        ],
        scratch_shapes=[
            pltpu.VMEM((pad, width), BF),
            pltpu.VMEM((pad, width), BF),
            pltpu.VMEM((ACCS, pad, width), F32),
            [pltpu.VMEM((2, SLOTS, sub, groups * 128), F32) for groups in OWNED],
            [pltpu.VMEM((SLOTS, sub, groups * 128), BF) for groups in OWNED],
            [pltpu.VMEM((SLOTS, sub, groups * 128), BF) for groups in OWNED],
            pltpu.SemaphoreType.DMA((tp, 2, SLOTS)),
            pltpu.SemaphoreType.DMA((tp, SLOTS)),
            pltpu.SemaphoreType.REGULAR((tp,)),
            pltpu.SemaphoreType.DMA((tp, total)),
            pltpu.SemaphoreType.DMA((tp, 2, SLOTS)),
            pltpu.SemaphoreType.DMA((tp, SLOTS)),
            pltpu.SemaphoreType.DMA((tp, SLOTS)),
            pltpu.SemaphoreType.DMA((CHUNKS, tp)),
            pltpu.SemaphoreType.DMA((CHUNKS, tp, 2)),
            pltpu.SemaphoreType.DMA((2 * tp + 2,)),
            pltpu.SemaphoreType.DMA(()),
        ],
        compiler_params=pltpu.CompilerParams(collective_id=0, has_side_effects=True, vmem_limit_bytes=67000000, dimension_semantics=('arbitrary', 'arbitrary')),
        cost_estimate=pl.CostEstimate(flops=flops, bytes_accessed=moved, transcendentals=0),
        name='layer_sums',
    )(ctx, dctx, mine, right, left, x, y, gain, w_full, w_gate_up, w_gate_up, w_down)[0]


def decode_project(tokens, cache_lens, gain, w_qkv):
    group_q = w_qkv.shape[2] - 2
    normed = rms_norm(tokens, gain)
    projected = jnp.einsum('bd,dkjh->bkjh', normed, w_qkv, preferred_element_type=F32)
    rotated = rope_rotate(projected[:, :, :group_q + 1], cache_lens)
    local_qkv = jnp.concatenate([rotated, projected[:, :, group_q + 1:]], axis=2).astype(BF)[:, 0]
    return local_qkv


def decode_local(full_qkv, cache_lens, k_cache, v_cache):
    group_q, head_dim = full_qkv.shape[2] - 2, full_qkv.shape[3]
    cache_local = k_cache.shape[1]
    cache_pos = lax.axis_index('tp') * cache_local + jnp.arange(cache_local)
    write_mask = (cache_pos[None, :] == cache_lens[:, None])[:, :, None, None]
    allowed = (cache_pos[None, :] <= cache_lens[:, None])[None, :, None, :]
    key_now = jnp.where(write_mask, jnp.moveaxis(full_qkv[:, :, group_q], 0, 1)[:, None], k_cache)
    value_now = jnp.where(write_mask, jnp.moveaxis(full_qkv[:, :, group_q + 1], 0, 1)[:, None], v_cache)
    scores = jnp.einsum('kbgh,btkh->kbgt', full_qkv[:, :, :group_q], key_now, preferred_element_type=F32) * head_dim ** -0.5
    scores = jnp.where(allowed, scores, -1e30)
    top = jnp.max(scores, axis=-1)
    weights = jnp.exp(scores - top[..., None])
    mixed = jnp.einsum('kbgt,btkh->kbgh', weights.astype(BF), value_now, preferred_element_type=F32)
    stats = jnp.concatenate([top, jnp.sum(weights, axis=-1)], axis=-1)
    stats = jnp.pad(stats, ((0, 0), (0, 0), (0, head_dim - stats.shape[-1])))
    return jnp.concatenate([mixed, stats[:, :, None]], axis=2), key_now, value_now


def decode_combine(own):
    heads = own.shape[2] - 1
    top, total = own[:, :, heads, :heads], own[:, :, heads, heads:2 * heads]
    factor = jnp.exp(top - jnp.max(top, axis=0))
    return (jnp.sum(own[:, :, :heads] * factor[..., None], axis=0) / jnp.sum(total * factor, axis=0)[..., None]).astype(BF)


def pass_on(right, left, hop, tp):
    return (lax.ppermute(right, 'tp', [(place, place + 1) for place in range(hop - 1, tp - 1)]),
            lax.ppermute(left, 'tp', [(place, place - 1) for place in range(tp - hop, 0, -1)]))


def gather_w_out(w_out, mesh):
    rows = w_out.shape[0] // (mesh.shape['pair'] * mesh.shape['side'])
    index = lax.axis_index('pair') * mesh.shape['side'] + lax.axis_index('side')
    own = lax.dynamic_slice_in_dim(w_out, index * rows, rows, 0)
    return lax.all_gather(own, ('tp', 'pair', 'side'))


def solution(mesh):
    side_size = mesh.shape['side']
    tp = mesh.shape['tp']
    send_pairs = [(source, (source + 1) % side_size) for source in range(side_size)]
    group_axes = ('pair', 'side')

    def device_fn(x_prompt, s_len, y_tok, c_len, k_cache, v_cache, attn_gain, w_qkv, w_out, mlp_gain, w_gate_up, w_down):
        x = x_prompt[0]
        seq_len, width = x.shape
        group_q, head = w_qkv.shape[3] - 2, w_qkv.shape[4]
        positions = jnp.arange(seq_len)
        keep_mask = (positions < s_len[0])[:, None].astype(BF)
        cos, sin = rope_tables(positions, head)
        cos, sin = jnp.concatenate([cos, cos], -1), jnp.concatenate([-sin, sin], -1)

        w_full = gather_w_out(w_out[0, 0].reshape(group_q * head, width), mesh).reshape(tp, group_q * head, width)
        local_qkv = decode_project(y_tok, c_len, attn_gain[0], w_qkv[0])
        local_qkv, x = lax.optimization_barrier((local_qkv, x))
        full_qkv = lax.all_to_all(jnp.broadcast_to(local_qkv, (tp,) + local_qkv.shape), 'tp', 0, 0)

        w_slots = jnp.transpose(w_qkv[0, :, 0], (1, 0, 2))
        qkv = project_qkv(x, attn_gain, cos, sin, w_slots)
        qkv, full_qkv = lax.optimization_barrier((qkv, full_qkv))
        step, dec = seq_len // CHUNKS, y_tok.shape[0] // CHUNKS
        mine = attend(s_len, qkv, 0, step, 0, step)
        moved = [pass_on(mine, mine, 1, tp)]
        kv_pair = qkv[group_q:] * keep_mask
        full_qkv, mine = lax.optimization_barrier((full_qkv, mine))
        mixed, key_now, value_now = decode_local(full_qkv, c_len, k_cache[0], v_cache[0])
        kv_near = lax.ppermute(kv_pair, 'side', send_pairs)
        late = seq_len - step
        ctx = attend(s_len, qkv, step, step, step, late)
        w_gate_up, moved[0], mixed, value_now, ctx = lax.optimization_barrier((w_gate_up, moved[0], mixed, value_now, ctx))
        mixed = lax.all_to_all(mixed, 'tp', 0, 0)
        moved.append(pass_on(*moved[0], 2, tp))
        gate_up = jnp.transpose(w_gate_up[0], (1, 0, 2))
        qkv, gate_up, ctx = lax.optimization_barrier((qkv, gate_up, ctx))
        ctx = attend(s_len, qkv, late, step, step, late, ctx)
        ctx, moved[1], mixed, kv_near = lax.optimization_barrier((ctx, moved[1], mixed, kv_near))
        dctx = decode_combine(mixed)
        kv_recv = lax.all_to_all(kv_near[:, :, None], 'tp', 1, 2, tiled=True)
        moved.append(pass_on(*moved[1], 3, tp))
        ctx = attend(s_len, qkv, 2 * step, late - 2 * step, step, late, ctx)
        ctx, moved[2], kv_recv = lax.optimization_barrier((ctx, moved[2], kv_recv))

        done = layer_sums(ctx, dctx.reshape(-1, ctx.shape[1]), mine, [r for r, _ in moved], [l for _, l in moved], x, y_tok, mlp_gain, w_full, gate_up, w_down[0])
        done = done.reshape(CHUNKS, step + dec, width)
        hidden = done[:, :step].reshape(seq_len, width)
        tokens = done[:, step:].reshape(CHUNKS * dec, width)

        return (hidden[None], tokens, kv_recv[0][None, None], kv_recv[1][None, None], key_now[None], value_now[None])

    cache_spec = P(None, group_axes, 'tp', None, None)
    in_specs = (P(group_axes, None, None), P(group_axes), P(group_axes, None), P(group_axes), cache_spec, cache_spec, P(), P(None, None, 'tp', None, None), P(None, 'tp', None, None, None), P(), P(None, None, None, 'tp'), P(None, 'tp', None))
    out_specs = (P(group_axes, None, None), P(group_axes, None), cache_spec, cache_spec, cache_spec, cache_spec)
    return jax.shard_map(device_fn, mesh=mesh, in_specs=in_specs, out_specs=out_specs, check_vma=False)
```
